32 devices in a mesh: gx: 4 (over z), gy: 2 (over x), gz: 4 (over y, core).
Axes of the slice: x: 2, y: 2, z: 4, core: 2. Of those that a mesh axis runs over, the one named last changes fastest.
Arguments:
- fields_now: float32 [24, 32, 16, 512], P(None, 'gx', 'gy', 'gz'), may hold values from -6 to 6
- parent: float32 [24, 32, 16, 512], P(None, 'gx', 'gy', 'gz'), may hold values from -6 to 6
- advect: float32 [3, 24, 24], replicated, may hold values from -0.75 to 0.75
- diffuse: float32 [3, 24, 24], replicated, may hold values from -0.25 to 0.25
- box_shift: int32 [3], replicated, may hold values from 1 to 4
Outputs:
- section_slope: float32 [24, 32, 16, 512], P(None, 'gx', 'gy', 'gz')
- section_value: float32 [24, 32, 16, 512], P(None, 'gx', 'gy', 'gz')
The draws below stay inside these ranges and needn't reach their ends.
All inputs are finite; a program needn't handle non-finite values.
Results may differ from the reference program's by a relative error of at most 0.0001.
Values sent between devices are 32-bit elements; how exact they have to be, the bound alone decides.
A program may use at most 64 MiB of HBM per device.

```python
import jax
import jax.numpy as jnp
from jax import lax

F = 24
NX = 32
NY = 16
NZ = 512


def level_of(rng, shape, shards, low, top_value):
    gain, own = 1.0, jax.random.fold_in(rng, 6)
    for dim, parts in shards:
        heights = jnp.exp(jax.random.uniform(jax.random.fold_in(own, dim), (parts,), jnp.float32, low / len(shards), top_value / len(shards)))
        gain = gain * jnp.repeat(heights, shape[dim] // parts).reshape([-1 if axis == dim else 1 for axis in range(len(shape))])
    return gain


def scatter_about(own_key, shape, width, most, pieces=(), held_as=jnp.bfloat16):
    values = width * jax.random.normal(own_key, shape, jnp.float32)
    if pieces:
        values = values * level_of(own_key, shape, pieces, -0.22, 0.18)
    return jnp.clip(values, -most, most).astype(held_as)


def setup_inputs(seed: int = 0) -> dict:
    keys = jax.random.split(jax.random.key(seed), 6)
    fields_now = scatter_about(keys[0], (F, NX, NY, NZ), 1.0, 6.0, ((1, 4), (2, 2), (3, 4)), jnp.float32)
    parent = scatter_about(keys[1], (F, NX, NY, NZ), 1.0, 6.0, ((1, 4), (2, 2), (3, 4)), jnp.float32)
    advect = scatter_about(keys[2], (3, F, F), (3 * F) ** -0.5, 0.75, (), jnp.float32)
    diffuse = scatter_about(keys[3], (3, F, F), (27 * F) ** -0.5, 0.25, (), jnp.float32)
    box_shift = jax.random.randint(keys[4], (3,), 1, 5).astype(jnp.int32)
    return {"fields_now": fields_now, "parent": parent, "advect": advect, "diffuse": diffuse, "box_shift": box_shift}


dissipation = 1.0
half_step = 0.125


def line_terms(padded_line, axis):
    length = padded_line.shape[axis] - 6

    def take_at(offset):
        return lax.slice_in_dim(padded_line, 3 + offset, 3 + offset + length, axis=axis)

    first_diff = (take_at(-2) - 8.0 * take_at(-1) + 8.0 * take_at(1) - take_at(2)) / 12.0
    second_diff = (-take_at(-2) + 16.0 * take_at(-1) - 30.0 * take_at(0) + 16.0 * take_at(1) - take_at(2)) / 12.0
    sixth_diff = (take_at(-3) - 6.0 * take_at(-2) + 15.0 * take_at(-1) - 20.0 * take_at(0)
                  + 15.0 * take_at(1) - 6.0 * take_at(2) + take_at(3))
    return first_diff, second_diff, sixth_diff


def mix_fields(matrix, field):
    flat = field.reshape(field.shape[0], -1)
    return jnp.dot(matrix, flat, precision=lax.Precision.HIGHEST,
                   preferred_element_type=jnp.float32).reshape(field.shape)


def center_crop(padded, axis):
    window = [slice(None)] * 4
    for other in (1, 2, 3):
        if other != axis:
            window[other] = slice(3, padded.shape[other] - 3)
    return padded[tuple(window)]


def axis_terms(line, axis, advect, diffuse):
    first_diff, second_diff, sixth_diff = line_terms(line, axis)
    coupled = mix_fields(advect[axis - 1], first_diff) + mix_fields(diffuse[axis - 1], second_diff)
    return coupled, sixth_diff


def whole_terms(padded, advect, diffuse):
    linear, smooth = axis_terms(center_crop(padded, 1), 1, advect, diffuse)
    for axis in (2, 3):
        coupled, sixth_diff = axis_terms(center_crop(padded, axis), axis, advect, diffuse)
        linear = linear + coupled
        smooth = smooth + sixth_diff
    return linear, smooth


def finish(new_box, linear, smooth):
    lapse_factor = 1.0 + 0.25 * jnp.tanh(new_box[0])
    section_slope = lapse_factor * linear + (dissipation / 64.0) * smooth
    section_value = new_box + half_step * section_slope
    return section_slope, section_value


def reference(fields_now, parent, advect, diffuse, box_shift):
    room = jnp.pad(fields_now, ((0, 0), (0, 4), (0, 4), (0, 4)))
    anchor = jnp.zeros((), jnp.int32)
    moved_cells = lax.dynamic_slice(room, (anchor, box_shift[0], box_shift[1], box_shift[2]), fields_now.shape)
    keep_mask = None
    for axis in (1, 2, 3):
        shape_one = [1, 1, 1, 1]
        shape_one[axis] = fields_now.shape[axis]
        position = lax.broadcasted_iota(jnp.int32, tuple(shape_one), axis)
        inside = position + box_shift[axis - 1] < fields_now.shape[axis]
        keep_mask = inside if keep_mask is None else keep_mask & inside
    new_box = jnp.where(keep_mask, moved_cells, parent)
    padded = jnp.pad(new_box, ((0, 0), (3, 3), (3, 3), (3, 3)))
    linear, smooth = whole_terms(padded, advect, diffuse)
    return finish(new_box, linear, smooth)
```

```python
import functools

import jax
import jax.numpy as jnp
import numpy as np
from jax import lax
from jax.experimental import pallas as pl
from jax.experimental.pallas import tpu as pltpu
from jax.sharding import PartitionSpec as P

MESH = pl.DeviceIdType.MESH
W = 4
H = 3
SLOT = 8
ROWS = 8
AXES = ("gx", "gy", "gz")
KINDS = ("x", "y", "xy")
MESSAGES = {"x": 12, "y": 12, "xy": 15}
FIRST = {-2: 1, -1: -8, 1: 8, 2: -1}
SECOND = {-2: -1, -1: 16, 0: -30, 1: 16, 2: -1}
SIXTH = {-3: 1, -2: -6, -1: 15, 0: -20, 1: 15, 2: -6, 3: 1}
BLOCKS = [(None, 0)] + [(a, o) for a in range(3) for o in (-3, -2, -1, 1, 2, 3)]
SIDES = [(a, sign) for a in range(2) for sign in (-1, 1)]
f32, bf16 = jnp.float32, jnp.bfloat16


def up_to(n, m):
    return -(-n // m) * m


def block_columns(block, fields):
    cols = np.zeros((16, 2 * fields), np.float32)
    for c in range(fields // ROWS):
        for h in range(2):
            for r in range(ROWS):
                n = (c * 2 + h) * ROWS + r
                cols[7, n] = c * ROWS + r
                cols[8, n] = 1 - h
    if block is None:
        return cols
    axis, o = block
    for a in range(3):
        if axis is None or a == axis:
            cols[a] = FIRST.get(o, 0)
            cols[3 + a] = SECOND.get(o, 0)
            cols[6] += SIXTH[o]
    return cols


def coefficients(fields):
    groups = [BLOCKS]
    for a, sign in SIDES:
        near = [(a, sign * o) for o in range(1, H + 1)]
        groups += [near[d:] + [None] * d for d in range(H)]
    out = []
    for g in groups:
        cols = np.concatenate([block_columns(b, fields) for b in g], axis=1)
        out.append(np.pad(cols, ((0, 0), (0, up_to(cols.shape[1], 256) - cols.shape[1]))))
    return np.concatenate(out, axis=1)


def scratch(dims):
    F, NX, NY, NZ = dims
    chunks = F // ROWS
    groups = NX * NY * SLOT // NZ
    tile = (ROWS, NZ)
    out = dict(
        shift=pltpu.SMEM((3,), jnp.int32),
        own=pltpu.VMEM((NX, NY, F, NZ), f32),
        par=pltpu.VMEM((NX, NY, F, NZ), f32),
        advect=pltpu.VMEM((3, F, F), f32),
        diffuse=pltpu.VMEM((3, F, F), f32),
        coef=pltpu.VMEM(coefficients(F).shape, f32),
        w_early=pltpu.VMEM((3 * F, len(BLOCKS) * 2 * F), bf16),
        w_late=pltpu.VMEM((len(SIDES), 7 * F, H * 2 * F), bf16),
        box=pltpu.VMEM((NX + 2 * H, NY + 2 * H, F, NZ), f32),
        ub=pltpu.VMEM((NX + 2 * H, NY + 2 * H, chunks, 2 * ROWS, NZ), bf16),
        acc=pltpu.VMEM((NX, NY, 2 * F, NZ), f32),
        rim=pltpu.VMEM((chunks, groups) + tile, f32),
        rim_up=pltpu.VMEM((chunks, groups) + tile, f32),
        rim_low=pltpu.VMEM((chunks, groups) + tile, f32),
        epk=pltpu.VMEM((chunks, 3) + tile, f32),
        ein=pltpu.VMEM((chunks, 4) + tile, f32),
    )
    for c in range(chunks):
        kind = KINDS[c % 3]
        if "x" in kind:
            out[f"rawx{c}"] = pltpu.VMEM((W, NY) + tile, f32)
        if "y" in kind:
            out[f"rawy{c}"] = pltpu.VMEM((NX, W) + tile, f32)
        ext = (W if "x" in kind else 0, W if "y" in kind else 0)
        out[f"zs{c}"] = pltpu.VMEM((NX + ext[0], NY + ext[1]) + tile, f32)
        if kind == "xy":
            out[f"ce{c}"] = pltpu.VMEM((W, W) + tile, f32)
        else:
            size = (NX, W) if kind == "x" else (W, NY)
            out[f"fw{c}"] = pltpu.VMEM(size + tile, f32)
            out[f"te{c}"] = pltpu.VMEM(size + tile, f32)
    n = sum(MESSAGES[KINDS[c % 3]] for c in range(chunks))
    out["send_sem"] = pltpu.SemaphoreType.DMA((n,))
    out["recv_sem"] = pltpu.SemaphoreType.DMA((n,))
    out["load_sem"] = pltpu.SemaphoreType.DMA((6,))
    return out


def kernel(
    dims, shift_hbm, now_hbm, parent_hbm, advect_hbm, diffuse_hbm, coef_hbm, slope_ref, value_ref, *refs
):
    F, NX, NY, NZ = dims
    chunks = F // ROWS
    cells = NX * NY
    s = dict(zip(scratch(dims), refs))
    own, par, box, ub, acc = s["own"], s["par"], s["box"], s["ub"], s["acc"]
    epk, ein, rim, rim_up, rim_low = s["epk"], s["ein"], s["rim"], s["rim_up"], s["rim_low"]
    slots = NZ // SLOT
    groups = cells // slots
    me = {a: lax.axis_index(a) for a in AXES}
    size = {a: lax.axis_size(a) for a in AXES}
    below = {a: me[a] > 0 for a in AXES}
    above = {a: me[a] < size[a] - 1 for a in AXES}
    sems = iter(range(1000))
    kinds = [KINDS[c % 3] for c in range(chunks)]
    rows = [pl.ds(c * ROWS, ROWS) for c in range(chunks)]

    def load_cell(src, dst, n, k):
        return pltpu.make_async_copy(src.at[:, k], dst.at[k // NY, k % NY], s["load_sem"].at[n])

    def load_cells(src, dst, n):
        def step(k, _):
            load_cell(src, dst, n, k).start()
            return 0

        lax.fori_loop(0, cells, step, 0, unroll=8)

    singles = [
        pltpu.make_async_copy(src, dst, s["load_sem"].at[2 + n])
        for n, (src, dst) in enumerate((
            (shift_hbm, s["shift"]), (advect_hbm, s["advect"]),
            (diffuse_hbm, s["diffuse"]), (coef_hbm, s["coef"]),
        ))
    ]
    singles[0].start()
    load_cells(now_hbm, own, 0)

    class Copy:
        def __init__(self, src, dst, to, parts=None):
            n = next(sems)
            self.to = to
            self.sem = dict(send_sem=s["send_sem"].at[n], recv_sem=s["recv_sem"].at[n])
            self.parts = parts
            self.copy = self.make(src, dst)
            self.sends = self.gets = None
            for a, by in to.items():
                sends = below[a] if by < 0 else above[a]
                gets = above[a] if by < 0 else below[a]
                self.sends = sends if self.sends is None else self.sends & sends
                self.gets = gets if self.gets is None else self.gets & gets

        def make(self, src, dst):
            return pltpu.make_async_remote_copy(
                src_ref=src, dst_ref=dst, device_id={a: me[a] + by for a, by in self.to.items()},
                device_id_type=MESH, **self.sem,
            )

        def start(self):
            pl.when(self.sends)(self.copy.start)

        def start_part(self, i):
            pl.when(self.sends)(self.make(*self.parts(i)).start)

        def arrived(self):
            pl.when(self.gets)(self.copy.wait_recv)

        def sent(self):
            pl.when(self.sends)(self.copy.wait_send)

    everything = []

    def message(src, dst, to, parts=None):
        everything.append(Copy(src, dst, to, parts))
        return everything[-1]

    DX, DY, DZ = {"gx": -1}, {"gy": -1}, {"gz": -1}
    UX, UY, UZ = {"gx": 1}, {"gy": 1}, {"gz": 1}
    lowx, lowy = pl.ds(0, W), pl.ds(0, W)
    raw, edge, diag, forward, corner = {}, {}, {}, {}, {}
    for c, kind in enumerate(kinds):
        if kind == "x":
            def cell(i, half, c=c):
                x, y = i // W, i % W + half * (NY // 2)
                return now_hbm.at[rows[c], x * NY + y], s[f"rawx{c}"].at[x, y]

            halves = [s[f"rawx{c}"].at[:, pl.ds(h * (NY // 2), NY // 2)] for h in range(2)]
            raw[c] = [message(r, r, DX, functools.partial(cell, half=h)) for h, r in enumerate(halves)]
            diag[c] = [message(epk.at[c, 0], ein.at[c, 2], DX | DZ)]
            forward[c] = message(s[f"fw{c}"], s[f"te{c}"], DY)
        elif kind == "y":
            def cell(i, half, c=c):
                x, y = i // W + half * (NX // 2), i % W
                return now_hbm.at[rows[c], x * NY + y], s[f"rawy{c}"].at[x, y]

            halves = [s[f"rawy{c}"].at[pl.ds(h * (NX // 2), NX // 2)] for h in range(2)]
            raw[c] = [message(r, r, DY, functools.partial(cell, half=h)) for h, r in enumerate(halves)]
            diag[c] = [message(epk.at[c, 0], ein.at[c, 2], DY | DZ)]
            forward[c] = message(s[f"fw{c}"], s[f"te{c}"], DX)
        else:
            raw[c] = [
                message(own.at[lowx, :, rows[c]], s[f"rawx{c}"], DX),
                message(own.at[:, lowy, rows[c]], s[f"rawy{c}"], DY),
            ]
            diag[c] = [
                message(epk.at[c, 0], ein.at[c, 2], DX | DZ), message(epk.at[c, 2], ein.at[c, 3], DY | DZ),
            ]
            near, far = pl.ds(0, W // 2), pl.ds(W // 2, W // 2)
            zs, ce = s[f"zs{c}"], s[f"ce{c}"]
            corner[c] = [
                message(zs.at[far, pl.ds(NY, W)], ce.at[far], DX),
                message(zs.at[pl.ds(NX, W // 2), lowy], ce.at[near], DY),
            ]
        edge[c] = message(epk.at[c, pl.ds(0, 2)], ein.at[c, pl.ds(0, 2)], DZ)

    inside = {side: [] for side in SIDES}

    def halo(c, a, by, lo, hi):
        n = (NX, NY)[a]
        src = pl.ds(H, H) if by < 0 else pl.ds(n, H)
        dst = pl.ds(n + H, H) if by < 0 else pl.ds(0, H)
        span = pl.ds(H + lo, hi - lo)
        to = {AXES[a]: by}
        if a == 0:
            m = message(box.at[src, span, rows[c]], box.at[dst, span, rows[c]], to)
        else:
            m = message(box.at[span, src, rows[c]], box.at[span, dst, rows[c]], to)
        inside[(a, -by)].append(m)
        return m

    early_halo, late_halo, rims = {}, {}, {}
    hx, hy = NX // 2, NY // 2
    for c, kind in enumerate(kinds):
        if kind == "x":
            early_halo[c] = [halo(c, 1, -1, 0, NX), halo(c, 0, 1, 0, hy)]
            late_halo[c] = [halo(c, 0, -1, 0, NY), halo(c, 0, 1, hy, NY), halo(c, 1, 1, 0, NX)]
        elif kind == "y":
            early_halo[c] = [halo(c, 0, -1, 0, NY), halo(c, 1, 1, 0, hx)]
            late_halo[c] = [halo(c, 1, -1, 0, NX), halo(c, 1, 1, hx, NX), halo(c, 0, 1, 0, NY)]
        else:
            early_halo[c] = [halo(c, 0, -1, 0, NY), halo(c, 1, -1, 0, NX), halo(c, 0, 1, 0, hy), halo(c, 1, 1, 0, hx)]
            late_halo[c] = [halo(c, 0, 1, hy, NY), halo(c, 1, 1, hx, NX)]
        rims[c] = [message(rim.at[c], rim_up.at[c], DZ), message(rim.at[c], rim_low.at[c], UZ)]

    barrier = pltpu.get_barrier_semaphore()
    count = 0
    for to in (DX, UX, DY, UY, DZ, UZ, UX | UZ, UY | UZ):
        cond = back = None
        for a, by in to.items():
            one, two = (below[a], above[a]) if by < 0 else (above[a], below[a])
            cond = one if cond is None else cond & one
            back = two if back is None else back & two

        @pl.when(cond)
        def _(to=to):
            pl.semaphore_signal(
                barrier, inc=1, device_id={a: me[a] + by for a, by in to.items()}, device_id_type=MESH
            )
        count = count + jnp.where(back, 1, 0)

    load_cells(parent_hbm, par, 1)
    for load in singles[1:]:
        load.start()
    pl.semaphore_wait(barrier, count)

    def send_raw(i, _, half):
        for c, kind in enumerate(kinds):
            if kind != "xy":
                raw[c][half].start_part(i)
        return 0

    for half in range(2):
        lax.fori_loop(0, W * W, functools.partial(send_raw, half=half), 0, unroll=4)

    lane = lax.broadcasted_iota(jnp.int32, (ROWS, NZ), 1)
    thin = lane // W
    wide = ((lane + SLOT // 2) % NZ) // SLOT
    blank = jnp.zeros((ROWS, NZ), f32)

    def pack(c, n, along, q):
        def step(i, packed):
            for j in range(NY if along == "x" else NX):
                x, y = (q * W + i, j) if along == "x" else (j, q * W + i)
                slot = i * (NY if along == "x" else NX) + j
                packed = jnp.where(thin == slot, pltpu.roll(own[x, y, rows[c]], W * slot, 1), packed)
            return packed

        epk[c, n] = lax.fori_loop(0, W, step, blank)

    pltpu.make_async_copy(par, own, s["load_sem"].at[0]).wait()
    for c, kind in enumerate(kinds):
        along = kind[0]
        for q in range(2):
            pack(c, q, along, q)
        if kind == "xy":
            pack(c, 2, "y", 0)
        for d in diag[c]:
            d.start()
        edge[c].start()
    for c, kind in enumerate(kinds):
        if kind == "xy":
            for r in raw[c]:
                r.start()

    zero16 = jnp.zeros((2 * ROWS, NZ), bf16)

    def clear(i, _):
        for o in (*range(H), *range(H)):
            pass
        for c in range(chunks):
            for o in range(H):
                ub[o, i + H, c] = zero16
                ub[NX + H + o, i + H, c] = zero16
                ub[i + H, o, c] = zero16
                ub[i + H, NY + H + o, c] = zero16
        return 0

    lax.fori_loop(0, NX, clear, 0)

    for load in singles:
        load.wait()
    move = [s["shift"][d] for d in range(3)]
    sz = move[2]

    def split16(u):
        low = u - u.astype(bf16).astype(f32)
        return jnp.concatenate([u, low], axis=0).astype(bf16)

    def weights():
        mats = []
        for m in (s["advect"], s["diffuse"]):
            for a in range(3):
                one = m[a]
                high = one.astype(bf16).astype(f32)
                mid = (one - high).astype(bf16).astype(f32)
                mats.append(jnp.concatenate([high, mid, one - high - mid], axis=0).astype(bf16))

        def columns(at, width, ks):
            table = s["coef"][:, at:at + width]
            hit = lax.broadcasted_iota(jnp.int32, (F, width), 0).astype(f32) == table[7:8]
            smooth = jnp.where(hit, table[6:7], 0.0)
            if not ks:
                return smooth
            total = None
            for k in ks:
                spread = jnp.where(hit, table[k:k + 1], 0.0).astype(bf16)
                part = jnp.dot(mats[k], spread, preferred_element_type=f32)
                total = part if total is None else total + part
            w = total[:F] + total[F:2 * F] + total[2 * F:]
            high = w.astype(bf16).astype(f32)
            return jnp.concatenate([high, (w - high) * table[8:9], smooth], axis=0)

        k_early = len(BLOCKS) * 2 * F
        for at in range(0, up_to(k_early, 256), 256):
            n = min(256, k_early - at)
            s["w_early"][:, at:at + n] = columns(at, 256, range(6))[:, :n].astype(bf16)
        at = up_to(k_early, 256)
        k_late = H * 2 * F
        step = up_to(k_late, 256)
        for n, (a, sign) in enumerate(SIDES):
            parts = [columns(at + d * step, step, (a, 3 + a) if d < 2 else ()) for d in range(H)]
            s["w_late"][n] = jnp.concatenate(parts, axis=0)[:, :k_late].astype(bf16)
            at += H * step

    weights()

    def z_row(row, packed, slot):
        tail = pltpu.roll(packed, lax.rem(2 * NZ - W * slot - sz, NZ), 1)
        return jnp.where(lane >= NZ - sz, tail, pltpu.roll(row, NZ - sz, 1))

    def z_own(c):
        kind = kinds[c]

        def step(x, _):
            for y in range(NY):
                q, slot = (x // W, x % W * NY + y) if "x" in kind else (y // W, y % W * NX + x)
                s[f"zs{c}"][x, y] = z_row(own[x, y, rows[c]], ein[c, q], slot)
            return 0

        lax.fori_loop(0, NX, step, 0)

    def z_ext_x(c, lo, hi):
        def step(x, _):
            for y in range(lo, hi):
                s[f"zs{c}"][NX + x, y] = z_row(s[f"rawx{c}"][x, y], ein[c, 2], x * NY + y)
            return 0

        lax.fori_loop(0, W, step, 0)

    def z_ext_y(c, lo, hi):
        n = 3 if kinds[c] == "xy" else 2

        def step(x, _):
            for y in range(W):
                s[f"zs{c}"][x, NY + y] = z_row(s[f"rawy{c}"][x, y], ein[c, n], y * NX + x)
            return 0

        lax.fori_loop(lo, hi, step, 0)

    def make_forward(c):
        zs, fw = s[f"zs{c}"], s[f"fw{c}"]

        def step(i, _):
            for j in range(W):
                if kinds[c] == "x":
                    fw[i, j] = zs[i + move[0], j]
                else:
                    fw[j, i] = zs[j, i + move[1]]
            return 0

        lax.fori_loop(0, NX if kinds[c] == "x" else NY, step, 0)

    in_z = me["gz"] * NZ + lane + sz < size["gz"] * NZ

    def renew(c, xs, ys, late):
        kind, zs = kinds[c], s[f"zs{c}"]

        def step(x, _):
            in_x = me["gx"] * NX + x + move[0] < size["gx"] * NX
            for y in range(*ys):
                in_y = me["gy"] * NY + y + move[1] < size["gy"] * NY
                X, Y = x + move[0], y + move[1]
                if not late:
                    row = zs[X, Y]
                elif kind == "x":
                    row = jnp.where(Y < NY, zs[X, jnp.minimum(Y, NY - 1)], s[f"te{c}"][x, jnp.maximum(Y - NY, 0)])
                elif kind == "y":
                    row = jnp.where(X < NX, zs[jnp.minimum(X, NX - 1), Y], s[f"te{c}"][jnp.maximum(X - NX, 0), y])
                else:
                    row = jnp.where(
                        (X < NX) | (Y < NY), zs[X, Y],
                        s[f"ce{c}"][jnp.maximum(X - NX, 0), jnp.maximum(Y - NY, 0)],
                    )
                row = jnp.where(in_z & (in_x & in_y), row, par[x, y, rows[c]])
                box[x + H, y + H, rows[c]] = row
                ub[x + H, y + H, c] = split16(row)
            return 0

        lax.fori_loop(*xs, step, 0)

    def renew_early(c):
        if kinds[c] == "x":
            renew(c, (0, NX), (0, hy), False)
        elif kinds[c] == "y":
            renew(c, (0, hx), (0, NY), False)
        else:
            renew(c, (0, hx), (0, NY), False)
            renew(c, (hx, NX), (0, hy), False)
        for h in early_halo[c]:
            h.start()

    def renew_late(c):
        if kinds[c] == "x":
            renew(c, (0, NX), (hy, NY), True)
        elif kinds[c] == "y":
            renew(c, (hx, NX), (0, NY), True)
        else:
            renew(c, (hx, NX), (hy, NY), True)
        for h in late_halo[c]:
            h.start()

        def step(g, _):
            packed = blank
            for j in range(slots):
                x, y = g * (slots // NY) + j // NY, j % NY
                packed = jnp.where(wide == j, pltpu.roll(box[x + H, y + H, rows[c]], SLOT * j, 1), packed)
            rim[c, g] = packed
            return 0

        lax.fori_loop(0, groups, step, 0)
        for r in rims[c]:
            r.start()

    one_way = [c for c in range(chunks) if kinds[c] != "xy"]
    both = [c for c in range(chunks) if kinds[c] == "xy"]
    for c in one_way:
        edge[c].arrived()
        z_own(c)
    for c in one_way:
        diag[c][0].arrived()
        raw[c][0].arrived()
        if kinds[c] == "x":
            z_ext_x(c, 0, hy)
        else:
            z_ext_y(c, 0, hx)
        make_forward(c)
        forward[c].start()
    for c in both:
        edge[c].arrived()
        z_own(c)
    for c in one_way:
        raw[c][1].arrived()
        if kinds[c] == "x":
            z_ext_x(c, hy, NY)
        else:
            z_ext_y(c, hx, NX)
    for c in both:
        for d in diag[c]:
            d.arrived()
        raw[c][0].arrived()
        z_ext_x(c, 0, NY)
        raw[c][1].arrived()
        z_ext_y(c, 0, NX)
        for k in corner[c]:
            k.start()
    pltpu.make_async_copy(own, par, s["load_sem"].at[1]).wait()
    for c in (*one_way, *both):
        renew_early(c)
    for c in one_way:
        forward[c].arrived()
        renew_late(c)
    for c in both:
        for k in corner[c]:
            k.arrived()
        renew_late(c)

    for c in range(chunks):
        for r in rims[c]:
            r.arrived()

    def early(i, _):
        per = 4
        x, y0 = i // (NY // per), i % (NY // per) * per
        g = x * NY // slots
        j0 = x * NY % slots + y0
        ends_all = [
            jnp.where(
                lane % SLOT < SLOT // 2,
                jnp.where(above["gz"], rim_up[c, g], 0.0), jnp.where(below["gz"], rim_low[c, g], 0.0),
            )
            for c in range(chunks)
        ]
        for y1 in range(0, per, 2):
            sides = []
            for y2 in range(2):
                y = y0 + y1 + y2
                z_at = {o: [] for o in range(-H, H + 1) if o}
                for c in range(chunks):
                    u = box[x + H, y + H, rows[c]]
                    ends = pltpu.roll(ends_all[c], lax.rem(NZ - SLOT * (j0 + y1 + y2), NZ), 1)
                    for o in range(1, H + 1):
                        z_at[o].append(split16(pltpu.roll(jnp.where(lane < o, ends, u), NZ - o, 1)))
                        z_at[-o].append(split16(pltpu.roll(jnp.where(lane >= NZ - o, ends, u), o, 1)))
                parts = []
                for a, o in BLOCKS:
                    if a == 2:
                        parts += z_at[o]
                    else:
                        dx, dy = (o, 0) if a == 0 else (0, o)
                        parts += [ub[x + H + dx, y + H + dy, c] for c in range(chunks)]
                sides.append(jnp.concatenate(parts, axis=0))
            out = jnp.dot(s["w_early"][...], jnp.concatenate(sides, axis=1), preferred_element_type=f32)
            for y2 in range(2):
                part = out[:, y2 * NZ:(y2 + 1) * NZ]
                acc[x, y0 + y1 + y2, pl.ds(0, F)] = part[:F] + part[F:2 * F]
                acc[x, y0 + y1 + y2, pl.ds(F, F)] = part[2 * F:]
        return 0

    lax.fori_loop(0, cells // 4, early, 0)

    def late(n):
        a, sign = SIDES[n]
        length = (NX, NY)[a]
        across = (NY, NX)[a]

        def step(p, _):
            sides = []
            for q in range(2):
                parts = []
                for h in range(1, H + 1):
                    at = H + (length - 1 + h if sign > 0 else -h)
                    for c in range(chunks):
                        where = (at, H + 2 * p + q) if a == 0 else (H + 2 * p + q, at)
                        parts.append(split16(box[(*where, rows[c])]))
                sides.append(jnp.concatenate(parts, axis=0))
            out = jnp.dot(s["w_late"][n], jnp.concatenate(sides, axis=1), preferred_element_type=f32)
            for q in range(2):
                part = out[:, q * NZ:(q + 1) * NZ]
                for d in range(H):
                    at = length - 1 - d if sign > 0 else d
                    where = (at, 2 * p + q) if a == 0 else (2 * p + q, at)
                    if d < 2:
                        own_part = part[3 * F * d:3 * F * (d + 1)]
                        acc[(*where, pl.ds(0, F))] += own_part[:F] + own_part[F:2 * F]
                        acc[(*where, pl.ds(F, F))] += own_part[2 * F:]
                    else:
                        acc[(*where, pl.ds(F, F))] += part[6 * F:]
            return 0

        lax.fori_loop(0, across // 2, step, 0)

    for sign in (-1, 1):
        for a in range(2):
            n = SIDES.index((a, sign))
            for m in inside[SIDES[n]]:
                m.arrived()
            pl.when((above if sign > 0 else below)[AXES[a]])(functools.partial(late, n))

    def finish(x, _):
        for y in range(NY):
            u = box[x + H, y + H]
            lapse = (1.0 + 0.25 * jnp.tanh(u[0:1])) * (1.0 / 12.0)
            slope = lapse * acc[x, y, pl.ds(0, F)] + acc[x, y, pl.ds(F, F)] * (1.0 / 64.0)
            slope_ref[x * NY + y] = slope
            value_ref[x * NY + y] = u + 0.125 * slope
        return 0

    lax.fori_loop(0, NX, finish, 0)

    for m in everything:
        m.sent()


def put_out(slope_in, value_in, slope_hbm, value_hbm, sem):
    cells = slope_in.shape[0]

    def step(k, _):
        pltpu.make_async_copy(slope_in.at[k], slope_hbm.at[:, k], sem.at[0]).start()
        pltpu.make_async_copy(value_in.at[k], value_hbm.at[:, k], sem.at[1]).start()
        return 0

    lax.fori_loop(0, cells, step, 0, unroll=8)
    pltpu.make_async_copy(slope_in, value_in, sem.at[0]).wait()
    pltpu.make_async_copy(slope_in, value_in, sem.at[1]).wait()


def local(fields_now, parent, advect, diffuse, box_shift):
    dims = fields_now.shape
    F, NX, NY, NZ = dims
    flat = (F, NX * NY, NZ)
    by_cell = (NX * NY, F, NZ)
    vmem = pl.BlockSpec(memory_space=pltpu.VMEM)
    hbm = pl.BlockSpec(memory_space=pltpu.HBM)
    operands = [
        pltpu.with_memory_space_constraint(x, pltpu.HBM)
        for x in (box_shift, fields_now.reshape(flat), parent.reshape(flat), advect, diffuse, jnp.asarray(coefficients(F)))
    ]
    results = pl.pallas_call(
        functools.partial(kernel, dims),
        out_shape=[pltpu.VMEM(by_cell, f32)] * 2,
        in_specs=[hbm] * 6,
        out_specs=[vmem] * 2,
        scratch_shapes=list(scratch(dims).values()),
        compiler_params=pltpu.CompilerParams(
            collective_id=0, has_side_effects=True, vmem_limit_bytes=VMEM_BYTES
        ),
    )(*operands)
    slope, value = pl.pallas_call(
        put_out,
        out_shape=[jax.ShapeDtypeStruct(flat, f32)] * 2,
        in_specs=[vmem] * 2,
        out_specs=[hbm] * 2,
        scratch_shapes=[pltpu.SemaphoreType.DMA((2,))],
        compiler_params=pltpu.CompilerParams(vmem_limit_bytes=VMEM_BYTES),
    )(*results)
    return slope.reshape(dims), value.reshape(dims)


VMEM_BYTES = 40 * 2**20


def solution(mesh):
    return jax.shard_map(
        local,
        mesh=mesh,
        in_specs=(P(None, "gx", "gy", "gz"), P(None, "gx", "gy", "gz"), P(), P(), P()),
        out_specs=(P(None, "gx", "gy", "gz"), P(None, "gx", "gy", "gz")),
        check_vma=False,
    )
```

```python
import functools

import jax
import jax.numpy as jnp
import numpy as np
from jax import lax
from jax.experimental import pallas as pl
from jax.experimental.pallas import tpu as pltpu
from jax.sharding import PartitionSpec as P

MESH = pl.DeviceIdType.MESH
W = 4
H = 3
SLOT = 8
ROWS = 8
AXES = ("gx", "gy", "gz")
KINDS = ("x", "y", "xy")
ARRIVALS = {"x": 5, "y": 5, "xy": 7}
ROUTES = 8
FIRST = {-2: 1, -1: -8, 1: 8, 2: -1}
SECOND = {-2: -1, -1: 16, 0: -30, 1: 16, 2: -1}
SIXTH = {-3: 1, -2: -6, -1: 15, 0: -20, 1: 15, 2: -6, 3: 1}
BLOCKS = [(None, 0)] + [(a, o) for a in range(2) for o in (-3, -2, -1, 1, 2, 3)]
ALONG = [(2, "first"), (2, "second")]
SIDES = [(a, sign) for a in range(2) for sign in (-1, 1)]
f32, bf16 = jnp.float32, jnp.bfloat16


def up_to(n, m):
    return -(-n // m) * m


def block_columns(block, fields):
    cols = np.zeros((16, 2 * fields), np.float32)
    for c in range(fields // ROWS):
        for h in range(2):
            for r in range(ROWS):
                n = (c * 2 + h) * ROWS + r
                cols[7, n] = c * ROWS + r
                cols[8, n] = 1 - h
    if block is None:
        return cols
    axis, o = block
    if o in ("first", "second"):
        cols[axis + (3 if o == "second" else 0)] = 1
        return cols
    for a in range(3):
        if axis is None or a == axis:
            cols[a] = FIRST.get(o, 0)
            cols[3 + a] = SECOND.get(o, 0)
            cols[6] += SIXTH[o]
    return cols


def coefficients(fields):
    groups = [BLOCKS, ALONG]
    for a, sign in SIDES:
        near = [(a, sign * o) for o in range(1, H + 1)]
        groups += [near[d:] + [None] * d for d in range(H)]
    out = []
    for g in groups:
        cols = np.concatenate([block_columns(b, fields) for b in g], axis=1)
        out.append(np.pad(cols, ((0, 0), (0, up_to(cols.shape[1], 256) - cols.shape[1]))))
    return np.concatenate(out, axis=1)


def scratch(dims):
    F, NX, NY, NZ = dims
    chunks = F // ROWS
    groups = NX * NY * SLOT // NZ
    tile = (ROWS, NZ)
    out = dict(
        shift=pltpu.SMEM((3,), jnp.int32),
        own=pltpu.VMEM((NX, NY, F, NZ), f32),
        par=pltpu.VMEM((NX, NY, F, NZ), f32),
        advect=pltpu.VMEM((3, F, F), f32),
        diffuse=pltpu.VMEM((3, F, F), f32),
        coef=pltpu.VMEM(coefficients(F).shape, f32),
        w_early=pltpu.VMEM((3 * F, len(BLOCKS) * 2 * F), bf16),
        w_along=pltpu.VMEM((2 * F, len(ALONG) * 2 * F), bf16),
        w_late=pltpu.VMEM((len(SIDES), 7 * F, H * 2 * F), bf16),
        box=pltpu.VMEM((NX + 2 * H, NY + 2 * H, F, NZ), f32),
        ub=pltpu.VMEM((NX + 2 * H, NY + 2 * H, chunks, 2 * ROWS, NZ), bf16),
        acc=pltpu.VMEM((NX, NY, 2 * F, NZ), f32),
        rim=pltpu.VMEM((chunks, groups) + tile, f32),
        rim_up=pltpu.VMEM((chunks, groups) + tile, f32),
        rim_low=pltpu.VMEM((chunks, groups) + tile, f32),
        epk=pltpu.VMEM((chunks, 3) + tile, f32),
        ein=pltpu.VMEM((chunks, 4) + tile, f32),
    )
    for c in range(chunks):
        kind = KINDS[c % 3]
        if "x" in kind:
            out[f"rawx{c}"] = pltpu.VMEM((W, NY) + tile, f32)
        if "y" in kind:
            out[f"rawy{c}"] = pltpu.VMEM((NX, W) + tile, f32)
        ext = (W if "x" in kind else 0, W if "y" in kind else 0)
        out[f"zs{c}"] = pltpu.VMEM((NX + ext[0], NY + ext[1]) + tile, f32)
        if kind == "xy":
            out[f"ce{c}"] = pltpu.VMEM((W, W) + tile, f32)
        else:
            size = (NX, W) if kind == "x" else (W, NY)
            out[f"fw{c}"] = pltpu.VMEM(size + tile, f32)
            out[f"te{c}"] = pltpu.VMEM(size + tile, f32)
    out["count"] = pltpu.VMEM((chunks * 8 * NX * NY,) + tile, f32)
    n = sum(ARRIVALS[KINDS[c % 3]] for c in range(chunks)) + len(SIDES) + 2
    out["send_sem"] = pltpu.SemaphoreType.DMA((ROUTES,))
    out["recv_sem"] = pltpu.SemaphoreType.DMA((n,))
    out["load_sem"] = pltpu.SemaphoreType.DMA((6,))
    return out


def kernel(
    dims, shift_hbm, now_hbm, parent_hbm, advect_hbm, diffuse_hbm, coef_hbm, slope_ref, value_ref, *refs
):
    F, NX, NY, NZ = dims
    chunks = F // ROWS
    cells = NX * NY
    s = dict(zip(scratch(dims), refs))
    own, par, box, ub, acc = s["own"], s["par"], s["box"], s["ub"], s["acc"]
    epk, ein, rim, rim_up, rim_low = s["epk"], s["ein"], s["rim"], s["rim_up"], s["rim_low"]
    slots = NZ // SLOT
    groups = cells // slots
    me = {a: lax.axis_index(a) for a in AXES}
    size = {a: lax.axis_size(a) for a in AXES}
    below = {a: me[a] > 0 for a in AXES}
    above = {a: me[a] < size[a] - 1 for a in AXES}
    sems = iter(range(1000))
    kinds = [KINDS[c % 3] for c in range(chunks)]
    rows = [pl.ds(c * ROWS, ROWS) for c in range(chunks)]

    def load_cells(src, dst, n):
        def step(x, _):
            for y in range(NY):
                pltpu.make_async_copy(src.at[:, x * NY + y], dst.at[x, y], s["load_sem"].at[n]).start()
            return 0

        lax.fori_loop(0, NX, step, 0)

    singles = [
        pltpu.make_async_copy(src, dst, s["load_sem"].at[2 + n])
        for n, (src, dst) in enumerate((
            (shift_hbm, s["shift"]), (advect_hbm, s["advect"]),
            (diffuse_hbm, s["diffuse"]), (coef_hbm, s["coef"]),
        ))
    ]
    DX, DY, DZ = {"gx": -1}, {"gy": -1}, {"gz": -1}
    UX, UY, UZ = {"gx": 1}, {"gy": 1}, {"gz": 1}
    barrier = pltpu.get_barrier_semaphore()
    count = 0
    for to in (DX, UX, DY, UY, DZ, UZ, UX | UZ, UY | UZ):
        cond = back = None
        for a, by in to.items():
            one, two = (below[a], above[a]) if by < 0 else (above[a], below[a])
            cond = one if cond is None else cond & one
            back = two if back is None else back & two

        @pl.when(cond)
        def _(to=to):
            pl.semaphore_signal(
                barrier, inc=1, device_id={a: me[a] + by for a, by in to.items()}, device_id_type=MESH
            )
        count = count + jnp.where(back, 1, 0)

    singles[0].start()
    load_cells(now_hbm, own, 0)
    pl.semaphore_wait(barrier, count)

    routes = {}

    class Route:
        def __init__(self, to):
            self.to = to
            self.send_sem = s["send_sem"].at[len(routes)]
            self.tiles = 0
            self.sends = self.gets = None
            for a, by in to.items():
                sends = below[a] if by < 0 else above[a]
                gets = above[a] if by < 0 else below[a]
                self.sends = sends if self.sends is None else self.sends & sends
                self.gets = gets if self.gets is None else self.gets & gets

        def copy(self, src, dst, recv_sem):
            return pltpu.make_async_remote_copy(
                src_ref=src, dst_ref=dst, send_sem=self.send_sem, recv_sem=recv_sem,
                device_id={a: me[a] + by for a, by in self.to.items()}, device_id_type=MESH,
            )

        def all_sent(self):
            done = s["count"].at[pl.ds(0, self.tiles)]
            pl.when(self.sends)(self.copy(done, done, s["recv_sem"].at[0]).wait_send)

    def route(to):
        key = tuple(sorted(to.items()))
        if key not in routes:
            routes[key] = Route(to)
        return routes[key]

    class Arrival:
        def __init__(self, to):
            self.route = route(to)
            self.recv_sem = s["recv_sem"].at[next(sems)]
            self.tiles = 0

        def arrived(self):
            done = s["count"].at[pl.ds(0, self.tiles)]
            pl.when(self.route.gets)(self.route.copy(done, done, self.recv_sem).wait_recv)

    def size_of(ref):
        return int(np.prod(ref.shape)) // (ROWS * NZ)

    class Message:
        def __init__(self, src, dst, to, arrival=None, parts=None):
            self.arrival = arrival or Arrival(to)
            self.route = route(to)
            tiles = size_of(dst)
            self.arrival.tiles += tiles
            self.route.tiles += tiles
            self.src, self.dst, self.parts = src, dst, parts

        def start(self):
            pl.when(self.route.sends)(self.route.copy(self.src, self.dst, self.arrival.recv_sem).start)

        def start_parts(self, i):
            @pl.when(self.route.sends)
            def _():
                for j in range(W):
                    self.route.copy(*self.parts(i, j), self.arrival.recv_sem).start()

        def arrived(self):
            self.arrival.arrived()

    message = Message

    lowx, lowy = pl.ds(0, W), pl.ds(0, W)
    raw, edge, diag, forward, corner = {}, {}, {}, {}, {}
    for c, kind in enumerate(kinds):
        if kind == "x":
            def cell(i, j, half, c=c):
                x, y = i, j + half * (NY // 2)
                return now_hbm.at[rows[c], x * NY + y], s[f"rawx{c}"].at[x, y]

            halves = [s[f"rawx{c}"].at[:, pl.ds(h * (NY // 2), NY // 2)] for h in range(2)]
            raw[c] = [message(r, r, DX, parts=functools.partial(cell, half=h)) for h, r in enumerate(halves)]
            diag[c] = [message(epk.at[c, 0], ein.at[c, 2], DX | DZ)]
            forward[c] = message(s[f"fw{c}"], s[f"te{c}"], DY)
        elif kind == "y":
            def cell(i, j, half, c=c):
                x, y = i + half * (NX // 2), j
                return now_hbm.at[rows[c], x * NY + y], s[f"rawy{c}"].at[x, y]

            halves = [s[f"rawy{c}"].at[pl.ds(h * (NX // 2), NX // 2)] for h in range(2)]
            raw[c] = [message(r, r, DY, parts=functools.partial(cell, half=h)) for h, r in enumerate(halves)]
            diag[c] = [message(epk.at[c, 0], ein.at[c, 2], DY | DZ)]
            forward[c] = message(s[f"fw{c}"], s[f"te{c}"], DX)
        else:
            raw[c] = [
                message(own.at[lowx, :, rows[c]], s[f"rawx{c}"], DX),
                message(own.at[:, lowy, rows[c]], s[f"rawy{c}"], DY),
            ]
            diag[c] = [
                message(epk.at[c, 0], ein.at[c, 2], DX | DZ), message(epk.at[c, 2], ein.at[c, 3], DY | DZ),
            ]
            near, far = pl.ds(0, W // 2), pl.ds(W // 2, W // 2)
            zs, ce = s[f"zs{c}"], s[f"ce{c}"]
            corner[c] = [
                message(zs.at[far, pl.ds(NY, W)], ce.at[far], DX),
                message(zs.at[pl.ds(NX, W // 2), lowy], ce.at[near], DY),
            ]
        edge[c] = message(epk.at[c, pl.ds(0, 2)], ein.at[c, pl.ds(0, 2)], DZ)

    inside = {(a, sign): Arrival({AXES[a]: -sign}) for a, sign in SIDES}
    rims_in = [Arrival(DZ), Arrival(UZ)]

    def halo(c, a, by, lo, hi):
        n = (NX, NY)[a]
        src = pl.ds(H, H) if by < 0 else pl.ds(n, H)
        dst = pl.ds(n + H, H) if by < 0 else pl.ds(0, H)
        span = pl.ds(H + lo, hi - lo)
        to = {AXES[a]: by}
        if a == 0:
            return message(box.at[src, span, rows[c]], box.at[dst, span, rows[c]], to, inside[(a, -by)])
        return message(box.at[span, src, rows[c]], box.at[span, dst, rows[c]], to, inside[(a, -by)])

    early_halo, late_halo, rims = {}, {}, {}
    hx, hy = NX // 2, NY // 2
    for c, kind in enumerate(kinds):
        if kind == "x":
            early_halo[c] = [halo(c, 1, -1, 0, NX), halo(c, 0, 1, 0, hy)]
            late_halo[c] = [halo(c, 0, -1, 0, NY), halo(c, 0, 1, hy, NY), halo(c, 1, 1, 0, NX)]
        elif kind == "y":
            early_halo[c] = [halo(c, 0, -1, 0, NY), halo(c, 1, 1, 0, hx)]
            late_halo[c] = [halo(c, 1, -1, 0, NX), halo(c, 1, 1, hx, NX), halo(c, 0, 1, 0, NY)]
        else:
            early_halo[c] = [halo(c, 0, -1, 0, NY), halo(c, 1, -1, 0, NX), halo(c, 0, 1, 0, hy), halo(c, 1, 1, 0, hx)]
            late_halo[c] = [halo(c, 0, 1, hy, NY), halo(c, 1, 1, hx, NX)]
        rims[c] = [
            message(rim.at[c], rim_up.at[c], DZ, rims_in[0]), message(rim.at[c], rim_low.at[c], UZ, rims_in[1]),
        ]

    def send_raw(i, _, half):
        for c, kind in enumerate(kinds):
            if kind != "xy":
                raw[c][half].start_parts(i)
        return 0

    for half in range(2):
        lax.fori_loop(0, W, functools.partial(send_raw, half=half), 0)

    lane = lax.broadcasted_iota(jnp.int32, (ROWS, NZ), 1)
    thin = lane // W
    wide = ((lane + SLOT // 2) % NZ) // SLOT
    blank = jnp.zeros((ROWS, NZ), f32)

    def pack(c, n, along, q):
        def step(i, packed):
            for j in range(NY if along == "x" else NX):
                x, y = (q * W + i, j) if along == "x" else (j, q * W + i)
                slot = i * (NY if along == "x" else NX) + j
                packed = jnp.where(thin == slot, pltpu.roll(own[x, y, rows[c]], W * slot, 1), packed)
            return packed

        epk[c, n] = lax.fori_loop(0, W, step, blank)

    pltpu.make_async_copy(par, own, s["load_sem"].at[0]).wait()
    for c, kind in enumerate(kinds):
        along = kind[0]
        for q in range(2):
            pack(c, q, along, q)
        if kind == "xy":
            pack(c, 2, "y", 0)
        for d in diag[c]:
            d.start()
        edge[c].start()
    for c, kind in enumerate(kinds):
        if kind == "xy":
            for r in raw[c]:
                r.start()

    for load in singles[1:]:
        load.start()
    load_cells(parent_hbm, par, 1)
    zero16 = jnp.zeros((2 * ROWS, NZ), bf16)

    def clear(i, _):
        for c in range(chunks):
            for o in range(H):
                ub[o, i + H, c] = zero16
                ub[NX + H + o, i + H, c] = zero16
                ub[i + H, o, c] = zero16
                ub[i + H, NY + H + o, c] = zero16
        return 0

    lax.fori_loop(0, NX, clear, 0)

    for load in singles:
        load.wait()
    move = [s["shift"][d] for d in range(3)]
    sz = move[2]

    def split16(u):
        low = u - u.astype(bf16).astype(f32)
        return jnp.concatenate([u, low], axis=0).astype(bf16)

    def weights():
        mats = []
        for m in (s["advect"], s["diffuse"]):
            for a in range(3):
                one = m[a]
                high = one.astype(bf16).astype(f32)
                mid = (one - high).astype(bf16).astype(f32)
                mats.append(jnp.concatenate([high, mid, one - high - mid], axis=0).astype(bf16))

        def columns(at, width, ks):
            table = s["coef"][:, at:at + width]
            hit = lax.broadcasted_iota(jnp.int32, (F, width), 0).astype(f32) == table[7:8]
            smooth = jnp.where(hit, table[6:7], 0.0)
            if not ks:
                return smooth
            total = None
            for k in ks:
                spread = jnp.where(hit, table[k:k + 1], 0.0).astype(bf16)
                part = jnp.dot(mats[k], spread, preferred_element_type=f32)
                total = part if total is None else total + part
            w = total[:F] + total[F:2 * F] + total[2 * F:]
            high = w.astype(bf16).astype(f32)
            return jnp.concatenate([high, (w - high) * table[8:9], smooth], axis=0)

        k_early = len(BLOCKS) * 2 * F
        for at in range(0, up_to(k_early, 256), 256):
            n = min(256, k_early - at)
            s["w_early"][:, at:at + n] = columns(at, 256, range(6))[:, :n].astype(bf16)
        at = up_to(k_early, 256)
        k_along = len(ALONG) * 2 * F
        s["w_along"][...] = columns(at, up_to(k_along, 256), (2, 5))[:2 * F, :k_along].astype(bf16)
        at += up_to(k_along, 256)
        k_late = H * 2 * F
        step = up_to(k_late, 256)
        for n, (a, sign) in enumerate(SIDES):
            parts = [columns(at + d * step, step, (a, 3 + a) if d < 2 else ()) for d in range(H)]
            s["w_late"][n] = jnp.concatenate(parts, axis=0)[:, :k_late].astype(bf16)
            at += H * step

    weights()

    def z_row(row, packed, slot):
        tail = pltpu.roll(packed, lax.rem(2 * NZ - W * slot - sz, NZ), 1)
        return jnp.where(lane >= NZ - sz, tail, pltpu.roll(row, NZ - sz, 1))

    def z_own(c):
        kind = kinds[c]

        def step(x, _):
            for y in range(NY):
                q, slot = (x // W, x % W * NY + y) if "x" in kind else (y // W, y % W * NX + x)
                s[f"zs{c}"][x, y] = z_row(own[x, y, rows[c]], ein[c, q], slot)
            return 0

        lax.fori_loop(0, NX, step, 0)

    def z_ext_x(c, lo, hi):
        def step(x, _):
            for y in range(lo, hi):
                s[f"zs{c}"][NX + x, y] = z_row(s[f"rawx{c}"][x, y], ein[c, 2], x * NY + y)
            return 0

        lax.fori_loop(0, W, step, 0)

    def z_ext_y(c, lo, hi):
        n = 3 if kinds[c] == "xy" else 2

        def step(x, _):
            for y in range(W):
                s[f"zs{c}"][x, NY + y] = z_row(s[f"rawy{c}"][x, y], ein[c, n], y * NX + x)
            return 0

        lax.fori_loop(lo, hi, step, 0)

    def make_forward(c):
        zs, fw = s[f"zs{c}"], s[f"fw{c}"]

        def step(i, _):
            for j in range(W):
                if kinds[c] == "x":
                    fw[i, j] = zs[i + move[0], j]
                else:
                    fw[j, i] = zs[j, i + move[1]]
            return 0

        lax.fori_loop(0, NX if kinds[c] == "x" else NY, step, 0)

    in_z = me["gz"] * NZ + lane + sz < size["gz"] * NZ

    def renew(c, xs, ys, late):
        kind, zs = kinds[c], s[f"zs{c}"]

        def step(x, _):
            in_x = me["gx"] * NX + x + move[0] < size["gx"] * NX
            for y in range(*ys):
                in_y = me["gy"] * NY + y + move[1] < size["gy"] * NY
                X, Y = x + move[0], y + move[1]
                if not late:
                    row = zs[X, Y]
                elif kind == "x":
                    row = jnp.where(Y < NY, zs[X, jnp.minimum(Y, NY - 1)], s[f"te{c}"][x, jnp.maximum(Y - NY, 0)])
                elif kind == "y":
                    row = jnp.where(X < NX, zs[jnp.minimum(X, NX - 1), Y], s[f"te{c}"][jnp.maximum(X - NX, 0), y])
                else:
                    row = jnp.where(
                        (X < NX) | (Y < NY), zs[X, Y],
                        s[f"ce{c}"][jnp.maximum(X - NX, 0), jnp.maximum(Y - NY, 0)],
                    )
                row = jnp.where(in_z & (in_x & in_y), row, par[x, y, rows[c]])
                box[x + H, y + H, rows[c]] = row
                ub[x + H, y + H, c] = split16(row)
            return 0

        lax.fori_loop(*xs, step, 0)

    def renew_early(c):
        if kinds[c] == "x":
            renew(c, (0, NX), (0, hy), False)
        elif kinds[c] == "y":
            renew(c, (0, hx), (0, NY), False)
        else:
            renew(c, (0, hx), (0, NY), False)
            renew(c, (hx, NX), (0, hy), False)
        for h in early_halo[c]:
            h.start()

    def renew_late(c):
        if kinds[c] == "x":
            renew(c, (0, NX), (hy, NY), True)
        elif kinds[c] == "y":
            renew(c, (hx, NX), (0, NY), True)
        else:
            renew(c, (hx, NX), (hy, NY), True)
        for h in late_halo[c]:
            h.start()

        def step(g, _):
            packed = blank
            for j in range(slots):
                x, y = g * (slots // NY) + j // NY, j % NY
                packed = jnp.where(wide == j, pltpu.roll(box[x + H, y + H, rows[c]], SLOT * j, 1), packed)
            rim[c, g] = packed
            return 0

        lax.fori_loop(0, groups, step, 0)
        for r in rims[c]:
            r.start()

    one_way = [c for c in range(chunks) if kinds[c] != "xy"]
    both = [c for c in range(chunks) if kinds[c] == "xy"]
    for c in one_way:
        edge[c].arrived()
        z_own(c)
    for c in one_way:
        diag[c][0].arrived()
        raw[c][0].arrived()
        if kinds[c] == "x":
            z_ext_x(c, 0, hy)
        else:
            z_ext_y(c, 0, hx)
        make_forward(c)
        forward[c].start()
    for c in both:
        edge[c].arrived()
        z_own(c)
    for c in one_way:
        raw[c][1].arrived()
        if kinds[c] == "x":
            z_ext_x(c, hy, NY)
        else:
            z_ext_y(c, hx, NX)
    for c in both:
        for d in diag[c]:
            d.arrived()
        raw[c][0].arrived()
        z_ext_x(c, 0, NY)
        raw[c][1].arrived()
        z_ext_y(c, 0, NX)
        for k in corner[c]:
            k.start()
    pltpu.make_async_copy(own, par, s["load_sem"].at[1]).wait()
    for c in (*one_way, *both):
        renew_early(c)
    for c in one_way:
        forward[c].arrived()
        renew_late(c)
    for c in both:
        for k in corner[c]:
            k.arrived()
        renew_late(c)

    def early(x, _):
        for y0 in range(0, NY, 2):
            sides = []
            for y in (y0, y0 + 1):
                parts = []
                for a, o in BLOCKS:
                    dx, dy = (0, o) if a == 1 else (o, 0)
                    parts += [ub[x + H + dx, y + H + dy, c] for c in range(chunks)]
                sides.append(jnp.concatenate(parts, axis=0))
            out = jnp.dot(s["w_early"][...], jnp.concatenate(sides, axis=1), preferred_element_type=f32)
            for q in range(2):
                part = out[:, q * NZ:(q + 1) * NZ]
                acc[x, y0 + q, pl.ds(0, F)] = part[:F] + part[F:2 * F]
                acc[x, y0 + q, pl.ds(F, F)] = part[2 * F:]
        return 0

    lax.fori_loop(0, NX, early, 0)

    for r in rims_in:
        r.arrived()

    def along(x, _):
        ends_all = [
            jnp.where(
                lane % SLOT < SLOT // 2,
                jnp.where(above["gz"], rim_up[c, x * NY // slots], 0.0),
                jnp.where(below["gz"], rim_low[c, x * NY // slots], 0.0),
            )
            for c in range(chunks)
        ]
        for y0 in range(0, NY, 2):
            sides = []
            for y in (y0, y0 + 1):
                firsts, seconds = [], []
                for c in range(chunks):
                    u = box[x + H, y + H, rows[c]]
                    ends = pltpu.roll(ends_all[c], lax.rem(2 * NZ - SLOT * (x * NY % slots + y), NZ), 1)
                    d, t = {}, {}
                    for o in range(1, H + 1):
                        after = pltpu.roll(jnp.where(lane < o, ends, u), NZ - o, 1)
                        before = pltpu.roll(jnp.where(lane >= NZ - o, ends, u), o, 1)
                        d[o], t[o] = after - before, after + before
                    firsts.append(split16(8.0 * d[1] - d[2]))
                    seconds.append(split16(16.0 * t[1] - t[2]))
                    acc[x, y, pl.ds(F + c * ROWS, ROWS)] += t[3] - 6.0 * t[2] + 15.0 * t[1]
                sides.append(jnp.concatenate(firsts + seconds, axis=0))
            out = jnp.dot(s["w_along"][...], jnp.concatenate(sides, axis=1), preferred_element_type=f32)
            for q in range(2):
                part = out[:, q * NZ:(q + 1) * NZ]
                acc[x, y0 + q, pl.ds(0, F)] += part[:F] + part[F:]
        return 0

    lax.fori_loop(0, NX, along, 0)

    def late(n):
        a, sign = SIDES[n]
        length = (NX, NY)[a]
        across = (NY, NX)[a]

        def step(p, _):
            sides = []
            for q in range(2):
                parts = []
                for h in range(1, H + 1):
                    at = H + (length - 1 + h if sign > 0 else -h)
                    for c in range(chunks):
                        where = (at, H + 2 * p + q) if a == 0 else (H + 2 * p + q, at)
                        parts.append(split16(box[(*where, rows[c])]))
                sides.append(jnp.concatenate(parts, axis=0))
            out = jnp.dot(s["w_late"][n], jnp.concatenate(sides, axis=1), preferred_element_type=f32)
            for q in range(2):
                part = out[:, q * NZ:(q + 1) * NZ]
                for d in range(H):
                    at = length - 1 - d if sign > 0 else d
                    where = (at, 2 * p + q) if a == 0 else (2 * p + q, at)
                    if d < 2:
                        own_part = part[3 * F * d:3 * F * (d + 1)]
                        acc[(*where, pl.ds(0, F))] += own_part[:F] + own_part[F:2 * F]
                        acc[(*where, pl.ds(F, F))] += own_part[2 * F:]
                    else:
                        acc[(*where, pl.ds(F, F))] += part[6 * F:]
            return 0

        lax.fori_loop(0, across // 2, step, 0)

    for sign in (-1, 1):
        for a in range(2):
            n = SIDES.index((a, sign))
            inside[SIDES[n]].arrived()
            pl.when((above if sign > 0 else below)[AXES[a]])(functools.partial(late, n))

    def finish(x, _):
        for y in range(NY):
            u = box[x + H, y + H]
            lapse = (1.0 + 0.25 * jnp.tanh(u[0:1])) * (1.0 / 12.0)
            slope = lapse * acc[x, y, pl.ds(0, F)] + acc[x, y, pl.ds(F, F)] * (1.0 / 64.0)
            slope_ref[x * NY + y] = slope
            value_ref[x * NY + y] = u + 0.125 * slope
        return 0

    lax.fori_loop(0, NX, finish, 0)

    for r in routes.values():
        r.all_sent()


def put_out(slope_in, value_in, slope_hbm, value_hbm, sem):
    cells = slope_in.shape[0]

    def step(k, _):
        pltpu.make_async_copy(slope_in.at[k], slope_hbm.at[:, k], sem.at[0]).start()
        pltpu.make_async_copy(value_in.at[k], value_hbm.at[:, k], sem.at[1]).start()
        return 0

    lax.fori_loop(0, cells, step, 0, unroll=8)
    pltpu.make_async_copy(slope_in, value_in, sem.at[0]).wait()
    pltpu.make_async_copy(slope_in, value_in, sem.at[1]).wait()


def local(fields_now, parent, advect, diffuse, box_shift):
    dims = fields_now.shape
    F, NX, NY, NZ = dims
    flat = (F, NX * NY, NZ)
    by_cell = (NX * NY, F, NZ)
    vmem = pl.BlockSpec(memory_space=pltpu.VMEM)
    hbm = pl.BlockSpec(memory_space=pltpu.HBM)
    operands = [
        pltpu.with_memory_space_constraint(x, pltpu.HBM)
        for x in (box_shift, fields_now.reshape(flat), parent.reshape(flat), advect, diffuse, jnp.asarray(coefficients(F)))
    ]
    results = pl.pallas_call(
        functools.partial(kernel, dims),
        out_shape=[pltpu.VMEM(by_cell, f32)] * 2,
        in_specs=[hbm] * 6,
        out_specs=[vmem] * 2,
        scratch_shapes=list(scratch(dims).values()),
        compiler_params=pltpu.CompilerParams(
            collective_id=0, has_side_effects=True, vmem_limit_bytes=VMEM_BYTES
        ),
    )(*operands)
    slope, value = pl.pallas_call(
        put_out,
        out_shape=[jax.ShapeDtypeStruct(flat, f32)] * 2,
        in_specs=[vmem] * 2,
        out_specs=[hbm] * 2,
        scratch_shapes=[pltpu.SemaphoreType.DMA((2,))],
        compiler_params=pltpu.CompilerParams(vmem_limit_bytes=VMEM_BYTES),
    )(*results)
    return slope.reshape(dims), value.reshape(dims)


VMEM_BYTES = 40 * 2**20


def solution(mesh):
    return jax.shard_map(
        local,
        mesh=mesh,
        in_specs=(P(None, "gx", "gy", "gz"), P(None, "gx", "gy", "gz"), P(), P(), P()),
        out_specs=(P(None, "gx", "gy", "gz"), P(None, "gx", "gy", "gz")),
        check_vma=False,
    )
```

```python
import functools

import jax
import jax.numpy as jnp
import numpy as np
from jax import lax
from jax.experimental import pallas as pl
from jax.experimental.pallas import tpu as pltpu
from jax.sharding import PartitionSpec as P

MESH = pl.DeviceIdType.MESH
W = 4
H = 3
SLOT = 8
ROWS = 8
AXES = ("gx", "gy", "gz")
KINDS = ("x", "y", "xy")
ARRIVALS = {"x": 5, "y": 5, "xy": 7}
ROUTES = 8
FIRST = {-2: 1, -1: -8, 1: 8, 2: -1}
SECOND = {-2: -1, -1: 16, 0: -30, 1: 16, 2: -1}
SIXTH = {-3: 1, -2: -6, -1: 15, 0: -20, 1: 15, 2: -6, 3: 1}
BLOCKS = [(None, 0)] + [(a, o) for a in range(2) for o in (-3, -2, -1, 1, 2, 3)]
ALONG = [(2, "first"), (2, "second")]
SIDES = [(a, sign) for a in range(2) for sign in (-1, 1)]
f32, bf16 = jnp.float32, jnp.bfloat16


def up_to(n, m):
    return -(-n // m) * m


def block_columns(block, fields):
    cols = np.zeros((16, 2 * fields), np.float32)
    for c in range(fields // ROWS):
        for h in range(2):
            for r in range(ROWS):
                n = (c * 2 + h) * ROWS + r
                cols[7, n] = c * ROWS + r
                cols[8, n] = 1 - h
    if block is None:
        return cols
    axis, o = block
    if o in ("first", "second"):
        cols[axis + (3 if o == "second" else 0)] = 1
        return cols
    for a in range(3):
        if axis is None or a == axis:
            cols[a] = FIRST.get(o, 0)
            cols[3 + a] = SECOND.get(o, 0)
            cols[6] += SIXTH[o]
    return cols


def coefficients(fields):
    groups = [BLOCKS, ALONG]
    for a, sign in SIDES:
        groups += [[(a, sign), (a, 2 * sign)], [(a, 2 * sign), None]]
    out = []
    for g in groups:
        cols = np.concatenate([block_columns(b, fields) for b in g], axis=1)
        out.append(np.pad(cols, ((0, 0), (0, up_to(cols.shape[1], 256) - cols.shape[1]))))
    return np.concatenate(out, axis=1)


def scratch(dims):
    F, NX, NY, NZ = dims
    chunks = F // ROWS
    groups = NX * NY * SLOT // NZ
    tile = (ROWS, NZ)
    out = dict(
        shift=pltpu.SMEM((3,), jnp.int32),
        own=pltpu.VMEM((NX, NY, F, NZ), f32),
        par=pltpu.VMEM((NX, NY, F, NZ), f32),
        advect=pltpu.VMEM((3, F, F), f32),
        diffuse=pltpu.VMEM((3, F, F), f32),
        coef=pltpu.VMEM(coefficients(F).shape, f32),
        w_early=pltpu.VMEM((3 * F, len(BLOCKS) * 2 * F), bf16),
        w_along=pltpu.VMEM((2 * F, len(ALONG) * 2 * F), bf16),
        ub=pltpu.VMEM((NX + 2 * H, NY + 2 * H, chunks, 2 * ROWS, NZ), bf16),
        rim=pltpu.VMEM((chunks, groups) + tile, f32),
        rim_up=pltpu.VMEM((chunks, groups) + tile, f32),
        rim_low=pltpu.VMEM((chunks, groups) + tile, f32),
        epk=pltpu.VMEM((chunks, 3) + tile, f32),
        ein=pltpu.VMEM((chunks, 4) + tile, f32),
    )
    for c in range(chunks):
        kind = KINDS[c % 3]
        if "x" in kind:
            out[f"rawx{c}"] = pltpu.VMEM((W, NY) + tile, f32)
        if "y" in kind:
            out[f"rawy{c}"] = pltpu.VMEM((NX, W) + tile, f32)
        ext = (W if "x" in kind else 0, W if "y" in kind else 0)
        out[f"zs{c}"] = pltpu.VMEM((NX + ext[0], NY + ext[1]) + tile, f32)
        if kind == "xy":
            out[f"ce{c}"] = pltpu.VMEM((W, W) + tile, f32)
        else:
            size = (NX, W) if kind == "x" else (W, NY)
            out[f"fw{c}"] = pltpu.VMEM(size + tile, f32)
            out[f"te{c}"] = pltpu.VMEM(size + tile, f32)
    out["count"] = pltpu.VMEM((chunks * 8 * NX * NY,) + tile, f32)
    n = sum(ARRIVALS[KINDS[c % 3]] for c in range(chunks)) + len(SIDES) + 2
    out["send_sem"] = pltpu.SemaphoreType.DMA((ROUTES,))
    out["recv_sem"] = pltpu.SemaphoreType.DMA((n,))
    out["load_sem"] = pltpu.SemaphoreType.DMA((6,))
    return out


def split16(u):
    low = u - u.astype(bf16).astype(f32)
    return jnp.concatenate([u, low], axis=0).astype(bf16)


def add_side(box, acc, out_acc, w_late, n, again=None):
    a, sign = SIDES[n]
    NX, NY, F, NZ = acc.shape[0], acc.shape[1], acc.shape[2] // 2, acc.shape[3]
    length, across = ((NX, NY), (NY, NX))[a]
    linear_rows, smooth_rows = pl.ds(0, F), pl.ds(F, F)

    def spot(depth, i):
        at = length - 1 - depth if sign > 0 else depth
        return (at, i) if a == 0 else (i, at)

    for i0 in range(0, across, 2):
        columns, smooth = [], []
        for i in (i0, i0 + 1):
            near = []
            for h in range(1, H + 1):
                x, y = spot(-h, i)
                near.append(box[x + H, y + H])
            smooth.append((15.0 * near[0] - 6.0 * near[1] + near[2], near[1] - 6.0 * near[0], near[0]))
            parts = [split16(u[c:c + ROWS]) for u in near[:2] for c in range(0, F, ROWS)]
            columns.append(jnp.concatenate(parts, axis=0))
        out = jnp.dot(w_late[n], jnp.concatenate(columns, axis=1), preferred_element_type=f32)
        for q in range(2):
            part = out[:, q * NZ:(q + 1) * NZ]
            for d in range(H):
                x, y = spot(d, i0 + q)
                source = out_acc if again is not None and again(x, y) else acc
                linear = source[x, y, linear_rows]
                if d < 2:
                    mine = part[2 * F * d:2 * F * (d + 1)]
                    linear = linear + (mine[:F] + mine[F:])
                out_acc[x, y, linear_rows] = linear
                out_acc[x, y, smooth_rows] = source[x, y, smooth_rows] + smooth[q][d]


def finished(box, acc, x, y):
    u = box[x + H, y + H]
    F = u.shape[0]
    lapse = (1.0 + 0.25 * jnp.tanh(u[0:1])) * (1.0 / 12.0)
    slope = lapse * acc[x, y, pl.ds(0, F)] + acc[x, y, pl.ds(F, F)] * (1.0 / 64.0)
    return slope, u + 0.125 * slope


def kernel(
    dims, shift_hbm, now_hbm, parent_hbm, advect_hbm, diffuse_hbm, coef_hbm,
    slope_ref, value_ref, acc, box, w_late, *refs
):
    F, NX, NY, NZ = dims
    chunks = F // ROWS
    cells = NX * NY
    s = dict(zip(scratch(dims), refs))
    own, par, ub = s["own"], s["par"], s["ub"]
    epk, ein, rim, rim_up, rim_low = s["epk"], s["ein"], s["rim"], s["rim_up"], s["rim_low"]
    slots = NZ // SLOT
    groups = cells // slots
    me = {a: lax.axis_index(a) for a in AXES}
    size = {a: lax.axis_size(a) for a in AXES}
    below = {a: me[a] > 0 for a in AXES}
    above = {a: me[a] < size[a] - 1 for a in AXES}
    sems = iter(range(1000))
    kinds = [KINDS[c % 3] for c in range(chunks)]
    rows = [pl.ds(c * ROWS, ROWS) for c in range(chunks)]

    def load_cells(src, dst, n):
        def step(x, _):
            for y in range(NY):
                pltpu.make_async_copy(src.at[:, x * NY + y], dst.at[x, y], s["load_sem"].at[n]).start()
            return 0

        lax.fori_loop(0, NX, step, 0)

    singles = [
        pltpu.make_async_copy(src, dst, s["load_sem"].at[2 + n])
        for n, (src, dst) in enumerate((
            (shift_hbm, s["shift"]), (advect_hbm, s["advect"]),
            (diffuse_hbm, s["diffuse"]), (coef_hbm, s["coef"]),
        ))
    ]
    DX, DY, DZ = {"gx": -1}, {"gy": -1}, {"gz": -1}
    UX, UY, UZ = {"gx": 1}, {"gy": 1}, {"gz": 1}
    barrier = pltpu.get_barrier_semaphore()
    count = 0
    for to in (DX, UX, DY, UY, DZ, UZ, UX | UZ, UY | UZ):
        cond = back = None
        for a, by in to.items():
            one, two = (below[a], above[a]) if by < 0 else (above[a], below[a])
            cond = one if cond is None else cond & one
            back = two if back is None else back & two

        @pl.when(cond)
        def _(to=to):
            pl.semaphore_signal(
                barrier, inc=1, device_id={a: me[a] + by for a, by in to.items()}, device_id_type=MESH
            )
        count = count + jnp.where(back, 1, 0)

    singles[0].start()
    load_cells(now_hbm, own, 0)
    pl.semaphore_wait(barrier, count)

    routes = {}

    class Route:
        def __init__(self, to):
            self.to = to
            self.send_sem = s["send_sem"].at[len(routes)]
            self.tiles = 0
            self.sends = self.gets = None
            for a, by in to.items():
                sends = below[a] if by < 0 else above[a]
                gets = above[a] if by < 0 else below[a]
                self.sends = sends if self.sends is None else self.sends & sends
                self.gets = gets if self.gets is None else self.gets & gets

        def copy(self, src, dst, recv_sem):
            return pltpu.make_async_remote_copy(
                src_ref=src, dst_ref=dst, send_sem=self.send_sem, recv_sem=recv_sem,
                device_id={a: me[a] + by for a, by in self.to.items()}, device_id_type=MESH,
            )

        def all_sent(self):
            done = s["count"].at[pl.ds(0, self.tiles)]
            pl.when(self.sends)(self.copy(done, done, s["recv_sem"].at[0]).wait_send)

    def route(to):
        key = tuple(sorted(to.items()))
        if key not in routes:
            routes[key] = Route(to)
        return routes[key]

    class Arrival:
        def __init__(self, to):
            self.route = route(to)
            self.recv_sem = s["recv_sem"].at[next(sems)]
            self.tiles = 0

        def arrived(self):
            done = s["count"].at[pl.ds(0, self.tiles)]
            pl.when(self.route.gets)(self.route.copy(done, done, self.recv_sem).wait_recv)

    def size_of(ref):
        return int(np.prod(ref.shape)) // (ROWS * NZ)

    class Message:
        def __init__(self, src, dst, to, arrival=None, parts=None):
            self.arrival = arrival or Arrival(to)
            self.route = route(to)
            tiles = size_of(dst)
            self.arrival.tiles += tiles
            self.route.tiles += tiles
            self.src, self.dst, self.parts = src, dst, parts

        def start(self):
            pl.when(self.route.sends)(self.route.copy(self.src, self.dst, self.arrival.recv_sem).start)

        def start_parts(self, i):
            @pl.when(self.route.sends)
            def _():
                for j in range(W):
                    self.route.copy(*self.parts(i, j), self.arrival.recv_sem).start()

        def arrived(self):
            self.arrival.arrived()

    message = Message

    lowx, lowy = pl.ds(0, W), pl.ds(0, W)
    raw, edge, diag, forward, corner = {}, {}, {}, {}, {}
    for c, kind in enumerate(kinds):
        if kind == "x":
            def cell(i, j, half, c=c):
                x, y = i, j + half * (NY // 2)
                return now_hbm.at[rows[c], x * NY + y], s[f"rawx{c}"].at[x, y]

            halves = [s[f"rawx{c}"].at[:, pl.ds(h * (NY // 2), NY // 2)] for h in range(2)]
            raw[c] = [message(r, r, DX, parts=functools.partial(cell, half=h)) for h, r in enumerate(halves)]
            diag[c] = [message(epk.at[c, 0], ein.at[c, 2], DX | DZ)]
            forward[c] = message(s[f"fw{c}"], s[f"te{c}"], DY)
        elif kind == "y":
            def cell(i, j, half, c=c):
                x, y = i + half * (NX // 2), j
                return now_hbm.at[rows[c], x * NY + y], s[f"rawy{c}"].at[x, y]

            halves = [s[f"rawy{c}"].at[pl.ds(h * (NX // 2), NX // 2)] for h in range(2)]
            raw[c] = [message(r, r, DY, parts=functools.partial(cell, half=h)) for h, r in enumerate(halves)]
            diag[c] = [message(epk.at[c, 0], ein.at[c, 2], DY | DZ)]
            forward[c] = message(s[f"fw{c}"], s[f"te{c}"], DX)
        else:
            raw[c] = [
                message(own.at[lowx, :, rows[c]], s[f"rawx{c}"], DX),
                message(own.at[:, lowy, rows[c]], s[f"rawy{c}"], DY),
            ]
            diag[c] = [
                message(epk.at[c, 0], ein.at[c, 2], DX | DZ), message(epk.at[c, 2], ein.at[c, 3], DY | DZ),
            ]
            near, far = pl.ds(0, W // 2), pl.ds(W // 2, W // 2)
            zs, ce = s[f"zs{c}"], s[f"ce{c}"]
            corner[c] = [
                message(zs.at[far, pl.ds(NY, W)], ce.at[far], DX),
                message(zs.at[pl.ds(NX, W // 2), lowy], ce.at[near], DY),
            ]
        edge[c] = message(epk.at[c, pl.ds(0, 2)], ein.at[c, pl.ds(0, 2)], DZ)

    inside = {(a, sign): Arrival({AXES[a]: -sign}) for a, sign in SIDES}
    rims_in = [Arrival(DZ), Arrival(UZ)]

    def halo(c, a, by, lo, hi):
        n = (NX, NY)[a]
        src = pl.ds(H, H) if by < 0 else pl.ds(n, H)
        dst = pl.ds(n + H, H) if by < 0 else pl.ds(0, H)
        span = pl.ds(H + lo, hi - lo)
        to = {AXES[a]: by}
        if a == 0:
            return message(box.at[src, span, rows[c]], box.at[dst, span, rows[c]], to, inside[(a, -by)])
        return message(box.at[span, src, rows[c]], box.at[span, dst, rows[c]], to, inside[(a, -by)])

    early_halo, late_halo, rims = {}, {}, {}
    hx, hy = NX // 2, NY // 2
    for c, kind in enumerate(kinds):
        if kind == "x":
            early_halo[c] = [halo(c, 1, -1, 0, NX), halo(c, 0, 1, 0, hy)]
            late_halo[c] = [halo(c, 0, -1, 0, NY), halo(c, 0, 1, hy, NY), halo(c, 1, 1, 0, NX)]
        elif kind == "y":
            early_halo[c] = [halo(c, 0, -1, 0, NY), halo(c, 1, 1, 0, hx)]
            late_halo[c] = [halo(c, 1, -1, 0, NX), halo(c, 1, 1, hx, NX), halo(c, 0, 1, 0, NY)]
        else:
            early_halo[c] = [halo(c, 0, -1, 0, NY), halo(c, 1, -1, 0, NX), halo(c, 0, 1, 0, hy), halo(c, 1, 1, 0, hx)]
            late_halo[c] = [halo(c, 0, 1, hy, NY), halo(c, 1, 1, hx, NX)]
        rims[c] = [
            message(rim.at[c], rim_up.at[c], DZ, rims_in[0]), message(rim.at[c], rim_low.at[c], UZ, rims_in[1]),
        ]

    def send_raw(i, _, half):
        for c, kind in enumerate(kinds):
            if kind != "xy":
                raw[c][half].start_parts(i)
        return 0

    for half in range(2):
        lax.fori_loop(0, W, functools.partial(send_raw, half=half), 0)

    lane = lax.broadcasted_iota(jnp.int32, (ROWS, NZ), 1)
    thin = lane // W
    wide = ((lane + SLOT // 2) % NZ) // SLOT
    blank = jnp.zeros((ROWS, NZ), f32)

    def pack(c, n, along, q):
        def step(i, packed):
            for j in range(NY if along == "x" else NX):
                x, y = (q * W + i, j) if along == "x" else (j, q * W + i)
                slot = i * (NY if along == "x" else NX) + j
                packed = jnp.where(thin == slot, pltpu.roll(own[x, y, rows[c]], W * slot, 1), packed)
            return packed

        epk[c, n] = lax.fori_loop(0, W, step, blank)

    pltpu.make_async_copy(par, own, s["load_sem"].at[0]).wait()
    for c, kind in enumerate(kinds):
        along = kind[0]
        for q in range(2):
            pack(c, q, along, q)
        if kind == "xy":
            pack(c, 2, "y", 0)
        for d in diag[c]:
            d.start()
        edge[c].start()
    for c, kind in enumerate(kinds):
        if kind == "xy":
            for r in raw[c]:
                r.start()

    for load in singles[1:]:
        load.start()
    load_cells(parent_hbm, par, 1)
    zero16 = jnp.zeros((2 * ROWS, NZ), bf16)

    def clear(i, _):
        for c in range(chunks):
            for o in range(H):
                ub[o, i + H, c] = zero16
                ub[NX + H + o, i + H, c] = zero16
                ub[i + H, o, c] = zero16
                ub[i + H, NY + H + o, c] = zero16
        return 0

    lax.fori_loop(0, NX, clear, 0)

    for load in singles:
        load.wait()
    move = [s["shift"][d] for d in range(3)]
    sz = move[2]

    def weights():
        mats = []
        for m in (s["advect"], s["diffuse"]):
            for a in range(3):
                one = m[a]
                high = one.astype(bf16).astype(f32)
                mid = (one - high).astype(bf16).astype(f32)
                mats.append(jnp.concatenate([high, mid, one - high - mid], axis=0).astype(bf16))

        def columns(at, width, ks):
            table = s["coef"][:, at:at + width]
            hit = lax.broadcasted_iota(jnp.int32, (F, width), 0).astype(f32) == table[7:8]
            smooth = jnp.where(hit, table[6:7], 0.0)
            total = None
            for k in ks:
                spread = jnp.where(hit, table[k:k + 1], 0.0).astype(bf16)
                part = jnp.dot(mats[k], spread, preferred_element_type=f32)
                total = part if total is None else total + part
            w = total[:F] + total[F:2 * F] + total[2 * F:]
            high = w.astype(bf16).astype(f32)
            return jnp.concatenate([high, (w - high) * table[8:9], smooth], axis=0)

        k_early = len(BLOCKS) * 2 * F
        for at in range(0, up_to(k_early, 256), 256):
            n = min(256, k_early - at)
            s["w_early"][:, at:at + n] = columns(at, 256, range(6))[:, :n].astype(bf16)
        at = up_to(k_early, 256)
        k_along = len(ALONG) * 2 * F
        s["w_along"][...] = columns(at, up_to(k_along, 256), (2, 5))[:2 * F, :k_along].astype(bf16)
        at += up_to(k_along, 256)
        k_late = 2 * 2 * F
        step = up_to(k_late, 256)
        for n, (a, sign) in enumerate(SIDES):
            parts = [columns(at + d * step, step, (a, 3 + a))[:2 * F] for d in range(2)]
            w_late[n] = jnp.concatenate(parts, axis=0)[:, :k_late].astype(bf16)
            at += 2 * step

    weights()

    def z_row(row, packed, slot):
        tail = pltpu.roll(packed, lax.rem(2 * NZ - W * slot - sz, NZ), 1)
        return jnp.where(lane >= NZ - sz, tail, pltpu.roll(row, NZ - sz, 1))

    def z_own(c):
        kind = kinds[c]

        def step(x, _):
            for y in range(NY):
                q, slot = (x // W, x % W * NY + y) if "x" in kind else (y // W, y % W * NX + x)
                s[f"zs{c}"][x, y] = z_row(own[x, y, rows[c]], ein[c, q], slot)
            return 0

        lax.fori_loop(0, NX, step, 0)

    def z_ext_x(c, lo, hi):
        def step(x, _):
            for y in range(lo, hi):
                s[f"zs{c}"][NX + x, y] = z_row(s[f"rawx{c}"][x, y], ein[c, 2], x * NY + y)
            return 0

        lax.fori_loop(0, W, step, 0)

    def z_ext_y(c, lo, hi):
        n = 3 if kinds[c] == "xy" else 2

        def step(x, _):
            for y in range(W):
                s[f"zs{c}"][x, NY + y] = z_row(s[f"rawy{c}"][x, y], ein[c, n], y * NX + x)
            return 0

        lax.fori_loop(lo, hi, step, 0)

    def make_forward(c):
        zs, fw = s[f"zs{c}"], s[f"fw{c}"]

        def step(i, _):
            for j in range(W):
                if kinds[c] == "x":
                    fw[i, j] = zs[i + move[0], j]
                else:
                    fw[j, i] = zs[j, i + move[1]]
            return 0

        lax.fori_loop(0, NX if kinds[c] == "x" else NY, step, 0)

    in_z = me["gz"] * NZ + lane + sz < size["gz"] * NZ

    def renew(c, xs, ys, late):
        kind, zs = kinds[c], s[f"zs{c}"]

        def step(x, _):
            in_x = me["gx"] * NX + x + move[0] < size["gx"] * NX
            for y in range(*ys):
                in_y = me["gy"] * NY + y + move[1] < size["gy"] * NY
                X, Y = x + move[0], y + move[1]
                if not late:
                    row = zs[X, Y]
                elif kind == "x":
                    row = jnp.where(Y < NY, zs[X, jnp.minimum(Y, NY - 1)], s[f"te{c}"][x, jnp.maximum(Y - NY, 0)])
                elif kind == "y":
                    row = jnp.where(X < NX, zs[jnp.minimum(X, NX - 1), Y], s[f"te{c}"][jnp.maximum(X - NX, 0), y])
                else:
                    row = jnp.where(
                        (X < NX) | (Y < NY), zs[X, Y],
                        s[f"ce{c}"][jnp.maximum(X - NX, 0), jnp.maximum(Y - NY, 0)],
                    )
                row = jnp.where(in_z & (in_x & in_y), row, par[x, y, rows[c]])
                box[x + H, y + H, rows[c]] = row
                ub[x + H, y + H, c] = split16(row)
            return 0

        lax.fori_loop(*xs, step, 0)

    def renew_early(c):
        if kinds[c] == "x":
            renew(c, (0, NX), (0, hy), False)
        elif kinds[c] == "y":
            renew(c, (0, hx), (0, NY), False)
        else:
            renew(c, (0, hx), (0, NY), False)
            renew(c, (hx, NX), (0, hy), False)
        for h in early_halo[c]:
            h.start()

    def renew_late(c):
        if kinds[c] == "x":
            renew(c, (0, NX), (hy, NY), True)
        elif kinds[c] == "y":
            renew(c, (hx, NX), (0, NY), True)
        else:
            renew(c, (hx, NX), (hy, NY), True)
        for h in late_halo[c]:
            h.start()

        def step(g, _):
            packed = blank
            for j in range(slots):
                x, y = g * (slots // NY) + j // NY, j % NY
                packed = jnp.where(wide == j, pltpu.roll(box[x + H, y + H, rows[c]], SLOT * j, 1), packed)
            rim[c, g] = packed
            return 0

        lax.fori_loop(0, groups, step, 0)
        for r in rims[c]:
            r.start()

    one_way = [c for c in range(chunks) if kinds[c] != "xy"]
    both = [c for c in range(chunks) if kinds[c] == "xy"]
    for c in one_way:
        edge[c].arrived()
        z_own(c)
    for c in one_way:
        diag[c][0].arrived()
        raw[c][0].arrived()
        if kinds[c] == "x":
            z_ext_x(c, 0, hy)
        else:
            z_ext_y(c, 0, hx)
        make_forward(c)
        forward[c].start()
    for c in both:
        edge[c].arrived()
        z_own(c)
    for c in one_way:
        raw[c][1].arrived()
        if kinds[c] == "x":
            z_ext_x(c, hy, NY)
        else:
            z_ext_y(c, hx, NX)
    for c in both:
        for d in diag[c]:
            d.arrived()
        raw[c][0].arrived()
        z_ext_x(c, 0, NY)
        raw[c][1].arrived()
        z_ext_y(c, 0, NX)
        for k in corner[c]:
            k.start()
    pltpu.make_async_copy(own, par, s["load_sem"].at[1]).wait()
    for c in (*one_way, *both):
        renew_early(c)
    for c in one_way:
        forward[c].arrived()
        renew_late(c)
    for c in both:
        for k in corner[c]:
            k.arrived()
        renew_late(c)

    def early(x, _):
        for y0 in range(0, NY, 2):
            sides = []
            for y in (y0, y0 + 1):
                parts = []
                for a, o in BLOCKS:
                    dx, dy = (0, o) if a == 1 else (o, 0)
                    parts += [ub[x + H + dx, y + H + dy, c] for c in range(chunks)]
                sides.append(jnp.concatenate(parts, axis=0))
            out = jnp.dot(s["w_early"][...], jnp.concatenate(sides, axis=1), preferred_element_type=f32)
            for q in range(2):
                part = out[:, q * NZ:(q + 1) * NZ]
                acc[x, y0 + q, pl.ds(0, F)] = part[:F] + part[F:2 * F]
                acc[x, y0 + q, pl.ds(F, F)] = part[2 * F:]
        return 0

    lax.fori_loop(0, NX, early, 0, unroll=2)

    for r in rims_in:
        r.arrived()

    def along(x, _):
        ends_all = [
            jnp.where(
                lane % SLOT < SLOT // 2,
                jnp.where(above["gz"], rim_up[c, x * NY // slots], 0.0),
                jnp.where(below["gz"], rim_low[c, x * NY // slots], 0.0),
            )
            for c in range(chunks)
        ]
        for y0 in range(0, NY, 2):
            sides = []
            for y in (y0, y0 + 1):
                firsts, seconds = [], []
                for c in range(chunks):
                    u = box[x + H, y + H, rows[c]]
                    ends = pltpu.roll(ends_all[c], lax.rem(2 * NZ - SLOT * (x * NY % slots + y), NZ), 1)
                    d, t = {}, {}
                    for o in range(1, H + 1):
                        after = pltpu.roll(jnp.where(lane < o, ends, u), NZ - o, 1)
                        before = pltpu.roll(jnp.where(lane >= NZ - o, ends, u), o, 1)
                        d[o], t[o] = after - before, after + before
                    firsts.append(split16(8.0 * d[1] - d[2]))
                    seconds.append(split16(16.0 * t[1] - t[2]))
                    acc[x, y, pl.ds(F + c * ROWS, ROWS)] += t[3] - 6.0 * t[2] + 15.0 * t[1]
                sides.append(jnp.concatenate(firsts + seconds, axis=0))
            out = jnp.dot(s["w_along"][...], jnp.concatenate(sides, axis=1), preferred_element_type=f32)
            for q in range(2):
                part = out[:, q * NZ:(q + 1) * NZ]
                acc[x, y0 + q, pl.ds(0, F)] += part[:F] + part[F:]
        return 0

    lax.fori_loop(0, NX, along, 0, unroll=2)

    for a in range(2):
        n = SIDES.index((a, -1))
        inside[(a, -1)].arrived()
        pl.when(below[AXES[a]])(functools.partial(add_side, box, acc, acc, w_late, n))

    def finish(x, _):
        for y in range(NY - H):
            slope_ref[x * NY + y], value_ref[x * NY + y] = finished(box, acc, x, y)
        return 0

    lax.fori_loop(0, NX - H, finish, 0)

    for a in range(2):
        inside[(a, 1)].arrived()

        @pl.when(jnp.logical_not(above[AXES[a]]))
        def _(a=a):
            def step(i, _):
                for h in range(H):
                    at = (NX, NY)[a] + H + h
                    where = (at, i + H) if a == 0 else (i + H, at)
                    box[where] = jnp.zeros((F, NZ), f32)
                return 0

            lax.fori_loop(0, (NY, NX)[a], step, 0)

    for r in routes.values():
        r.all_sent()


def put_out(slope_in, value_in, acc_in, box, w_late, slope_hbm, value_hbm, slope_rest, value_rest, acc, sem):
    NX, NY = acc_in.shape[:2]
    sources = ((slope_in, slope_rest, slope_hbm), (value_in, value_rest, value_hbm))

    def send(x, y, rest):
        k = x * NY + y
        for n, source in enumerate(sources):
            pltpu.make_async_copy(source[rest].at[k], source[2].at[:, k], sem.at[n]).start()

    def send_inner(x, _):
        for y in range(NY - H):
            send(x, y, 0)
        return 0

    lax.fori_loop(0, NX - H, send_inner, 0)
    add_side(box, acc_in, acc, w_late, SIDES.index((0, 1)))
    add_side(box, acc_in, acc, w_late, SIDES.index((1, 1)), lambda x, y: x >= NX - H)

    def finish(x, y):
        k = x * NY + y
        slope_rest[k], value_rest[k] = finished(box, acc, x, y)

    def right(x, _):
        for y in range(NY - H, NY):
            finish(x, y)
            send(x, y, 1)
        return 0

    def low(x, _):
        for y in range(NY):
            finish(x, y)
            send(x, y, 1)
        return 0

    lax.fori_loop(0, NX - H, right, 0)
    lax.fori_loop(NX - H, NX, low, 0)
    for n in range(2):
        pltpu.make_async_copy(slope_rest, value_rest, sem.at[n]).wait()


def local(fields_now, parent, advect, diffuse, box_shift):
    dims = fields_now.shape
    F, NX, NY, NZ = dims
    flat = (F, NX * NY, NZ)
    by_cell = (NX * NY, F, NZ)
    vmem = pl.BlockSpec(memory_space=pltpu.VMEM)
    hbm = pl.BlockSpec(memory_space=pltpu.HBM)
    operands = [
        pltpu.with_memory_space_constraint(x, pltpu.HBM)
        for x in (box_shift, fields_now.reshape(flat), parent.reshape(flat), advect, diffuse, jnp.asarray(coefficients(F)))
    ]
    held = [
        pltpu.VMEM((NX, NY, 2 * F, NZ), f32),
        pltpu.VMEM((NX + 2 * H, NY + 2 * H, F, NZ), f32),
        pltpu.VMEM((len(SIDES), 4 * F, 4 * F), bf16),
    ]
    results = pl.pallas_call(
        functools.partial(kernel, dims),
        out_shape=[pltpu.VMEM(by_cell, f32)] * 2 + held,
        in_specs=[hbm] * 6,
        out_specs=[vmem] * 5,
        scratch_shapes=list(scratch(dims).values()),
        compiler_params=pltpu.CompilerParams(
            collective_id=0, has_side_effects=True, vmem_limit_bytes=VMEM_BYTES
        ),
    )(*operands)
    slope, value = pl.pallas_call(
        put_out,
        out_shape=[jax.ShapeDtypeStruct(flat, f32)] * 2,
        in_specs=[vmem] * 5,
        out_specs=[hbm] * 2,
        scratch_shapes=[pltpu.VMEM(by_cell, f32)] * 2 + [held[0], pltpu.SemaphoreType.DMA((2,))],
        compiler_params=pltpu.CompilerParams(vmem_limit_bytes=VMEM_BYTES),
    )(*results)
    return slope.reshape(dims), value.reshape(dims)


VMEM_BYTES = 40 * 2**20


def solution(mesh):
    return jax.shard_map(
        local,
        mesh=mesh,
        in_specs=(P(None, "gx", "gy", "gz"), P(None, "gx", "gy", "gz"), P(), P(), P()),
        out_specs=(P(None, "gx", "gy", "gz"), P(None, "gx", "gy", "gz")),
        check_vma=False,
    )
```

```python
import functools

import jax
import jax.numpy as jnp
import numpy as np
from jax import lax
from jax.experimental import pallas as pl
from jax.experimental.pallas import tpu as pltpu
from jax.sharding import PartitionSpec as P

MESH = pl.DeviceIdType.MESH
W = 4
H = 3
SLOT = 8
ROWS = 8
AXES = ("gx", "gy", "gz")
KINDS = ("x", "y", "xy")
ARRIVALS = {"x": 5, "y": 5, "xy": 7}
ROUTES = 8
FIRST = {-2: 1, -1: -8, 1: 8, 2: -1}
SECOND = {-2: -1, -1: 16, 0: -30, 1: 16, 2: -1}
SIXTH = {-3: 1, -2: -6, -1: 15, 0: -20, 1: 15, 2: -6, 3: 1}
BLOCKS = [(None, 0)] + [(a, o) for a in range(2) for o in (-2, -1, 1, 2)]
ALONG = [(2, "first"), (2, "second")]
SIDES = [(a, sign) for a in range(2) for sign in (-1, 1)]
f32, bf16 = jnp.float32, jnp.bfloat16


def up_to(n, m):
    return -(-n // m) * m


def block_columns(block, fields):
    cols = np.zeros((16, 2 * fields), np.float32)
    for c in range(fields // ROWS):
        for h in range(2):
            for r in range(ROWS):
                n = (c * 2 + h) * ROWS + r
                cols[7, n] = c * ROWS + r
                cols[8, n] = 1 - h
    if block is None:
        return cols
    axis, o = block
    if o in ("first", "second"):
        cols[axis + (3 if o == "second" else 0)] = 1
        return cols
    for a in range(3):
        if axis is None or a == axis:
            cols[a] = FIRST.get(o, 0)
            cols[3 + a] = SECOND.get(o, 0)
            cols[6] += SIXTH[o]
    return cols


def coefficients(fields):
    groups = [BLOCKS, ALONG]
    for a, sign in SIDES:
        groups += [[(a, sign), (a, 2 * sign)], [(a, 2 * sign), None]]
    out = []
    for g in groups:
        cols = np.concatenate([block_columns(b, fields) for b in g], axis=1)
        out.append(np.pad(cols, ((0, 0), (0, up_to(cols.shape[1], 256) - cols.shape[1]))))
    return np.concatenate(out, axis=1)


def band(length):
    out = np.zeros((2, length, 3, length), np.float32)
    for n, terms in enumerate((FIRST, SECOND, SIXTH)):
        for o, factor in terms.items():
            for lane in range(length):
                if o:
                    part, at = divmod(lane + o, length)
                    out[abs(part), at, n, lane] = factor
    return out.reshape(2 * length, 3 * length)


def scratch(dims):
    F, NX, NY, NZ = dims
    chunks = F // ROWS
    groups = NX * NY * SLOT // NZ
    tile = (ROWS, NZ)
    out = dict(
        shift=pltpu.SMEM((3,), jnp.int32),
        own=pltpu.VMEM((NX, NY, F, NZ), f32),
        par=pltpu.VMEM((NX, NY, F, NZ), f32),
        advect=pltpu.VMEM((3, F, F), f32),
        diffuse=pltpu.VMEM((3, F, F), f32),
        coef=pltpu.VMEM(coefficients(F).shape, f32),
        band=pltpu.VMEM((2 * NZ, 3 * NZ), bf16),
        w_early=pltpu.VMEM((3 * F, len(BLOCKS) * 2 * F), bf16),
        w_along=pltpu.VMEM((2 * F, len(ALONG) * 2 * F), bf16),
        ub=pltpu.VMEM((NX + 2 * H, NY + 2 * H, chunks, 2 * ROWS, NZ), bf16),
        rim=pltpu.VMEM((chunks, groups) + tile, f32),
        rim_up=pltpu.VMEM((chunks, groups) + tile, f32),
        rim_low=pltpu.VMEM((chunks, groups) + tile, f32),
        epk=pltpu.VMEM((chunks, 3) + tile, f32),
        ein=pltpu.VMEM((chunks, 4) + tile, f32),
    )
    for c in range(chunks):
        kind = KINDS[c % 3]
        if "x" in kind:
            out[f"rawx{c}"] = pltpu.VMEM((W, NY) + tile, f32)
        if "y" in kind:
            out[f"rawy{c}"] = pltpu.VMEM((NX, W) + tile, f32)
        ext = (W if "x" in kind else 0, W if "y" in kind else 0)
        out[f"zs{c}"] = pltpu.VMEM((NX + ext[0], NY + ext[1]) + tile, f32)
        if kind == "xy":
            out[f"ce{c}"] = pltpu.VMEM((W, W) + tile, f32)
        else:
            size = (NX, W) if kind == "x" else (W, NY)
            out[f"fw{c}"] = pltpu.VMEM(size + tile, f32)
            out[f"te{c}"] = pltpu.VMEM(size + tile, f32)
    out["count"] = pltpu.VMEM((chunks * 8 * NX * NY,) + tile, f32)
    n = sum(ARRIVALS[KINDS[c % 3]] for c in range(chunks)) + len(SIDES) + 2
    out["send_sem"] = pltpu.SemaphoreType.DMA((ROUTES,))
    out["recv_sem"] = pltpu.SemaphoreType.DMA((n,))
    out["load_sem"] = pltpu.SemaphoreType.DMA((7,))
    return out


def split16(u):
    low = u - u.astype(bf16).astype(f32)
    return jnp.concatenate([u, low], axis=0).astype(bf16)


def add_side(box, acc, out_acc, w_late, n, again=None):
    a, sign = SIDES[n]
    NX, NY, F, NZ = acc.shape[0], acc.shape[1], acc.shape[2] // 2, acc.shape[3]
    length, across = ((NX, NY), (NY, NX))[a]
    linear_rows, smooth_rows = pl.ds(0, F), pl.ds(F, F)

    def spot(depth, i):
        at = length - 1 - depth if sign > 0 else depth
        return (at, i) if a == 0 else (i, at)

    for i0 in range(0, across, 2):
        columns, smooth = [], []
        for i in (i0, i0 + 1):
            near = []
            for h in range(1, H + 1):
                x, y = spot(-h, i)
                near.append(box[x + H, y + H])
            smooth.append((15.0 * near[0] - 6.0 * near[1] + near[2], near[1] - 6.0 * near[0], near[0]))
            parts = [split16(u[c:c + ROWS]) for u in near[:2] for c in range(0, F, ROWS)]
            columns.append(jnp.concatenate(parts, axis=0))
        out = jnp.dot(w_late[n], jnp.concatenate(columns, axis=1), preferred_element_type=f32)
        for q in range(2):
            part = out[:, q * NZ:(q + 1) * NZ]
            for d in range(H):
                x, y = spot(d, i0 + q)
                source = out_acc if again is not None and again(x, y) else acc
                linear = source[x, y, linear_rows]
                if d < 2:
                    mine = part[2 * F * d:2 * F * (d + 1)]
                    linear = linear + (mine[:F] + mine[F:])
                out_acc[x, y, linear_rows] = linear
                out_acc[x, y, smooth_rows] = source[x, y, smooth_rows] + smooth[q][d]


def finished(box, acc, x, y):
    u = box[x + H, y + H]
    F = u.shape[0]
    lapse = (1.0 + 0.25 * jnp.tanh(u[0:1])) * (1.0 / 12.0)
    slope = lapse * acc[x, y, pl.ds(0, F)] + acc[x, y, pl.ds(F, F)] * (1.0 / 64.0)
    return slope, u + 0.125 * slope


def kernel(
    dims, shift_hbm, now_hbm, parent_hbm, advect_hbm, diffuse_hbm, coef_hbm, band_hbm,
    slope_ref, value_ref, acc, box, w_late, *refs
):
    F, NX, NY, NZ = dims
    chunks = F // ROWS
    cells = NX * NY
    s = dict(zip(scratch(dims), refs))
    own, par, ub = s["own"], s["par"], s["ub"]
    epk, ein, rim, rim_up, rim_low = s["epk"], s["ein"], s["rim"], s["rim_up"], s["rim_low"]
    slots = NZ // SLOT
    groups = cells // slots
    me = {a: lax.axis_index(a) for a in AXES}
    size = {a: lax.axis_size(a) for a in AXES}
    below = {a: me[a] > 0 for a in AXES}
    above = {a: me[a] < size[a] - 1 for a in AXES}
    sems = iter(range(1000))
    kinds = [KINDS[c % 3] for c in range(chunks)]
    rows = [pl.ds(c * ROWS, ROWS) for c in range(chunks)]

    def load_cells(src, dst, n):
        def step(x, _):
            for y in range(NY):
                pltpu.make_async_copy(src.at[:, x * NY + y], dst.at[x, y], s["load_sem"].at[n]).start()
            return 0

        lax.fori_loop(0, NX, step, 0)

    singles = [
        pltpu.make_async_copy(src, dst, s["load_sem"].at[2 + n])
        for n, (src, dst) in enumerate((
            (shift_hbm, s["shift"]), (advect_hbm, s["advect"]),
            (diffuse_hbm, s["diffuse"]), (coef_hbm, s["coef"]), (band_hbm, s["band"]),
        ))
    ]
    DX, DY, DZ = {"gx": -1}, {"gy": -1}, {"gz": -1}
    UX, UY, UZ = {"gx": 1}, {"gy": 1}, {"gz": 1}
    barrier = pltpu.get_barrier_semaphore()
    count = 0
    for to in (DX, UX, DY, UY, DZ, UZ, UX | UZ, UY | UZ):
        cond = back = None
        for a, by in to.items():
            one, two = (below[a], above[a]) if by < 0 else (above[a], below[a])
            cond = one if cond is None else cond & one
            back = two if back is None else back & two

        @pl.when(cond)
        def _(to=to):
            pl.semaphore_signal(
                barrier, inc=1, device_id={a: me[a] + by for a, by in to.items()}, device_id_type=MESH
            )
        count = count + jnp.where(back, 1, 0)

    singles[0].start()
    load_cells(now_hbm, own, 0)
    pl.semaphore_wait(barrier, count)

    routes = {}

    class Route:
        def __init__(self, to):
            self.to = to
            self.send_sem = s["send_sem"].at[len(routes)]
            self.tiles = 0
            self.sends = self.gets = None
            for a, by in to.items():
                sends = below[a] if by < 0 else above[a]
                gets = above[a] if by < 0 else below[a]
                self.sends = sends if self.sends is None else self.sends & sends
                self.gets = gets if self.gets is None else self.gets & gets

        def copy(self, src, dst, recv_sem):
            return pltpu.make_async_remote_copy(
                src_ref=src, dst_ref=dst, send_sem=self.send_sem, recv_sem=recv_sem,
                device_id={a: me[a] + by for a, by in self.to.items()}, device_id_type=MESH,
            )

        def all_sent(self):
            done = s["count"].at[pl.ds(0, self.tiles)]
            pl.when(self.sends)(self.copy(done, done, s["recv_sem"].at[0]).wait_send)

    def route(to):
        key = tuple(sorted(to.items()))
        if key not in routes:
            routes[key] = Route(to)
        return routes[key]

    class Arrival:
        def __init__(self, to):
            self.route = route(to)
            self.recv_sem = s["recv_sem"].at[next(sems)]
            self.tiles = 0

        def arrived(self):
            done = s["count"].at[pl.ds(0, self.tiles)]
            pl.when(self.route.gets)(self.route.copy(done, done, self.recv_sem).wait_recv)

    def size_of(ref):
        return int(np.prod(ref.shape)) // (ROWS * NZ)

    class Message:
        def __init__(self, src, dst, to, arrival=None, parts=None):
            self.arrival = arrival or Arrival(to)
            self.route = route(to)
            tiles = size_of(dst)
            self.arrival.tiles += tiles
            self.route.tiles += tiles
            self.src, self.dst, self.parts = src, dst, parts

        def start(self):
            pl.when(self.route.sends)(self.route.copy(self.src, self.dst, self.arrival.recv_sem).start)

        def start_parts(self, i):
            @pl.when(self.route.sends)
            def _():
                for j in range(W):
                    self.route.copy(*self.parts(i, j), self.arrival.recv_sem).start()

        def arrived(self):
            self.arrival.arrived()

    message = Message

    lowx, lowy = pl.ds(0, W), pl.ds(0, W)
    raw, edge, diag, forward, corner = {}, {}, {}, {}, {}
    for c, kind in enumerate(kinds):
        if kind == "x":
            def cell(i, j, half, c=c):
                x, y = i, j + half * (NY // 2)
                return now_hbm.at[rows[c], x * NY + y], s[f"rawx{c}"].at[x, y]

            halves = [s[f"rawx{c}"].at[:, pl.ds(h * (NY // 2), NY // 2)] for h in range(2)]
            raw[c] = [message(r, r, DX, parts=functools.partial(cell, half=h)) for h, r in enumerate(halves)]
            diag[c] = [message(epk.at[c, 0], ein.at[c, 2], DX | DZ)]
            forward[c] = message(s[f"fw{c}"], s[f"te{c}"], DY)
        elif kind == "y":
            def cell(i, j, half, c=c):
                x, y = i + half * (NX // 2), j
                return now_hbm.at[rows[c], x * NY + y], s[f"rawy{c}"].at[x, y]

            halves = [s[f"rawy{c}"].at[pl.ds(h * (NX // 2), NX // 2)] for h in range(2)]
            raw[c] = [message(r, r, DY, parts=functools.partial(cell, half=h)) for h, r in enumerate(halves)]
            diag[c] = [message(epk.at[c, 0], ein.at[c, 2], DY | DZ)]
            forward[c] = message(s[f"fw{c}"], s[f"te{c}"], DX)
        else:
            raw[c] = [
                message(own.at[lowx, :, rows[c]], s[f"rawx{c}"], DX),
                message(own.at[:, lowy, rows[c]], s[f"rawy{c}"], DY),
            ]
            diag[c] = [
                message(epk.at[c, 0], ein.at[c, 2], DX | DZ), message(epk.at[c, 2], ein.at[c, 3], DY | DZ),
            ]
            near, far = pl.ds(0, W // 2), pl.ds(W // 2, W // 2)
            zs, ce = s[f"zs{c}"], s[f"ce{c}"]
            corner[c] = [
                message(zs.at[far, pl.ds(NY, W)], ce.at[far], DX),
                message(zs.at[pl.ds(NX, W // 2), lowy], ce.at[near], DY),
            ]
        edge[c] = message(epk.at[c, pl.ds(0, 2)], ein.at[c, pl.ds(0, 2)], DZ)

    inside = {(a, sign): Arrival({AXES[a]: -sign}) for a, sign in SIDES}
    rims_in = [Arrival(DZ), Arrival(UZ)]

    def halo(c, a, by, lo, hi):
        n = (NX, NY)[a]
        src = pl.ds(H, H) if by < 0 else pl.ds(n, H)
        dst = pl.ds(n + H, H) if by < 0 else pl.ds(0, H)
        span = pl.ds(H + lo, hi - lo)
        to = {AXES[a]: by}
        if a == 0:
            return message(box.at[src, span, rows[c]], box.at[dst, span, rows[c]], to, inside[(a, -by)])
        return message(box.at[span, src, rows[c]], box.at[span, dst, rows[c]], to, inside[(a, -by)])

    early_halo, late_halo, rims = {}, {}, {}
    hx, hy = NX // 2, NY // 2
    for c, kind in enumerate(kinds):
        if kind == "x":
            early_halo[c] = [halo(c, 1, -1, 0, NX), halo(c, 0, 1, 0, hy)]
            late_halo[c] = [halo(c, 0, -1, 0, NY), halo(c, 0, 1, hy, NY), halo(c, 1, 1, 0, NX)]
        elif kind == "y":
            early_halo[c] = [halo(c, 0, -1, 0, NY), halo(c, 1, 1, 0, hx)]
            late_halo[c] = [halo(c, 1, -1, 0, NX), halo(c, 1, 1, hx, NX), halo(c, 0, 1, 0, NY)]
        else:
            early_halo[c] = [halo(c, 0, -1, 0, NY), halo(c, 1, -1, 0, NX), halo(c, 0, 1, 0, hy), halo(c, 1, 1, 0, hx)]
            late_halo[c] = [halo(c, 0, 1, hy, NY), halo(c, 1, 1, hx, NX)]
        rims[c] = [
            message(rim.at[c], rim_up.at[c], DZ, rims_in[0]), message(rim.at[c], rim_low.at[c], UZ, rims_in[1]),
        ]

    def send_raw(i, _, half):
        for c, kind in enumerate(kinds):
            if kind != "xy":
                raw[c][half].start_parts(i)
        return 0

    def send_raws(half, lo, hi):
        lax.fori_loop(lo, hi, functools.partial(send_raw, half=half), 0)

    send_raws(0, 0, W)
    send_raws(1, 0, W // 2)

    lane = lax.broadcasted_iota(jnp.int32, (ROWS, NZ), 1)
    thin = lane // W
    wide = ((lane + SLOT // 2) % NZ) // SLOT
    blank = jnp.zeros((ROWS, NZ), f32)

    def pack(c, n, along, q):
        packed = blank
        across = NY if along == "x" else NX
        for slot in range(W * across):
            i, j = q * W + slot // across, slot % across
            x, y = (i, j) if along == "x" else (j, i)
            packed = jnp.where(thin == slot, pltpu.roll(own[x, y, rows[c]], W * slot, 1), packed)
        epk[c, n] = packed

    pltpu.make_async_copy(par, own, s["load_sem"].at[0]).wait()
    one_way = [c for c in range(chunks) if kinds[c] != "xy"]
    both = [c for c in range(chunks) if kinds[c] == "xy"]
    for c in one_way:
        pack(c, 0, kinds[c], 0)
        diag[c][0].start()
    send_raws(1, W // 2, W)
    for c in one_way:
        pack(c, 1, kinds[c], 1)
        edge[c].start()
    for c in both:
        pack(c, 0, "x", 0)
        pack(c, 2, "y", 0)
        for d in diag[c]:
            d.start()
        for r in raw[c]:
            r.start()
        pack(c, 1, "x", 1)
        edge[c].start()

    for load in singles[1:]:
        load.start()
    load_cells(parent_hbm, par, 1)
    zero16 = jnp.zeros((2 * ROWS, NZ), bf16)

    def clear(i, _):
        for c in range(chunks):
            for o in range(H):
                ub[o, i + H, c] = zero16
                ub[NX + H + o, i + H, c] = zero16
                ub[i + H, o, c] = zero16
                ub[i + H, NY + H + o, c] = zero16
        return 0

    lax.fori_loop(0, NX, clear, 0)

    singles[0].wait()
    move = [s["shift"][d] for d in range(3)]
    sz = move[2]

    def weights():
        for load in singles[1:]:
            load.wait()
        mats = []
        for m in (s["advect"], s["diffuse"]):
            for a in range(3):
                one = m[a]
                high = one.astype(bf16).astype(f32)
                mid = (one - high).astype(bf16).astype(f32)
                mats.append(jnp.concatenate([high, mid, one - high - mid], axis=0).astype(bf16))

        def columns(at, width, ks):
            table = s["coef"][:, at:at + width]
            hit = lax.broadcasted_iota(jnp.int32, (F, width), 0).astype(f32) == table[7:8]
            smooth = jnp.where(hit, table[6:7], 0.0)
            total = None
            for k in ks:
                spread = jnp.where(hit, table[k:k + 1], 0.0).astype(bf16)
                part = jnp.dot(mats[k], spread, preferred_element_type=f32)
                total = part if total is None else total + part
            w = total[:F] + total[F:2 * F] + total[2 * F:]
            high = w.astype(bf16).astype(f32)
            return jnp.concatenate([high, (w - high) * table[8:9], smooth], axis=0)

        k_early = len(BLOCKS) * 2 * F
        for at in range(0, up_to(k_early, 256), 256):
            n = min(256, k_early - at)
            s["w_early"][:, at:at + n] = columns(at, 256, range(6))[:, :n].astype(bf16)
        at = up_to(k_early, 256)
        k_along = len(ALONG) * 2 * F
        s["w_along"][...] = columns(at, up_to(k_along, 256), (2, 5))[:2 * F, :k_along].astype(bf16)
        at += up_to(k_along, 256)
        k_late = 2 * 2 * F
        step = up_to(k_late, 256)
        for n, (a, sign) in enumerate(SIDES):
            parts = [columns(at + d * step, step, (a, 3 + a))[:2 * F] for d in range(2)]
            w_late[n] = jnp.concatenate(parts, axis=0)[:, :k_late].astype(bf16)
            at += 2 * step

    def z_row(row, packed, slot):
        tail = pltpu.roll(packed, NZ - W * slot - sz, 1)
        return jnp.where(lane >= NZ - sz, tail, pltpu.roll(row, NZ - sz, 1))

    def z_own(c, xs, ys):
        kind = kinds[c]
        for x in range(*xs):
            for y in range(*ys):
                q, slot = (x // W, x % W * NY + y) if "x" in kind else (y // W, y % W * NX + x)
                s[f"zs{c}"][x, y] = z_row(own[x, y, rows[c]], ein[c, q], slot)

    def z_ext_x(c, lo, hi):
        for x in range(W):
            for y in range(lo, hi):
                s[f"zs{c}"][NX + x, y] = z_row(s[f"rawx{c}"][x, y], ein[c, 2], x * NY + y)

    def z_ext_y(c, lo, hi):
        n = 3 if kinds[c] == "xy" else 2
        for x in range(lo, hi):
            for y in range(W):
                s[f"zs{c}"][x, NY + y] = z_row(s[f"rawy{c}"][x, y], ein[c, n], y * NX + x)

    def make_forward(c):
        zs, fw = s[f"zs{c}"], s[f"fw{c}"]

        def step(i, _):
            for j in range(W):
                if kinds[c] == "x":
                    fw[i, j] = zs[i + move[0], j]
                else:
                    fw[j, i] = zs[j, i + move[1]]
            return 0

        lax.fori_loop(0, NX if kinds[c] == "x" else NY, step, 0)

    in_z = me["gz"] * NZ + lane + sz < size["gz"] * NZ

    def renew(c, xs, ys, late):
        kind, zs = kinds[c], s[f"zs{c}"]

        def step(x, _):
            in_x = me["gx"] * NX + x + move[0] < size["gx"] * NX
            for y in range(*ys):
                in_y = me["gy"] * NY + y + move[1] < size["gy"] * NY
                X, Y = x + move[0], y + move[1]
                if not late:
                    row = zs[X, Y]
                elif kind == "x":
                    row = jnp.where(Y < NY, zs[X, jnp.minimum(Y, NY - 1)], s[f"te{c}"][x, jnp.maximum(Y - NY, 0)])
                elif kind == "y":
                    row = jnp.where(X < NX, zs[jnp.minimum(X, NX - 1), Y], s[f"te{c}"][jnp.maximum(X - NX, 0), y])
                else:
                    row = jnp.where(
                        (X < NX) | (Y < NY), zs[X, Y],
                        s[f"ce{c}"][jnp.maximum(X - NX, 0), jnp.maximum(Y - NY, 0)],
                    )
                row = jnp.where(in_z & (in_x & in_y), row, par[x, y, rows[c]])
                box[x + H, y + H, rows[c]] = row
                ub[x + H, y + H, c] = split16(row)
            return 0

        lax.fori_loop(*xs, step, 0)

    def renew_early(c):
        if kinds[c] == "x":
            renew(c, (0, NX), (0, hy), False)
        elif kinds[c] == "y":
            renew(c, (0, hx), (0, NY), False)
        else:
            renew(c, (0, hx), (0, NY), False)
            renew(c, (hx, NX), (0, hy), False)
        for h in early_halo[c]:
            h.start()

    def renew_late(c):
        if kinds[c] == "x":
            renew(c, (0, NX), (hy, NY), True)
        elif kinds[c] == "y":
            renew(c, (hx, NX), (0, NY), True)
        else:
            renew(c, (hx, NX), (hy, NY), True)
        for h in late_halo[c]:
            h.start()

        for g in range(groups):
            packed = blank
            for j in range(slots):
                x, y = g * (slots // NY) + j // NY, j % NY
                packed = jnp.where(wide == j, pltpu.roll(box[x + H, y + H, rows[c]], SLOT * j, 1), packed)
            rim[c, g] = packed
        for r in rims[c]:
            r.start()

    for c in one_way:
        edge[c].arrived()
        z_own(c, (0, NX if kinds[c] == "x" else hx), (0, NY if kinds[c] == "y" else hy))
    for c in one_way:
        diag[c][0].arrived()
        raw[c][0].arrived()
        if kinds[c] == "x":
            z_ext_x(c, 0, hy)
        else:
            z_ext_y(c, 0, hx)
        make_forward(c)
        forward[c].start()
    for c in one_way:
        z_own(c, (0 if kinds[c] == "x" else hx, NX), (0 if kinds[c] == "y" else hy, NY))
    for c in both:
        edge[c].arrived()
        z_own(c, (0, NX), (0, NY))
    for c in one_way:
        raw[c][1].arrived()
        if kinds[c] == "x":
            z_ext_x(c, hy, NY)
        else:
            z_ext_y(c, hx, NX)
    for c in both:
        for d in diag[c]:
            d.arrived()
        raw[c][0].arrived()
        z_ext_x(c, 0, NY)
        raw[c][1].arrived()
        z_ext_y(c, 0, NX)
        for k in corner[c]:
            k.start()
    pltpu.make_async_copy(own, par, s["load_sem"].at[1]).wait()
    for c in (*one_way, *both):
        renew_early(c)
    weights()
    for c in one_way:
        forward[c].arrived()
        renew_late(c)
    for c in both:
        for k in corner[c]:
            k.arrived()
        renew_late(c)

    def early(x):
        for y0 in range(0, NY, 2):
            sides = []
            for y in (y0, y0 + 1):
                parts = []
                for a, o in BLOCKS:
                    dx, dy = (0, o) if a == 1 else (o, 0)
                    parts += [ub[x + H + dx, y + H + dy, c] for c in range(chunks)]
                sides.append(jnp.concatenate(parts, axis=0))
            out = jnp.dot(s["w_early"][...], jnp.concatenate(sides, axis=1), preferred_element_type=f32)
            for q in range(2):
                part = out[:, q * NZ:(q + 1) * NZ]
                smooth = part[2 * F:]
                for o in (-H, H):
                    for u, v in ((x + o, y0 + q), (x, y0 + q + o)):
                        if 0 <= u < NX and 0 <= v < NY:
                            smooth = smooth + box[u + H, v + H]
                acc[x, y0 + q, pl.ds(0, F)] = part[:F] + part[F:2 * F]
                acc[x, y0 + q, pl.ds(F, F)] = smooth

    for x in range(NX):
        early(x)

    for r in rims_in:
        r.arrived()

    def along(g, _):
        ends_all = [
            jnp.where(
                lane % SLOT < SLOT // 2,
                jnp.where(above["gz"], rim_up[c, g], 0.0), jnp.where(below["gz"], rim_low[c, g], 0.0),
            )
            for c in range(chunks)
        ]
        per = slots // NY
        for i in range(per):
            x = g * per + i
            lines = []
            for y in range(NY):
                for c in range(chunks):
                    ends = pltpu.roll(ends_all[c], (NZ - SLOT * (i * NY + y)) % NZ, 1)
                    lines.append(jnp.concatenate([ub[x + H, y + H, c], split16(ends)], axis=1))
            spread = jnp.dot(jnp.concatenate(lines, axis=0), s["band"][...], preferred_element_type=f32)
            terms = [
                spread[n * 2 * ROWS:n * 2 * ROWS + ROWS] + spread[n * 2 * ROWS + ROWS:(n + 1) * 2 * ROWS]
                for n in range(NY * chunks)
            ]
            for y0 in range(0, NY, 2):
                sides = []
                for y in (y0, y0 + 1):
                    mine = terms[y * chunks:(y + 1) * chunks]
                    parts = [split16(t[:, n * NZ:(n + 1) * NZ]) for n in range(2) for t in mine]
                    sides.append(jnp.concatenate(parts, axis=0))
                    for c in range(chunks):
                        acc[x, y, pl.ds(F + c * ROWS, ROWS)] += mine[c][:, 2 * NZ:]
                out = jnp.dot(s["w_along"][...], jnp.concatenate(sides, axis=1), preferred_element_type=f32)
                for q in range(2):
                    part = out[:, q * NZ:(q + 1) * NZ]
                    acc[x, y0 + q, pl.ds(0, F)] += part[:F] + part[F:]
        return 0

    lax.fori_loop(0, groups, along, 0, unroll=4)

    for a in range(2):
        n = SIDES.index((a, -1))
        inside[(a, -1)].arrived()
        pl.when(below[AXES[a]])(functools.partial(add_side, box, acc, acc, w_late, n))

    def finish(x, _):
        for y in range(NY - H):
            slope_ref[x * NY + y], value_ref[x * NY + y] = finished(box, acc, x, y)
        return 0

    lax.fori_loop(0, NX - H, finish, 0)

    for a in range(2):
        inside[(a, 1)].arrived()

        @pl.when(jnp.logical_not(above[AXES[a]]))
        def _(a=a):
            def step(i, _):
                for h in range(H):
                    at = (NX, NY)[a] + H + h
                    where = (at, i + H) if a == 0 else (i + H, at)
                    box[where] = jnp.zeros((F, NZ), f32)
                return 0

            lax.fori_loop(0, (NY, NX)[a], step, 0)

    for r in routes.values():
        r.all_sent()


def put_out(slope_in, value_in, acc_in, box, w_late, slope_hbm, value_hbm, slope_rest, value_rest, acc, sem):
    NX, NY = acc_in.shape[:2]
    sources = ((slope_in, slope_rest, slope_hbm), (value_in, value_rest, value_hbm))

    def send(x, y, rest):
        k = x * NY + y
        for n, source in enumerate(sources):
            pltpu.make_async_copy(source[rest].at[k], source[2].at[:, k], sem.at[n]).start()

    def send_inner(x, _):
        for y in range(NY - H):
            send(x, y, 0)
        return 0

    lax.fori_loop(0, NX - H, send_inner, 0)
    add_side(box, acc_in, acc, w_late, SIDES.index((0, 1)))
    add_side(box, acc_in, acc, w_late, SIDES.index((1, 1)), lambda x, y: x >= NX - H)

    def finish(x, y):
        k = x * NY + y
        slope_rest[k], value_rest[k] = finished(box, acc, x, y)

    def right(x, _):
        for y in range(NY - H, NY):
            finish(x, y)
            send(x, y, 1)
        return 0

    def low(x, _):
        for y in range(NY):
            finish(x, y)
            send(x, y, 1)
        return 0

    lax.fori_loop(0, NX - H, right, 0)
    lax.fori_loop(NX - H, NX, low, 0)
    for n in range(2):
        pltpu.make_async_copy(slope_rest, value_rest, sem.at[n]).wait()


def local(fields_now, parent, advect, diffuse, box_shift):
    dims = fields_now.shape
    F, NX, NY, NZ = dims
    flat = (F, NX * NY, NZ)
    by_cell = (NX * NY, F, NZ)
    vmem = pl.BlockSpec(memory_space=pltpu.VMEM)
    hbm = pl.BlockSpec(memory_space=pltpu.HBM)
    operands = [
        pltpu.with_memory_space_constraint(x, pltpu.HBM)
        for x in (
            box_shift, fields_now.reshape(flat), parent.reshape(flat), advect, diffuse,
            jnp.asarray(coefficients(F)), jnp.asarray(band(NZ), bf16),
        )
    ]
    held = [
        pltpu.VMEM((NX, NY, 2 * F, NZ), f32),
        pltpu.VMEM((NX + 2 * H, NY + 2 * H, F, NZ), f32),
        pltpu.VMEM((len(SIDES), 4 * F, 4 * F), bf16),
    ]
    results = pl.pallas_call(
        functools.partial(kernel, dims),
        out_shape=[pltpu.VMEM(by_cell, f32)] * 2 + held,
        in_specs=[hbm] * len(operands),
        out_specs=[vmem] * 5,
        scratch_shapes=list(scratch(dims).values()),
        compiler_params=pltpu.CompilerParams(
            collective_id=0, has_side_effects=True, vmem_limit_bytes=VMEM_BYTES
        ),
    )(*operands)
    slope, value = pl.pallas_call(
        put_out,
        out_shape=[jax.ShapeDtypeStruct(flat, f32)] * 2,
        in_specs=[vmem] * 5,
        out_specs=[hbm] * 2,
        scratch_shapes=[pltpu.VMEM(by_cell, f32)] * 2 + [held[0], pltpu.SemaphoreType.DMA((2,))],
        compiler_params=pltpu.CompilerParams(vmem_limit_bytes=VMEM_BYTES),
    )(*results)
    return slope.reshape(dims), value.reshape(dims)


VMEM_BYTES = 40 * 2**20


def solution(mesh):
    return jax.shard_map(
        local,
        mesh=mesh,
        in_specs=(P(None, "gx", "gy", "gz"), P(None, "gx", "gy", "gz"), P(), P(), P()),
        out_specs=(P(None, "gx", "gy", "gz"), P(None, "gx", "gy", "gz")),
        check_vma=False,
    )
```

```python
import functools

import jax
import jax.numpy as jnp
import numpy as np
from jax import lax
from jax.experimental import pallas as pl
from jax.experimental.pallas import tpu as pltpu
from jax.sharding import PartitionSpec as P

MESH = pl.DeviceIdType.MESH
W = 4
H = 3
SLOT = 8
ROWS = 8
AXES = ("gx", "gy", "gz")
KINDS = ("x", "y", "split")
HALF = ROWS // 2
ARRIVALS = {"x": 5, "y": 5, "split": 7}
ROUTES = 8
FIRST = {-2: 1, -1: -8, 1: 8, 2: -1}
SECOND = {-2: -1, -1: 16, 0: -30, 1: 16, 2: -1}
SIXTH = {-3: 1, -2: -6, -1: 15, 0: -20, 1: 15, 2: -6, 3: 1}
BLOCKS = [(None, 0)] + [(a, o) for a in range(2) for o in (-2, -1, 1, 2)]
ALONG = [(2, "first"), (2, "second")]
SIDES = [(a, sign) for a in range(2) for sign in (-1, 1)]
f32, bf16 = jnp.float32, jnp.bfloat16


def up_to(n, m):
    return -(-n // m) * m


def block_columns(block, fields):
    cols = np.zeros((16, 2 * fields), np.float32)
    for c in range(fields // ROWS):
        for h in range(2):
            for r in range(ROWS):
                n = (c * 2 + h) * ROWS + r
                cols[7, n] = c * ROWS + r
                cols[8, n] = 1 - h
    if block is None:
        return cols
    axis, o = block
    if o in ("first", "second"):
        cols[axis + (3 if o == "second" else 0)] = 1
        return cols
    for a in range(3):
        if axis is None or a == axis:
            cols[a] = FIRST.get(o, 0)
            cols[3 + a] = SECOND.get(o, 0)
            cols[6] += SIXTH[o]
    return cols


def coefficients(fields):
    groups = [BLOCKS, ALONG]
    for a, sign in SIDES:
        groups += [[(a, sign), (a, 2 * sign)], [(a, 2 * sign), None]]
    out = []
    for g in groups:
        cols = np.concatenate([block_columns(b, fields) for b in g], axis=1)
        out.append(np.pad(cols, ((0, 0), (0, up_to(cols.shape[1], 256) - cols.shape[1]))))
    return np.concatenate(out, axis=1)


def band(length):
    out = np.zeros((2, length, 3, length), np.float32)
    for n, terms in enumerate((FIRST, SECOND, SIXTH)):
        for o, factor in terms.items():
            for lane in range(length):
                if o and 0 <= lane + o < length:
                    out[0, lane + o, n, lane] = factor
                at = (lane + SLOT // 2) % SLOT - SLOT // 2
                if (0 <= at + o < H and at < 0) or (-H <= at + o < 0 <= at):
                    out[1, (lane + o) % length, n, lane] = factor
    return out.reshape(2 * length, 3 * length)


def scratch(dims):
    F, NX, NY, NZ = dims
    chunks = F // ROWS
    groups = NX * NY * SLOT // NZ
    tile = (ROWS, NZ)
    out = dict(
        shift=pltpu.SMEM((3,), jnp.int32),
        own=pltpu.VMEM((NX, NY, F, NZ), f32),
        par=pltpu.VMEM((NX, NY, F, NZ), f32),
        advect=pltpu.VMEM((3, F, F), f32),
        diffuse=pltpu.VMEM((3, F, F), f32),
        coef=pltpu.VMEM(coefficients(F).shape, f32),
        band=pltpu.VMEM((2 * NZ, 3 * NZ), bf16),
        w_early=pltpu.VMEM((3 * F, len(BLOCKS) * 2 * F), bf16),
        w_along=pltpu.VMEM((2 * F, len(ALONG) * 2 * F), bf16),
        ub=pltpu.VMEM((NX + 2 * H, NY + 2 * H, chunks, 2 * ROWS, NZ), bf16),
        rim=pltpu.VMEM((chunks, groups) + tile, f32),
        rim_up=pltpu.VMEM((chunks, groups) + tile, f32),
        rim_low=pltpu.VMEM((chunks, groups) + tile, f32),
        epk=pltpu.VMEM((chunks, 3) + tile, f32),
        ein=pltpu.VMEM((chunks, 4) + tile, f32),
    )
    for c in range(chunks):
        kind = KINDS[c % 3]
        if kind != "y":
            out[f"rawx{c}"] = pltpu.VMEM((W, NY) + tile, f32)
        if kind != "x":
            out[f"rawy{c}"] = pltpu.VMEM((NX, W) + tile, f32)
        ext = (W if kind != "y" else 0, W if kind != "x" else 0)
        out[f"zs{c}"] = pltpu.VMEM((NX + ext[0], NY + ext[1]) + tile, f32)
        for way, size in (("x", (NX, W)), ("y", (W, NY))):
            if kind in (way, "split"):
                out[f"fw{way}{c}"] = pltpu.VMEM(size + tile, f32)
                out[f"te{way}{c}"] = pltpu.VMEM(size + tile, f32)
    out["count"] = pltpu.VMEM((chunks * 8 * NX * NY,) + tile, f32)
    n = sum(ARRIVALS[KINDS[c % 3]] for c in range(chunks)) + len(SIDES) + 2
    out["send_sem"] = pltpu.SemaphoreType.DMA((ROUTES,))
    out["recv_sem"] = pltpu.SemaphoreType.DMA((n,))
    out["load_sem"] = pltpu.SemaphoreType.DMA((7,))
    return out


def split16(u):
    low = u - u.astype(bf16).astype(f32)
    return jnp.concatenate([u, low], axis=0).astype(bf16)


def add_side(box, acc, out_acc, w_late, n, again=None):
    a, sign = SIDES[n]
    NX, NY, F, NZ = acc.shape[0], acc.shape[1], acc.shape[2] // 2, acc.shape[3]
    length, across = ((NX, NY), (NY, NX))[a]
    linear_rows, smooth_rows = pl.ds(0, F), pl.ds(F, F)

    def spot(depth, i):
        at = length - 1 - depth if sign > 0 else depth
        return (at, i) if a == 0 else (i, at)

    for i0 in range(0, across, 2):
        columns, smooth = [], []
        for i in (i0, i0 + 1):
            near = []
            for h in range(1, H + 1):
                x, y = spot(-h, i)
                near.append(box[x + H, y + H])
            smooth.append((15.0 * near[0] - 6.0 * near[1] + near[2], near[1] - 6.0 * near[0], near[0]))
            parts = [split16(u[c:c + ROWS]) for u in near[:2] for c in range(0, F, ROWS)]
            columns.append(jnp.concatenate(parts, axis=0))
        out = jnp.dot(w_late[n], jnp.concatenate(columns, axis=1), preferred_element_type=f32)
        for q in range(2):
            part = out[:, q * NZ:(q + 1) * NZ]
            for d in range(H):
                x, y = spot(d, i0 + q)
                source = out_acc if again is not None and again(x, y) else acc
                linear = source[x, y, linear_rows]
                if d < 2:
                    mine = part[2 * F * d:2 * F * (d + 1)]
                    linear = linear + (mine[:F] + mine[F:])
                out_acc[x, y, linear_rows] = linear
                out_acc[x, y, smooth_rows] = source[x, y, smooth_rows] + smooth[q][d]


def finished(box, acc, x, y):
    u = box[x + H, y + H]
    F = u.shape[0]
    lapse = (1.0 + 0.25 * jnp.tanh(u[0:1])) * (1.0 / 12.0)
    slope = lapse * acc[x, y, pl.ds(0, F)] + acc[x, y, pl.ds(F, F)] * (1.0 / 64.0)
    return slope, u + 0.125 * slope


def kernel(
    dims, shift_hbm, now_hbm, parent_hbm, advect_hbm, diffuse_hbm, coef_hbm, band_hbm,
    slope_ref, value_ref, acc, box, w_late, *refs
):
    F, NX, NY, NZ = dims
    chunks = F // ROWS
    cells = NX * NY
    s = dict(zip(scratch(dims), refs))
    own, par, ub = s["own"], s["par"], s["ub"]
    epk, ein, rim, rim_up, rim_low = s["epk"], s["ein"], s["rim"], s["rim_up"], s["rim_low"]
    slots = NZ // SLOT
    groups = cells // slots
    me = {a: lax.axis_index(a) for a in AXES}
    size = {a: lax.axis_size(a) for a in AXES}
    below = {a: me[a] > 0 for a in AXES}
    above = {a: me[a] < size[a] - 1 for a in AXES}
    sems = iter(range(1000))
    kinds = [KINDS[c % 3] for c in range(chunks)]
    rows = [pl.ds(c * ROWS, ROWS) for c in range(chunks)]

    def load_cells(src, dst, n):
        def step(x, _):
            for y in range(NY):
                pltpu.make_async_copy(src.at[:, x * NY + y], dst.at[x, y], s["load_sem"].at[n]).start()
            return 0

        lax.fori_loop(0, NX, step, 0)

    singles = [
        pltpu.make_async_copy(src, dst, s["load_sem"].at[2 + n])
        for n, (src, dst) in enumerate((
            (shift_hbm, s["shift"]), (advect_hbm, s["advect"]),
            (diffuse_hbm, s["diffuse"]), (coef_hbm, s["coef"]), (band_hbm, s["band"]),
        ))
    ]
    DX, DY, DZ = {"gx": -1}, {"gy": -1}, {"gz": -1}
    UX, UY, UZ = {"gx": 1}, {"gy": 1}, {"gz": 1}
    barrier = pltpu.get_barrier_semaphore()
    count = 0
    for to in (DX, UX, DY, UY, DZ, UZ, UX | UZ, UY | UZ):
        cond = back = None
        for a, by in to.items():
            one, two = (below[a], above[a]) if by < 0 else (above[a], below[a])
            cond = one if cond is None else cond & one
            back = two if back is None else back & two

        @pl.when(cond)
        def _(to=to):
            pl.semaphore_signal(
                barrier, inc=1, device_id={a: me[a] + by for a, by in to.items()}, device_id_type=MESH
            )
        count = count + jnp.where(back, 1, 0)

    singles[0].start()
    load_cells(now_hbm, own, 0)
    pl.semaphore_wait(barrier, count)

    routes = {}

    class Route:
        def __init__(self, to):
            self.to = to
            self.send_sem = s["send_sem"].at[len(routes)]
            self.tiles = 0
            self.sends = self.gets = None
            for a, by in to.items():
                sends = below[a] if by < 0 else above[a]
                gets = above[a] if by < 0 else below[a]
                self.sends = sends if self.sends is None else self.sends & sends
                self.gets = gets if self.gets is None else self.gets & gets

        def copy(self, src, dst, recv_sem):
            return pltpu.make_async_remote_copy(
                src_ref=src, dst_ref=dst, send_sem=self.send_sem, recv_sem=recv_sem,
                device_id={a: me[a] + by for a, by in self.to.items()}, device_id_type=MESH,
            )

        def all_sent(self):
            done = s["count"].at[pl.ds(0, self.tiles // 2)]
            pl.when(self.sends)(self.copy(done, done, s["recv_sem"].at[0]).wait_send)

    def route(to):
        key = tuple(sorted(to.items()))
        if key not in routes:
            routes[key] = Route(to)
        return routes[key]

    class Arrival:
        def __init__(self, to):
            self.route = route(to)
            self.recv_sem = s["recv_sem"].at[next(sems)]
            self.tiles = 0

        def arrived(self):
            done = s["count"].at[pl.ds(0, self.tiles // 2)]
            pl.when(self.route.gets)(self.route.copy(done, done, self.recv_sem).wait_recv)

    def size_of(ref):
        return int(np.prod(ref.shape)) // (HALF * NZ)

    class Message:
        def __init__(self, src, dst, to, arrival=None, parts=None):
            self.arrival = arrival or Arrival(to)
            self.route = route(to)
            tiles = size_of(dst)
            self.arrival.tiles += tiles
            self.route.tiles += tiles
            self.src, self.dst, self.parts = src, dst, parts

        def start(self):
            pl.when(self.route.sends)(self.route.copy(self.src, self.dst, self.arrival.recv_sem).start)

        def start_parts(self, i):
            @pl.when(self.route.sends)
            def _():
                for j in range(W):
                    self.route.copy(*self.parts(i, j), self.arrival.recv_sem).start()

        def arrived(self):
            self.arrival.arrived()

    message = Message

    lowx, lowy = pl.ds(0, W), pl.ds(0, W)
    raw, edge, diag, forward = {}, {}, {}, {}
    for c, kind in enumerate(kinds):
        if kind == "x":
            def cell(i, j, half, c=c):
                x, y = i, j + half * (NY // 2)
                return now_hbm.at[rows[c], x * NY + y], s[f"rawx{c}"].at[x, y]

            halves = [s[f"rawx{c}"].at[:, pl.ds(h * (NY // 2), NY // 2)] for h in range(2)]
            raw[c] = [message(r, r, DX, parts=functools.partial(cell, half=h)) for h, r in enumerate(halves)]
            diag[c] = [message(epk.at[c, 0], ein.at[c, 2], DX | DZ)]
            forward[c] = [message(s[f"fwx{c}"], s[f"tex{c}"], DY)]
        elif kind == "y":
            def cell(i, j, half, c=c):
                x, y = i + half * (NX // 2), j
                return now_hbm.at[rows[c], x * NY + y], s[f"rawy{c}"].at[x, y]

            halves = [s[f"rawy{c}"].at[pl.ds(h * (NX // 2), NX // 2)] for h in range(2)]
            raw[c] = [message(r, r, DY, parts=functools.partial(cell, half=h)) for h, r in enumerate(halves)]
            diag[c] = [message(epk.at[c, 0], ein.at[c, 2], DY | DZ)]
            forward[c] = [message(s[f"fwy{c}"], s[f"tey{c}"], DX)]
        else:
            a_rows, b_rows = pl.ds(0, HALF), pl.ds(HALF, HALF)
            raw[c] = [
                message(own.at[lowx, :, pl.ds(c * ROWS, HALF)], s[f"rawx{c}"].at[:, :, a_rows], DX),
                message(own.at[:, lowy, pl.ds(c * ROWS + HALF, HALF)], s[f"rawy{c}"].at[:, :, b_rows], DY),
            ]
            diag[c] = [
                message(epk.at[c, 0], ein.at[c, 2], DX | DZ), message(epk.at[c, 2], ein.at[c, 3], DY | DZ),
            ]
            forward[c] = [
                message(s[f"fwx{c}"].at[:, :, a_rows], s[f"tex{c}"].at[:, :, a_rows], DY),
                message(s[f"fwy{c}"].at[:, :, b_rows], s[f"tey{c}"].at[:, :, b_rows], DX),
            ]
        edge[c] = message(epk.at[c, pl.ds(0, 2)], ein.at[c, pl.ds(0, 2)], DZ)

    inside = {(a, sign): Arrival({AXES[a]: -sign}) for a, sign in SIDES}
    rims_in = [Arrival(DZ), Arrival(UZ)]

    def halo(c, a, by, lo, hi, part=None):
        fields = rows[c] if part is None else pl.ds(c * ROWS + part * HALF, HALF)
        n = (NX, NY)[a]
        src = pl.ds(H, H) if by < 0 else pl.ds(n, H)
        dst = pl.ds(n + H, H) if by < 0 else pl.ds(0, H)
        span = pl.ds(H + lo, hi - lo)
        to = {AXES[a]: by}
        if a == 0:
            return message(box.at[src, span, fields], box.at[dst, span, fields], to, inside[(a, -by)])
        return message(box.at[span, src, fields], box.at[span, dst, fields], to, inside[(a, -by)])

    early_halo, late_halo, rims = {}, {}, {}
    hx, hy = NX // 2, NY // 2
    for c, kind in enumerate(kinds):
        if kind == "x":
            early_halo[c] = [halo(c, 1, -1, 0, NX), halo(c, 0, 1, 0, hy)]
            late_halo[c] = [halo(c, 0, -1, 0, NY), halo(c, 0, 1, hy, NY), halo(c, 1, 1, 0, NX)]
        elif kind == "y":
            early_halo[c] = [halo(c, 0, -1, 0, NY), halo(c, 1, 1, 0, hx)]
            late_halo[c] = [halo(c, 1, -1, 0, NX), halo(c, 1, 1, hx, NX), halo(c, 0, 1, 0, NY)]
        else:
            early_halo[c] = [
                halo(c, 1, -1, 0, NX, 0), halo(c, 0, -1, 0, NY, 1), halo(c, 0, 1, 0, hy, 0), halo(c, 1, 1, 0, hx, 1),
            ]
            late_halo[c] = [
                halo(c, 0, -1, 0, NY, 0), halo(c, 1, -1, 0, NX, 1), halo(c, 0, 1, hy, NY, 0),
                halo(c, 1, 1, hx, NX, 1), halo(c, 0, 1, 0, NY, 1), halo(c, 1, 1, 0, NX, 0),
            ]
        rims[c] = [
            message(rim.at[c], rim_up.at[c], DZ, rims_in[0]), message(rim.at[c], rim_low.at[c], UZ, rims_in[1]),
        ]

    def send_raw(i, _, half):
        for c, kind in enumerate(kinds):
            if kind != "split":
                raw[c][half].start_parts(i)
        return 0

    def send_raws(half, lo, hi):
        lax.fori_loop(lo, hi, functools.partial(send_raw, half=half), 0)

    send_raws(0, 0, W)
    send_raws(1, 0, W // 2)

    lane = lax.broadcasted_iota(jnp.int32, (ROWS, NZ), 1)
    thin = lane // W
    wide = ((lane + SLOT // 2) % NZ) // SLOT
    blank = jnp.zeros((ROWS, NZ), f32)

    def pack(c, n, along, q):
        packed = blank
        across = NY if along == "x" else NX
        for slot in range(W * across):
            i, j = q * W + slot // across, slot % across
            x, y = (i, j) if along == "x" else (j, i)
            packed = jnp.where(thin == slot, pltpu.roll(own[x, y, rows[c]], W * slot, 1), packed)
        epk[c, n] = packed

    pltpu.make_async_copy(par, own, s["load_sem"].at[0]).wait()
    one_way = [c for c in range(chunks) if kinds[c] != "split"]
    both = [c for c in range(chunks) if kinds[c] == "split"]
    for c in one_way:
        pack(c, 0, kinds[c], 0)
        diag[c][0].start()
    send_raws(1, W // 2, W)
    for c in one_way:
        pack(c, 1, kinds[c], 1)
        edge[c].start()
    for c in both:
        pack(c, 0, "x", 0)
        pack(c, 2, "y", 0)
        for d in diag[c]:
            d.start()
        for r in raw[c]:
            r.start()
        pack(c, 1, "x", 1)
        edge[c].start()

    for load in singles[1:]:
        load.start()
    load_cells(parent_hbm, par, 1)
    zero16 = jnp.zeros((2 * ROWS, NZ), bf16)

    def clear(i, _):
        for c in range(chunks):
            for o in range(H):
                ub[o, i + H, c] = zero16
                ub[NX + H + o, i + H, c] = zero16
                ub[i + H, o, c] = zero16
                ub[i + H, NY + H + o, c] = zero16
        return 0

    lax.fori_loop(0, NX, clear, 0)

    singles[0].wait()
    move = [s["shift"][d] for d in range(3)]
    sz = move[2]

    def weights():
        for load in singles[1:]:
            load.wait()
        mats = []
        for m in (s["advect"], s["diffuse"]):
            for a in range(3):
                one = m[a]
                high = one.astype(bf16).astype(f32)
                mid = (one - high).astype(bf16).astype(f32)
                mats.append(jnp.concatenate([high, mid, one - high - mid], axis=0).astype(bf16))

        def columns(at, width, ks):
            table = s["coef"][:, at:at + width]
            hit = lax.broadcasted_iota(jnp.int32, (F, width), 0).astype(f32) == table[7:8]
            smooth = jnp.where(hit, table[6:7], 0.0)
            total = None
            for k in ks:
                spread = jnp.where(hit, table[k:k + 1], 0.0).astype(bf16)
                part = jnp.dot(mats[k], spread, preferred_element_type=f32)
                total = part if total is None else total + part
            w = total[:F] + total[F:2 * F] + total[2 * F:]
            high = w.astype(bf16).astype(f32)
            return jnp.concatenate([high, (w - high) * table[8:9], smooth], axis=0)

        k_early = len(BLOCKS) * 2 * F
        for at in range(0, up_to(k_early, 256), 256):
            n = min(256, k_early - at)
            s["w_early"][:, at:at + n] = columns(at, 256, range(6))[:, :n].astype(bf16)
        at = up_to(k_early, 256)
        k_along = len(ALONG) * 2 * F
        s["w_along"][...] = columns(at, up_to(k_along, 256), (2, 5))[:2 * F, :k_along].astype(bf16)
        at += up_to(k_along, 256)
        k_late = 2 * 2 * F
        step = up_to(k_late, 256)
        for n, (a, sign) in enumerate(SIDES):
            parts = [columns(at + d * step, step, (a, 3 + a))[:2 * F] for d in range(2)]
            w_late[n] = jnp.concatenate(parts, axis=0)[:, :k_late].astype(bf16)
            at += 2 * step

    def z_row(row, packed, slot):
        tail = pltpu.roll(packed, NZ - W * slot - sz, 1)
        return jnp.where(lane >= NZ - sz, tail, pltpu.roll(row, NZ - sz, 1))

    def z_own(c, xs, ys):
        kind = kinds[c]
        for x in range(*xs):
            for y in range(*ys):
                q, slot = (x // W, x % W * NY + y) if kind != "y" else (y // W, y % W * NX + x)
                s[f"zs{c}"][x, y] = z_row(own[x, y, rows[c]], ein[c, q], slot)

    def z_ext_x(c, lo, hi):
        for x in range(W):
            for y in range(lo, hi):
                s[f"zs{c}"][NX + x, y] = z_row(s[f"rawx{c}"][x, y], ein[c, 2], x * NY + y)

    def z_ext_y(c, lo, hi):
        n = 3 if kinds[c] == "split" else 2
        for x in range(lo, hi):
            for y in range(W):
                s[f"zs{c}"][x, NY + y] = z_row(s[f"rawy{c}"][x, y], ein[c, n], y * NX + x)

    def make_forward(c):
        zs = s[f"zs{c}"]

        def step(i, _):
            for j in range(W):
                if kinds[c] != "y":
                    s[f"fwx{c}"][i, j] = zs[i + move[0], j]
                if kinds[c] != "x":
                    s[f"fwy{c}"][j, i] = zs[j, i + move[1]]
            return 0

        lax.fori_loop(0, NX, step, 0)
        for f in forward[c]:
            f.start()

    in_z = me["gz"] * NZ + lane + sz < size["gz"] * NZ

    upper = lax.broadcasted_iota(jnp.int32, (ROWS, NZ), 0) < HALF

    def renew(c, xs, ys, late, part=None, whole=True):
        kind, zs = kinds[c], s[f"zs{c}"]

        def step(x, _):
            in_x = me["gx"] * NX + x + move[0] < size["gx"] * NX
            for y in range(*ys):
                in_y = me["gy"] * NY + y + move[1] < size["gy"] * NY
                X, Y = x + move[0], y + move[1]
                if late:
                    if kind != "y":
                        x_first = jnp.where(
                            Y < NY, zs[X, jnp.minimum(Y, NY - 1)], s[f"tex{c}"][x, jnp.maximum(Y - NY, 0)]
                        )
                    if kind != "x":
                        y_first = jnp.where(
                            X < NX, zs[jnp.minimum(X, NX - 1), Y], s[f"tey{c}"][jnp.maximum(X - NX, 0), y]
                        )
                    row = x_first if kind == "x" else y_first
                    if kind == "split":
                        row = jnp.where(upper, x_first, y_first)
                else:
                    row = zs[X, Y]
                row = jnp.where(in_z & (in_x & in_y), row, par[x, y, rows[c]])
                if part is None:
                    box[x + H, y + H, rows[c]] = row
                else:
                    kept = slice(part * HALF, (part + 1) * HALF)
                    box[x + H, y + H, pl.ds(c * ROWS + part * HALF, HALF)] = row[kept]
                if whole:
                    ub[x + H, y + H, c] = split16(row)
            return 0

        lax.fori_loop(*xs, step, 0)

    def renew_early(c):
        if kinds[c] == "x":
            renew(c, (0, NX), (0, hy), False)
        elif kinds[c] == "y":
            renew(c, (0, hx), (0, NY), False)
        else:
            renew(c, (0, hx), (0, hy), False)
            renew(c, (hx, NX), (0, hy), False, 0, False)
            renew(c, (0, hx), (hy, NY), False, 1, False)
        for h in early_halo[c]:
            h.start()

    def renew_late(c):
        for f in forward[c]:
            f.arrived()
        if kinds[c] == "x":
            renew(c, (0, NX), (hy, NY), True)
        elif kinds[c] == "y":
            renew(c, (hx, NX), (0, NY), True)
        else:
            renew(c, (hx, NX), (0, hy), True, 1)
            renew(c, (0, hx), (hy, NY), True, 0)
            renew(c, (hx, NX), (hy, NY), True)
        for h in late_halo[c]:
            h.start()

        for g in range(groups):
            packed = blank
            for j in range(slots):
                x, y = g * (slots // NY) + j // NY, j % NY
                packed = jnp.where(wide == j, pltpu.roll(box[x + H, y + H, rows[c]], SLOT * j, 1), packed)
            rim[c, g] = packed
        for r in rims[c]:
            r.start()

    for c in one_way:
        edge[c].arrived()
        z_own(c, (0, NX if kinds[c] == "x" else hx), (0, NY if kinds[c] == "y" else hy))
    for c in one_way:
        diag[c][0].arrived()
        raw[c][0].arrived()
        if kinds[c] == "x":
            z_ext_x(c, 0, hy)
        else:
            z_ext_y(c, 0, hx)
        make_forward(c)
    for c in one_way:
        z_own(c, (0 if kinds[c] == "x" else hx, NX), (0 if kinds[c] == "y" else hy, NY))
    for c in both:
        edge[c].arrived()
        z_own(c, (0, NX), (0, NY))
    for c in one_way:
        raw[c][1].arrived()
        if kinds[c] == "x":
            z_ext_x(c, hy, NY)
        else:
            z_ext_y(c, hx, NX)
    for c in both:
        for d in diag[c]:
            d.arrived()
        raw[c][0].arrived()
        z_ext_x(c, 0, NY)
        raw[c][1].arrived()
        z_ext_y(c, 0, NX)
        make_forward(c)
    pltpu.make_async_copy(own, par, s["load_sem"].at[1]).wait()
    for c in (*one_way, *both):
        renew_early(c)
    weights()
    for c in (*one_way, *both):
        renew_late(c)

    def early(x):
        for y0 in range(0, NY, 2):
            sides = []
            for y in (y0, y0 + 1):
                parts = []
                for a, o in BLOCKS:
                    dx, dy = (0, o) if a == 1 else (o, 0)
                    parts += [ub[x + H + dx, y + H + dy, c] for c in range(chunks)]
                sides.append(jnp.concatenate(parts, axis=0))
            out = jnp.dot(s["w_early"][...], jnp.concatenate(sides, axis=1), preferred_element_type=f32)
            for q in range(2):
                part = out[:, q * NZ:(q + 1) * NZ]
                smooth = part[2 * F:]
                for o in (-H, H):
                    for u, v in ((x + o, y0 + q), (x, y0 + q + o)):
                        if 0 <= u < NX and 0 <= v < NY:
                            smooth = smooth + box[u + H, v + H]
                acc[x, y0 + q, pl.ds(0, F)] = part[:F] + part[F:2 * F]
                acc[x, y0 + q, pl.ds(F, F)] = smooth

    for x in range(NX):
        early(x)

    def summed(spread, n):
        at = n * 2 * ROWS
        return spread[at:at + ROWS] + spread[at + ROWS:at + 2 * ROWS]

    def mixed_along(columns):
        sides = [
            jnp.concatenate([split16(t[:, n * NZ:(n + 1) * NZ]) for n in range(2) for t in terms], axis=0)
            for terms in columns
        ]
        out = jnp.dot(s["w_along"][...], jnp.concatenate(sides, axis=1), preferred_element_type=f32)
        out = out[:F] + out[F:]
        return [out[:, q * NZ:(q + 1) * NZ] for q in range(2)]

    def along(x):
        lines = [ub[x + H, y + H, c] for y in range(NY) for c in range(chunks)]
        spread = jnp.dot(jnp.concatenate(lines, axis=0), s["band"][:NZ], preferred_element_type=f32)
        terms = [[summed(spread, y * chunks + c) for c in range(chunks)] for y in range(NY)]
        for y0 in range(0, NY, 2):
            linear = mixed_along(terms[y0:y0 + 2])
            for q in range(2):
                acc[x, y0 + q, pl.ds(0, F)] += linear[q]
                for c in range(chunks):
                    acc[x, y0 + q, pl.ds(F + c * ROWS, ROWS)] += terms[y0 + q][c][:, 2 * NZ:]

    for x in range(NX):
        along(x)

    for r in rims_in:
        r.arrived()

    lines = []
    for g in range(groups):
        for c in range(chunks):
            lines.append(split16(jnp.where(
                lane % SLOT < SLOT // 2,
                jnp.where(above["gz"], rim_up[c, g], 0.0), jnp.where(below["gz"], rim_low[c, g], 0.0),
            )))
    spread = jnp.dot(jnp.concatenate(lines, axis=0), s["band"][NZ:], preferred_element_type=f32)
    terms = [[summed(spread, g * chunks + c) for c in range(chunks)] for g in range(groups)]
    at_ends = (lane < SLOT // 2) | (lane >= NZ - SLOT // 2)
    for g0 in range(0, groups, 2):
        linear = mixed_along(terms[g0:g0 + 2])
        for q in range(2):
            g = g0 + q
            lapse = (1.0 + 0.25 * jnp.tanh(rim[0, g, 0:1, :])) * (64.0 / 12.0)
            for c in range(chunks):
                extra = lapse * linear[q][c * ROWS:(c + 1) * ROWS] + terms[g][c][:, 2 * NZ:]
                for j in range(slots):
                    x, y = g * (slots // NY) + j // NY, j % NY
                    placed = jnp.where(at_ends, pltpu.roll(extra, (NZ - SLOT * j) % NZ, 1), 0.0)
                    acc[x, y, pl.ds(F + c * ROWS, ROWS)] += placed

    for a in range(2):
        n = SIDES.index((a, -1))
        inside[(a, -1)].arrived()
        pl.when(below[AXES[a]])(functools.partial(add_side, box, acc, acc, w_late, n))

    def finish(x, _):
        for y in range(NY - H):
            slope_ref[x * NY + y], value_ref[x * NY + y] = finished(box, acc, x, y)
        return 0

    lax.fori_loop(0, NX - H, finish, 0)

    for a in range(2):
        inside[(a, 1)].arrived()

        @pl.when(jnp.logical_not(above[AXES[a]]))
        def _(a=a):
            def step(i, _):
                for h in range(H):
                    at = (NX, NY)[a] + H + h
                    where = (at, i + H) if a == 0 else (i + H, at)
                    box[where] = jnp.zeros((F, NZ), f32)
                return 0

            lax.fori_loop(0, (NY, NX)[a], step, 0)

    for r in routes.values():
        r.all_sent()


def put_out(slope_in, value_in, acc_in, box, w_late, slope_hbm, value_hbm, slope_rest, value_rest, acc, sem):
    NX, NY = acc_in.shape[:2]
    sources = ((slope_in, slope_rest, slope_hbm), (value_in, value_rest, value_hbm))

    def send(x, y, rest):
        k = x * NY + y
        for n, source in enumerate(sources):
            pltpu.make_async_copy(source[rest].at[k], source[2].at[:, k], sem.at[n]).start()

    def send_inner(x, _):
        for y in range(NY - H):
            send(x, y, 0)
        return 0

    lax.fori_loop(0, NX - H, send_inner, 0)
    add_side(box, acc_in, acc, w_late, SIDES.index((0, 1)))
    add_side(box, acc_in, acc, w_late, SIDES.index((1, 1)), lambda x, y: x >= NX - H)

    def finish(x, y):
        k = x * NY + y
        slope_rest[k], value_rest[k] = finished(box, acc, x, y)

    def right(x, _):
        for y in range(NY - H, NY):
            finish(x, y)
            send(x, y, 1)
        return 0

    def low(x, _):
        for y in range(NY):
            finish(x, y)
            send(x, y, 1)
        return 0

    lax.fori_loop(0, NX - H, right, 0)
    lax.fori_loop(NX - H, NX, low, 0)
    for n in range(2):
        pltpu.make_async_copy(slope_rest, value_rest, sem.at[n]).wait()


def local(fields_now, parent, advect, diffuse, box_shift):
    dims = fields_now.shape
    F, NX, NY, NZ = dims
    flat = (F, NX * NY, NZ)
    by_cell = (NX * NY, F, NZ)
    vmem = pl.BlockSpec(memory_space=pltpu.VMEM)
    hbm = pl.BlockSpec(memory_space=pltpu.HBM)
    operands = [
        pltpu.with_memory_space_constraint(x, pltpu.HBM)
        for x in (
            box_shift, fields_now.reshape(flat), parent.reshape(flat), advect, diffuse,
            jnp.asarray(coefficients(F)), jnp.asarray(band(NZ), bf16),
        )
    ]
    held = [
        pltpu.VMEM((NX, NY, 2 * F, NZ), f32),
        pltpu.VMEM((NX + 2 * H, NY + 2 * H, F, NZ), f32),
        pltpu.VMEM((len(SIDES), 4 * F, 4 * F), bf16),
    ]
    results = pl.pallas_call(
        functools.partial(kernel, dims),
        out_shape=[pltpu.VMEM(by_cell, f32)] * 2 + held,
        in_specs=[hbm] * len(operands),
        out_specs=[vmem] * 5,
        scratch_shapes=list(scratch(dims).values()),
        compiler_params=pltpu.CompilerParams(
            collective_id=0, has_side_effects=True, vmem_limit_bytes=VMEM_BYTES
        ),
    )(*operands)
    slope, value = pl.pallas_call(
        put_out,
        out_shape=[jax.ShapeDtypeStruct(flat, f32)] * 2,
        in_specs=[vmem] * 5,
        out_specs=[hbm] * 2,
        scratch_shapes=[pltpu.VMEM(by_cell, f32)] * 2 + [held[0], pltpu.SemaphoreType.DMA((2,))],
        compiler_params=pltpu.CompilerParams(vmem_limit_bytes=VMEM_BYTES),
    )(*results)
    return slope.reshape(dims), value.reshape(dims)


VMEM_BYTES = 40 * 2**20


def solution(mesh):
    return jax.shard_map(
        local,
        mesh=mesh,
        in_specs=(P(None, "gx", "gy", "gz"), P(None, "gx", "gy", "gz"), P(), P(), P()),
        out_specs=(P(None, "gx", "gy", "gz"), P(None, "gx", "gy", "gz")),
        check_vma=False,
    )
```

```python
import functools

import jax
import jax.numpy as jnp
import numpy as np
from jax import lax
from jax.experimental import pallas as pl
from jax.experimental.pallas import tpu as pltpu
from jax.sharding import PartitionSpec as P

MESH = pl.DeviceIdType.MESH
W = 4
H = 3
SLOT = 8
ROWS = 8
AXES = ("gx", "gy", "gz")
KINDS = ("x", "y", "split")
HALF = ROWS // 2
ARRIVALS = {"x": 5, "y": 5, "split": 7}
ROUTES = 8
FIRST = {-2: 1, -1: -8, 1: 8, 2: -1}
SECOND = {-2: -1, -1: 16, 0: -30, 1: 16, 2: -1}
SIXTH = {-3: 1, -2: -6, -1: 15, 0: -20, 1: 15, 2: -6, 3: 1}
BLOCKS = [(None, 0)] + [(a, o) for a in range(2) for o in (-2, -1, 1, 2)]
ALONG = [(2, "first"), (2, "second")]
SIDES = [(a, sign) for a in range(2) for sign in (-1, 1)]
f32, bf16 = jnp.float32, jnp.bfloat16


def up_to(n, m):
    return -(-n // m) * m


def block_columns(block, fields):
    cols = np.zeros((16, 2 * fields), np.float32)
    for c in range(fields // ROWS):
        for h in range(2):
            for r in range(ROWS):
                n = (c * 2 + h) * ROWS + r
                cols[7, n] = c * ROWS + r
                cols[8, n] = 1 - h
    if block is None:
        return cols
    axis, o = block
    if o in ("first", "second"):
        cols[axis + (3 if o == "second" else 0)] = 1
        return cols
    for a in range(3):
        if axis is None or a == axis:
            cols[a] = FIRST.get(o, 0)
            cols[3 + a] = SECOND.get(o, 0)
            cols[6] += SIXTH[o]
    return cols


def coefficients(fields):
    groups = [BLOCKS, ALONG]
    for a, sign in SIDES:
        groups += [[(a, sign), (a, 2 * sign)], [(a, 2 * sign), None]]
    out = []
    for g in groups:
        cols = np.concatenate([block_columns(b, fields) for b in g], axis=1)
        out.append(np.pad(cols, ((0, 0), (0, up_to(cols.shape[1], 256) - cols.shape[1]))))
    return np.concatenate(out, axis=1)


def band(length):
    out = np.zeros((2, length, 3, length), np.float32)
    for n, terms in enumerate((FIRST, SECOND, SIXTH)):
        for o, factor in terms.items():
            for lane in range(length):
                if o and 0 <= lane + o < length:
                    out[0, lane + o, n, lane] = factor
                at = (lane + SLOT // 2) % SLOT - SLOT // 2
                if (0 <= at + o < H and at < 0) or (-H <= at + o < 0 <= at):
                    out[1, (lane + o) % length, n, lane] = factor
    return out.reshape(2 * length, 3 * length)


def scratch(dims):
    F, NX, NY, NZ = dims
    chunks = F // ROWS
    groups = NX * NY * SLOT // NZ
    tile = (ROWS, NZ)
    out = dict(
        shift=pltpu.SMEM((3,), jnp.int32),
        own=pltpu.VMEM((NX, NY, F, NZ), f32),
        par=pltpu.VMEM((NX, NY, F, NZ), f32),
        advect=pltpu.VMEM((3, F, F), f32),
        diffuse=pltpu.VMEM((3, F, F), f32),
        coef=pltpu.VMEM(coefficients(F).shape, f32),
        band=pltpu.VMEM((2 * NZ, 3 * NZ), bf16),
        w_early=pltpu.VMEM((3 * F, len(BLOCKS) * 2 * F), bf16),
        w_along=pltpu.VMEM((2 * F, len(ALONG) * 2 * F), bf16),
        ub=pltpu.VMEM((NX + 2 * H, NY + 2 * H, chunks, 2 * ROWS, NZ), bf16),
        rim=pltpu.VMEM((chunks, groups) + tile, f32),
        rim_up=pltpu.VMEM((chunks, groups) + tile, f32),
        rim_low=pltpu.VMEM((chunks, groups) + tile, f32),
        epk=pltpu.VMEM((chunks, 3) + tile, f32),
        ein=pltpu.VMEM((chunks, 4) + tile, f32),
    )
    for c in range(chunks):
        kind = KINDS[c % 3]
        if kind != "y":
            out[f"rawx{c}"] = pltpu.VMEM((W, NY) + tile, f32)
        if kind != "x":
            out[f"rawy{c}"] = pltpu.VMEM((NX, W) + tile, f32)
        ext = (W if kind != "y" else 0, W if kind != "x" else 0)
        out[f"zs{c}"] = pltpu.VMEM((NX + ext[0], NY + ext[1]) + tile, f32)
        for way, size in (("x", (NX, W)), ("y", (W, NY))):
            if kind in (way, "split"):
                out[f"fw{way}{c}"] = pltpu.VMEM(size + tile, f32)
                out[f"te{way}{c}"] = pltpu.VMEM(size + tile, f32)
    out["count"] = pltpu.VMEM((chunks * 8 * NX * NY,) + tile, f32)
    n = sum(ARRIVALS[KINDS[c % 3]] for c in range(chunks)) + len(SIDES) + 2
    out["send_sem"] = pltpu.SemaphoreType.DMA((ROUTES,))
    out["recv_sem"] = pltpu.SemaphoreType.DMA((n,))
    out["load_sem"] = pltpu.SemaphoreType.DMA((7,))
    return out


def split16(u):
    low = u - u.astype(bf16).astype(f32)
    return jnp.concatenate([u, low], axis=0).astype(bf16)


def add_side(box, acc, out_acc, w_late, n, again=None):
    a, sign = SIDES[n]
    NX, NY, F, NZ = acc.shape[0], acc.shape[1], acc.shape[2] // 2, acc.shape[3]
    length, across = ((NX, NY), (NY, NX))[a]
    linear_rows, smooth_rows = pl.ds(0, F), pl.ds(F, F)

    def spot(depth, i):
        at = length - 1 - depth if sign > 0 else depth
        return (at, i) if a == 0 else (i, at)

    for i0 in range(0, across, 2):
        columns, smooth = [], []
        for i in (i0, i0 + 1):
            near = []
            for h in range(1, H + 1):
                x, y = spot(-h, i)
                near.append(box[x + H, y + H])
            smooth.append((15.0 * near[0] - 6.0 * near[1] + near[2], near[1] - 6.0 * near[0], near[0]))
            parts = [split16(u[c:c + ROWS]) for u in near[:2] for c in range(0, F, ROWS)]
            columns.append(jnp.concatenate(parts, axis=0))
        out = jnp.dot(w_late[n], jnp.concatenate(columns, axis=1), preferred_element_type=f32)
        for q in range(2):
            part = out[:, q * NZ:(q + 1) * NZ]
            for d in range(H):
                x, y = spot(d, i0 + q)
                source = out_acc if again is not None and again(x, y) else acc
                linear = source[x, y, linear_rows]
                if d < 2:
                    mine = part[2 * F * d:2 * F * (d + 1)]
                    linear = linear + (mine[:F] + mine[F:])
                out_acc[x, y, linear_rows] = linear
                out_acc[x, y, smooth_rows] = source[x, y, smooth_rows] + smooth[q][d]


def finished(box, acc, x, y):
    u = box[x + H, y + H]
    F = u.shape[0]
    lapse = (1.0 + 0.25 * jnp.tanh(u[0:1])) * (1.0 / 12.0)
    slope = lapse * acc[x, y, pl.ds(0, F)] + acc[x, y, pl.ds(F, F)] * (1.0 / 64.0)
    return slope, u + 0.125 * slope


def kernel(
    dims, shift_hbm, now_hbm, parent_hbm, advect_hbm, diffuse_hbm, coef_hbm, band_hbm,
    slope_ref, value_ref, acc, box, w_late, *refs
):
    F, NX, NY, NZ = dims
    chunks = F // ROWS
    cells = NX * NY
    s = dict(zip(scratch(dims), refs))
    own, par, ub = s["own"], s["par"], s["ub"]
    epk, ein, rim, rim_up, rim_low = s["epk"], s["ein"], s["rim"], s["rim_up"], s["rim_low"]
    slots = NZ // SLOT
    groups = cells // slots
    me = {a: lax.axis_index(a) for a in AXES}
    size = {a: lax.axis_size(a) for a in AXES}
    below = {a: me[a] > 0 for a in AXES}
    above = {a: me[a] < size[a] - 1 for a in AXES}
    sems = iter(range(1000))
    kinds = [KINDS[c % 3] for c in range(chunks)]
    rows = [pl.ds(c * ROWS, ROWS) for c in range(chunks)]

    def load_cells(src, dst, n):
        def step(x, _):
            for y in range(NY):
                pltpu.make_async_copy(src.at[:, x * NY + y], dst.at[x, y], s["load_sem"].at[n]).start()
            return 0

        lax.fori_loop(0, NX, step, 0)

    singles = [
        pltpu.make_async_copy(src, dst, s["load_sem"].at[2 + n])
        for n, (src, dst) in enumerate((
            (shift_hbm, s["shift"]), (advect_hbm, s["advect"]),
            (diffuse_hbm, s["diffuse"]), (coef_hbm, s["coef"]), (band_hbm, s["band"]),
        ))
    ]
    DX, DY, DZ = {"gx": -1}, {"gy": -1}, {"gz": -1}
    UX, UY, UZ = {"gx": 1}, {"gy": 1}, {"gz": 1}
    barrier = pltpu.get_barrier_semaphore()
    count = 0
    for to in (DX, UX, DY, UY, DZ, UZ, UX | UZ, UY | UZ):
        cond = back = None
        for a, by in to.items():
            one, two = (below[a], above[a]) if by < 0 else (above[a], below[a])
            cond = one if cond is None else cond & one
            back = two if back is None else back & two

        @pl.when(cond)
        def _(to=to):
            pl.semaphore_signal(
                barrier, inc=1, device_id={a: me[a] + by for a, by in to.items()}, device_id_type=MESH
            )
        count = count + jnp.where(back, 1, 0)

    singles[0].start()
    load_cells(now_hbm, own, 0)
    pl.semaphore_wait(barrier, count)

    routes = {}

    class Route:
        def __init__(self, to):
            self.to = to
            self.send_sem = s["send_sem"].at[len(routes)]
            self.tiles = 0
            self.sends = self.gets = None
            for a, by in to.items():
                sends = below[a] if by < 0 else above[a]
                gets = above[a] if by < 0 else below[a]
                self.sends = sends if self.sends is None else self.sends & sends
                self.gets = gets if self.gets is None else self.gets & gets

        def copy(self, src, dst, recv_sem):
            return pltpu.make_async_remote_copy(
                src_ref=src, dst_ref=dst, send_sem=self.send_sem, recv_sem=recv_sem,
                device_id={a: me[a] + by for a, by in self.to.items()}, device_id_type=MESH,
            )

        def all_sent(self):
            done = s["count"].at[pl.ds(0, self.tiles // 2)]
            pl.when(self.sends)(self.copy(done, done, s["recv_sem"].at[0]).wait_send)

    def route(to):
        key = tuple(sorted(to.items()))
        if key not in routes:
            routes[key] = Route(to)
        return routes[key]

    class Arrival:
        def __init__(self, to):
            self.route = route(to)
            self.recv_sem = s["recv_sem"].at[next(sems)]
            self.tiles = 0

        def arrived(self):
            done = s["count"].at[pl.ds(0, self.tiles // 2)]
            pl.when(self.route.gets)(self.route.copy(done, done, self.recv_sem).wait_recv)

    def size_of(ref):
        return int(np.prod(ref.shape)) // (HALF * NZ)

    class Message:
        def __init__(self, src, dst, to, arrival=None, parts=None):
            self.arrival = arrival or Arrival(to)
            self.route = route(to)
            tiles = size_of(dst)
            self.arrival.tiles += tiles
            self.route.tiles += tiles
            self.src, self.dst, self.parts = src, dst, parts

        def start(self):
            pl.when(self.route.sends)(self.route.copy(self.src, self.dst, self.arrival.recv_sem).start)

        def start_parts(self, i):
            @pl.when(self.route.sends)
            def _():
                for j in range(W):
                    self.route.copy(*self.parts(i, j), self.arrival.recv_sem).start()

        def arrived(self):
            self.arrival.arrived()

    message = Message

    lowx, lowy = pl.ds(0, W), pl.ds(0, W)
    raw, edge, diag, forward = {}, {}, {}, {}
    whole = pl.ds(0, ROWS)

    def halves_of(src, dst, way, fields, to):
        arrival = Arrival(to)
        out = []
        for h in range(2):
            n = (NX if way == "x" else NY) // 2
            span = pl.ds(h * n, n)
            at = (span, slice(None), fields) if way == "x" else (slice(None), span, fields)
            out.append([message(src.at[at], dst.at[at], to, arrival)])
        return out

    for c, kind in enumerate(kinds):
        if kind == "x":
            def cell(i, j, half, c=c):
                x, y = i, j + half * (NY // 2)
                return now_hbm.at[rows[c], x * NY + y], s[f"rawx{c}"].at[x, y]

            halves = [s[f"rawx{c}"].at[:, pl.ds(h * (NY // 2), NY // 2)] for h in range(2)]
            raw[c] = [message(r, r, DX, parts=functools.partial(cell, half=h)) for h, r in enumerate(halves)]
            diag[c] = [message(epk.at[c, 0], ein.at[c, 2], DX | DZ)]
            forward[c] = halves_of(s[f"fwx{c}"], s[f"tex{c}"], "x", whole, DY)
        elif kind == "y":
            def cell(i, j, half, c=c):
                x, y = i + half * (NX // 2), j
                return now_hbm.at[rows[c], x * NY + y], s[f"rawy{c}"].at[x, y]

            halves = [s[f"rawy{c}"].at[pl.ds(h * (NX // 2), NX // 2)] for h in range(2)]
            raw[c] = [message(r, r, DY, parts=functools.partial(cell, half=h)) for h, r in enumerate(halves)]
            diag[c] = [message(epk.at[c, 0], ein.at[c, 2], DY | DZ)]
            forward[c] = halves_of(s[f"fwy{c}"], s[f"tey{c}"], "y", whole, DX)
        else:
            a_rows, b_rows = pl.ds(0, HALF), pl.ds(HALF, HALF)
            raw[c] = [
                message(own.at[lowx, :, pl.ds(c * ROWS, HALF)], s[f"rawx{c}"].at[:, :, a_rows], DX),
                message(own.at[:, lowy, pl.ds(c * ROWS + HALF, HALF)], s[f"rawy{c}"].at[:, :, b_rows], DY),
            ]
            diag[c] = [
                message(epk.at[c, 0], ein.at[c, 2], DX | DZ), message(epk.at[c, 2], ein.at[c, 3], DY | DZ),
            ]
            along_x = halves_of(s[f"fwx{c}"], s[f"tex{c}"], "x", a_rows, DY)
            along_y = halves_of(s[f"fwy{c}"], s[f"tey{c}"], "y", b_rows, DX)
            forward[c] = [x + y for x, y in zip(along_x, along_y)]
        edge[c] = message(epk.at[c, pl.ds(0, 2)], ein.at[c, pl.ds(0, 2)], DZ)

    inside = {(a, sign): Arrival({AXES[a]: -sign}) for a, sign in SIDES}
    rims_in = [Arrival(DZ), Arrival(UZ)]

    def halo(c, a, by, lo, hi, part=None):
        fields = rows[c] if part is None else pl.ds(c * ROWS + part * HALF, HALF)
        n = (NX, NY)[a]
        src = pl.ds(H, H) if by < 0 else pl.ds(n, H)
        dst = pl.ds(n + H, H) if by < 0 else pl.ds(0, H)
        span = pl.ds(H + lo, hi - lo)
        to = {AXES[a]: by}
        if a == 0:
            return message(box.at[src, span, fields], box.at[dst, span, fields], to, inside[(a, -by)])
        return message(box.at[span, src, fields], box.at[span, dst, fields], to, inside[(a, -by)])

    early_halo, late_halo, rims = {}, {}, {}
    hx, hy = NX // 2, NY // 2
    for c, kind in enumerate(kinds):
        if kind == "x":
            early_halo[c] = [halo(c, 1, -1, 0, NX), halo(c, 0, 1, 0, hy)]
            late_halo[c] = [halo(c, 0, -1, 0, NY), halo(c, 0, 1, hy, NY), halo(c, 1, 1, 0, NX)]
        elif kind == "y":
            early_halo[c] = [halo(c, 0, -1, 0, NY), halo(c, 1, 1, 0, hx)]
            late_halo[c] = [halo(c, 1, -1, 0, NX), halo(c, 1, 1, hx, NX), halo(c, 0, 1, 0, NY)]
        else:
            early_halo[c] = [
                halo(c, 1, -1, 0, NX, 0), halo(c, 0, -1, 0, NY, 1), halo(c, 0, 1, 0, hy, 0), halo(c, 1, 1, 0, hx, 1),
            ]
            late_halo[c] = [
                halo(c, 0, -1, 0, NY, 0), halo(c, 1, -1, 0, NX, 1), halo(c, 0, 1, hy, NY, 0),
                halo(c, 1, 1, hx, NX, 1), halo(c, 0, 1, 0, NY, 1), halo(c, 1, 1, 0, NX, 0),
            ]
        rims[c] = [
            message(rim.at[c], rim_up.at[c], DZ, rims_in[0]), message(rim.at[c], rim_low.at[c], UZ, rims_in[1]),
        ]

    def send_raw(i, _, half):
        for c, kind in enumerate(kinds):
            if kind != "split":
                raw[c][half].start_parts(i)
        return 0

    def send_raws(half, lo, hi):
        lax.fori_loop(lo, hi, functools.partial(send_raw, half=half), 0)

    send_raws(0, 0, W)
    send_raws(1, 0, W // 2)

    lane = lax.broadcasted_iota(jnp.int32, (ROWS, NZ), 1)
    thin = lane // W
    wide = ((lane + SLOT // 2) % NZ) // SLOT
    blank = jnp.zeros((ROWS, NZ), f32)

    def pack(c, n, along, q):
        packed = blank
        across = NY if along == "x" else NX
        for slot in range(W * across):
            i, j = q * W + slot // across, slot % across
            x, y = (i, j) if along == "x" else (j, i)
            packed = jnp.where(thin == slot, pltpu.roll(own[x, y, rows[c]], W * slot, 1), packed)
        epk[c, n] = packed

    pltpu.make_async_copy(par, own, s["load_sem"].at[0]).wait()
    one_way = [c for c in range(chunks) if kinds[c] != "split"]
    both = [c for c in range(chunks) if kinds[c] == "split"]
    for c in one_way:
        pack(c, 0, kinds[c], 0)
        diag[c][0].start()
    send_raws(1, W // 2, W)
    for c in one_way:
        pack(c, 1, kinds[c], 1)
        edge[c].start()
    for c in both:
        pack(c, 0, "x", 0)
        pack(c, 2, "y", 0)
        for d in diag[c]:
            d.start()
        for r in raw[c]:
            r.start()
        pack(c, 1, "x", 1)
        edge[c].start()

    for load in singles[1:]:
        load.start()
    load_cells(parent_hbm, par, 1)
    zero16 = jnp.zeros((2 * ROWS, NZ), bf16)

    def clear(i, _):
        for c in range(chunks):
            for o in range(H):
                ub[o, i + H, c] = zero16
                ub[NX + H + o, i + H, c] = zero16
                ub[i + H, o, c] = zero16
                ub[i + H, NY + H + o, c] = zero16
        return 0

    lax.fori_loop(0, NX, clear, 0)

    singles[0].wait()
    move = [s["shift"][d] for d in range(3)]
    sz = move[2]

    def weights():
        for load in singles[1:]:
            load.wait()
        mats = []
        for m in (s["advect"], s["diffuse"]):
            for a in range(3):
                one = m[a]
                high = one.astype(bf16).astype(f32)
                mid = (one - high).astype(bf16).astype(f32)
                mats.append(jnp.concatenate([high, mid, one - high - mid], axis=0).astype(bf16))

        def columns(at, width, ks):
            table = s["coef"][:, at:at + width]
            hit = lax.broadcasted_iota(jnp.int32, (F, width), 0).astype(f32) == table[7:8]
            smooth = jnp.where(hit, table[6:7], 0.0)
            total = None
            for k in ks:
                spread = jnp.where(hit, table[k:k + 1], 0.0).astype(bf16)
                part = jnp.dot(mats[k], spread, preferred_element_type=f32)
                total = part if total is None else total + part
            w = total[:F] + total[F:2 * F] + total[2 * F:]
            high = w.astype(bf16).astype(f32)
            return jnp.concatenate([high, (w - high) * table[8:9], smooth], axis=0)

        k_early = len(BLOCKS) * 2 * F
        for at in range(0, up_to(k_early, 256), 256):
            n = min(256, k_early - at)
            s["w_early"][:, at:at + n] = columns(at, 256, range(6))[:, :n].astype(bf16)
        at = up_to(k_early, 256)
        k_along = len(ALONG) * 2 * F
        s["w_along"][...] = columns(at, up_to(k_along, 256), (2, 5))[:2 * F, :k_along].astype(bf16)
        at += up_to(k_along, 256)
        k_late = 2 * 2 * F
        step = up_to(k_late, 256)
        for n, (a, sign) in enumerate(SIDES):
            parts = [columns(at + d * step, step, (a, 3 + a))[:2 * F] for d in range(2)]
            w_late[n] = jnp.concatenate(parts, axis=0)[:, :k_late].astype(bf16)
            at += 2 * step

    def z_row(row, packed, slot):
        tail = pltpu.roll(packed, NZ - W * slot - sz, 1)
        return jnp.where(lane >= NZ - sz, tail, pltpu.roll(row, NZ - sz, 1))

    def z_own(c, xs, ys):
        kind = kinds[c]
        for x in range(*xs):
            for y in range(*ys):
                q, slot = (x // W, x % W * NY + y) if kind != "y" else (y // W, y % W * NX + x)
                s[f"zs{c}"][x, y] = z_row(own[x, y, rows[c]], ein[c, q], slot)

    def z_ext_x(c, lo, hi):
        for x in range(W):
            for y in range(lo, hi):
                s[f"zs{c}"][NX + x, y] = z_row(s[f"rawx{c}"][x, y], ein[c, 2], x * NY + y)

    def z_ext_y(c, lo, hi):
        n = 3 if kinds[c] == "split" else 2
        for x in range(lo, hi):
            for y in range(W):
                s[f"zs{c}"][x, NY + y] = z_row(s[f"rawy{c}"][x, y], ein[c, n], y * NX + x)

    def make_forward(c, half):
        zs = s[f"zs{c}"]

        def step(i, _):
            for j in range(W):
                if kinds[c] != "y":
                    s[f"fwx{c}"][i, j] = zs[i + move[0], j]
                if kinds[c] != "x":
                    s[f"fwy{c}"][j, i] = zs[j, i + move[1]]
            return 0

        lax.fori_loop(half * hx, (half + 1) * hx, step, 0)
        for f in forward[c][half]:
            f.start()

    in_z = me["gz"] * NZ + lane + sz < size["gz"] * NZ

    upper = lax.broadcasted_iota(jnp.int32, (ROWS, NZ), 0) < HALF

    def renew(c, xs, ys, late, part=None, whole=True):
        kind, zs = kinds[c], s[f"zs{c}"]

        def step(x, _):
            in_x = me["gx"] * NX + x + move[0] < size["gx"] * NX
            for y in range(*ys):
                in_y = me["gy"] * NY + y + move[1] < size["gy"] * NY
                X, Y = x + move[0], y + move[1]
                if late:
                    if kind != "y":
                        x_first = jnp.where(
                            Y < NY, zs[X, jnp.minimum(Y, NY - 1)], s[f"tex{c}"][x, jnp.maximum(Y - NY, 0)]
                        )
                    if kind != "x":
                        y_first = jnp.where(
                            X < NX, zs[jnp.minimum(X, NX - 1), Y], s[f"tey{c}"][jnp.maximum(X - NX, 0), y]
                        )
                    row = x_first if kind == "x" else y_first
                    if kind == "split":
                        row = jnp.where(upper, x_first, y_first)
                else:
                    row = zs[X, Y]
                row = jnp.where(in_z & (in_x & in_y), row, par[x, y, rows[c]])
                if part is None:
                    box[x + H, y + H, rows[c]] = row
                else:
                    kept = slice(part * HALF, (part + 1) * HALF)
                    box[x + H, y + H, pl.ds(c * ROWS + part * HALF, HALF)] = row[kept]
                if whole:
                    ub[x + H, y + H, c] = split16(row)
            return 0

        lax.fori_loop(*xs, step, 0)

    def renew_early(c):
        if kinds[c] == "x":
            renew(c, (0, NX), (0, hy), False)
        elif kinds[c] == "y":
            renew(c, (0, hx), (0, NY), False)
        else:
            renew(c, (0, hx), (0, hy), False)
            renew(c, (hx, NX), (0, hy), False, 0, False)
            renew(c, (0, hx), (hy, NY), False, 1, False)
        for h in early_halo[c]:
            h.start()

    def renew_late(c):
        for f in forward[c][0]:
            f.arrived()
        if kinds[c] == "x":
            renew(c, (0, NX), (hy, NY), True)
        elif kinds[c] == "y":
            renew(c, (hx, NX), (0, NY), True)
        else:
            renew(c, (hx, NX), (0, hy), True, 1)
            renew(c, (0, hx), (hy, NY), True, 0)
            renew(c, (hx, NX), (hy, NY), True)
        for h in late_halo[c]:
            h.start()

        for g in range(groups):
            packed = blank
            for j in range(slots):
                x, y = g * (slots // NY) + j // NY, j % NY
                packed = jnp.where(wide == j, pltpu.roll(box[x + H, y + H, rows[c]], SLOT * j, 1), packed)
            rim[c, g] = packed
        for r in rims[c]:
            r.start()

    for c in one_way:
        edge[c].arrived()
        z_own(c, (0, NX if kinds[c] == "x" else hx), (0, NY if kinds[c] == "y" else hy))
        make_forward(c, 0)
    for c in both:
        edge[c].arrived()
        z_own(c, (0, NX), (0, NY))
        make_forward(c, 0)
    for c in one_way:
        z_own(c, (0 if kinds[c] == "x" else hx, NX), (0 if kinds[c] == "y" else hy, NY))
    for c in one_way:
        diag[c][0].arrived()
        raw[c][0].arrived()
        if kinds[c] == "x":
            z_ext_x(c, 0, hy)
        else:
            z_ext_y(c, 0, hx)
        make_forward(c, 1)
    for c in one_way:
        raw[c][1].arrived()
        if kinds[c] == "x":
            z_ext_x(c, hy, NY)
        else:
            z_ext_y(c, hx, NX)
    for c in both:
        for d in diag[c]:
            d.arrived()
        raw[c][0].arrived()
        z_ext_x(c, 0, NY)
        raw[c][1].arrived()
        z_ext_y(c, 0, NX)
        make_forward(c, 1)
    pltpu.make_async_copy(own, par, s["load_sem"].at[1]).wait()
    for c in (*one_way, *both):
        renew_early(c)
    weights()
    for c in (*one_way, *both):
        renew_late(c)

    def early(x):
        for y0 in range(0, NY, 2):
            sides = []
            for y in (y0, y0 + 1):
                parts = []
                for a, o in BLOCKS:
                    dx, dy = (0, o) if a == 1 else (o, 0)
                    parts += [ub[x + H + dx, y + H + dy, c] for c in range(chunks)]
                sides.append(jnp.concatenate(parts, axis=0))
            out = jnp.dot(s["w_early"][...], jnp.concatenate(sides, axis=1), preferred_element_type=f32)
            for q in range(2):
                part = out[:, q * NZ:(q + 1) * NZ]
                smooth = part[2 * F:]
                for o in (-H, H):
                    for u, v in ((x + o, y0 + q), (x, y0 + q + o)):
                        if 0 <= u < NX and 0 <= v < NY:
                            smooth = smooth + box[u + H, v + H]
                acc[x, y0 + q, pl.ds(0, F)] = part[:F] + part[F:2 * F]
                acc[x, y0 + q, pl.ds(F, F)] = smooth

    for x in range(NX):
        early(x)

    def summed(spread, n):
        at = n * 2 * ROWS
        return spread[at:at + ROWS] + spread[at + ROWS:at + 2 * ROWS]

    def mixed_along(columns):
        sides = [
            jnp.concatenate([split16(t[:, n * NZ:(n + 1) * NZ]) for n in range(2) for t in terms], axis=0)
            for terms in columns
        ]
        out = jnp.dot(s["w_along"][...], jnp.concatenate(sides, axis=1), preferred_element_type=f32)
        out = out[:F] + out[F:]
        return [out[:, q * NZ:(q + 1) * NZ] for q in range(2)]

    def along(x):
        lines = [ub[x + H, y + H, c] for y in range(NY) for c in range(chunks)]
        spread = jnp.dot(jnp.concatenate(lines, axis=0), s["band"][:NZ], preferred_element_type=f32)
        terms = [[summed(spread, y * chunks + c) for c in range(chunks)] for y in range(NY)]
        for y0 in range(0, NY, 2):
            linear = mixed_along(terms[y0:y0 + 2])
            for q in range(2):
                acc[x, y0 + q, pl.ds(0, F)] += linear[q]
                for c in range(chunks):
                    acc[x, y0 + q, pl.ds(F + c * ROWS, ROWS)] += terms[y0 + q][c][:, 2 * NZ:]

    for x in range(NX):
        along(x)

    for r in rims_in:
        r.arrived()

    lines = []
    for g in range(groups):
        for c in range(chunks):
            lines.append(split16(jnp.where(
                lane % SLOT < SLOT // 2,
                jnp.where(above["gz"], rim_up[c, g], 0.0), jnp.where(below["gz"], rim_low[c, g], 0.0),
            )))
    spread = jnp.dot(jnp.concatenate(lines, axis=0), s["band"][NZ:], preferred_element_type=f32)
    terms = [[summed(spread, g * chunks + c) for c in range(chunks)] for g in range(groups)]
    at_ends = (lane < SLOT // 2) | (lane >= NZ - SLOT // 2)
    for g0 in range(0, groups, 2):
        linear = mixed_along(terms[g0:g0 + 2])
        for q in range(2):
            g = g0 + q
            lapse = (1.0 + 0.25 * jnp.tanh(rim[0, g, 0:1, :])) * (64.0 / 12.0)
            for c in range(chunks):
                extra = lapse * linear[q][c * ROWS:(c + 1) * ROWS] + terms[g][c][:, 2 * NZ:]
                for j in range(slots):
                    x, y = g * (slots // NY) + j // NY, j % NY
                    placed = jnp.where(at_ends, pltpu.roll(extra, (NZ - SLOT * j) % NZ, 1), 0.0)
                    acc[x, y, pl.ds(F + c * ROWS, ROWS)] += placed

    for a in range(2):
        n = SIDES.index((a, -1))
        inside[(a, -1)].arrived()
        pl.when(below[AXES[a]])(functools.partial(add_side, box, acc, acc, w_late, n))

    def finish(x, _):
        for y in range(NY - H):
            slope_ref[x * NY + y], value_ref[x * NY + y] = finished(box, acc, x, y)
        return 0

    lax.fori_loop(0, NX - H, finish, 0)

    for a in range(2):
        inside[(a, 1)].arrived()

        @pl.when(jnp.logical_not(above[AXES[a]]))
        def _(a=a):
            def step(i, _):
                for h in range(H):
                    at = (NX, NY)[a] + H + h
                    where = (at, i + H) if a == 0 else (i + H, at)
                    box[where] = jnp.zeros((F, NZ), f32)
                return 0

            lax.fori_loop(0, (NY, NX)[a], step, 0)

    for r in routes.values():
        r.all_sent()


def put_out(slope_in, value_in, acc_in, box, w_late, slope_hbm, value_hbm, slope_rest, value_rest, acc, sem):
    NX, NY = acc_in.shape[:2]
    sources = ((slope_in, slope_rest, slope_hbm), (value_in, value_rest, value_hbm))

    def send(x, y, rest):
        k = x * NY + y
        for n, source in enumerate(sources):
            pltpu.make_async_copy(source[rest].at[k], source[2].at[:, k], sem.at[n]).start()

    def send_inner(x, _):
        for y in range(NY - H):
            send(x, y, 0)
        return 0

    lax.fori_loop(0, NX - H, send_inner, 0)
    add_side(box, acc_in, acc, w_late, SIDES.index((0, 1)))
    add_side(box, acc_in, acc, w_late, SIDES.index((1, 1)), lambda x, y: x >= NX - H)

    def finish(x, y):
        k = x * NY + y
        slope_rest[k], value_rest[k] = finished(box, acc, x, y)

    def right(x, _):
        for y in range(NY - H, NY):
            finish(x, y)
            send(x, y, 1)
        return 0

    def low(x, _):
        for y in range(NY):
            finish(x, y)
            send(x, y, 1)
        return 0

    lax.fori_loop(0, NX - H, right, 0)
    lax.fori_loop(NX - H, NX, low, 0)
    for n in range(2):
        pltpu.make_async_copy(slope_rest, value_rest, sem.at[n]).wait()


def local(fields_now, parent, advect, diffuse, box_shift):
    dims = fields_now.shape
    F, NX, NY, NZ = dims
    flat = (F, NX * NY, NZ)
    by_cell = (NX * NY, F, NZ)
    vmem = pl.BlockSpec(memory_space=pltpu.VMEM)
    hbm = pl.BlockSpec(memory_space=pltpu.HBM)
    operands = [
        pltpu.with_memory_space_constraint(x, pltpu.HBM)
        for x in (
            box_shift, fields_now.reshape(flat), parent.reshape(flat), advect, diffuse,
            jnp.asarray(coefficients(F)), jnp.asarray(band(NZ), bf16),
        )
    ]
    held = [
        pltpu.VMEM((NX, NY, 2 * F, NZ), f32),
        pltpu.VMEM((NX + 2 * H, NY + 2 * H, F, NZ), f32),
        pltpu.VMEM((len(SIDES), 4 * F, 4 * F), bf16),
    ]
    results = pl.pallas_call(
        functools.partial(kernel, dims),
        out_shape=[pltpu.VMEM(by_cell, f32)] * 2 + held,
        in_specs=[hbm] * len(operands),
        out_specs=[vmem] * 5,
        scratch_shapes=list(scratch(dims).values()),
        compiler_params=pltpu.CompilerParams(
            collective_id=0, has_side_effects=True, vmem_limit_bytes=VMEM_BYTES
        ),
    )(*operands)
    slope, value = pl.pallas_call(
        put_out,
        out_shape=[jax.ShapeDtypeStruct(flat, f32)] * 2,
        in_specs=[vmem] * 5,
        out_specs=[hbm] * 2,
        scratch_shapes=[pltpu.VMEM(by_cell, f32)] * 2 + [held[0], pltpu.SemaphoreType.DMA((2,))],
        compiler_params=pltpu.CompilerParams(vmem_limit_bytes=VMEM_BYTES),
    )(*results)
    return slope.reshape(dims), value.reshape(dims)


VMEM_BYTES = 40 * 2**20


def solution(mesh):
    return jax.shard_map(
        local,
        mesh=mesh,
        in_specs=(P(None, "gx", "gy", "gz"), P(None, "gx", "gy", "gz"), P(), P(), P()),
        out_specs=(P(None, "gx", "gy", "gz"), P(None, "gx", "gy", "gz")),
        check_vma=False,
    )
```

```python
import functools

import jax
import jax.numpy as jnp
import numpy as np
from jax import lax
from jax.experimental import pallas as pl
from jax.experimental.pallas import tpu as pltpu
from jax.sharding import PartitionSpec as P

MESH = pl.DeviceIdType.MESH
W = 4
H = 3
SLOT = 8
ROWS = 8
AXES = ("gx", "gy", "gz")
KINDS = ("x", "y", "split")
HALF = ROWS // 2
ARRIVALS = {"x": 5, "y": 5, "split": 7}
ROUTES = 8
FIRST = {-2: 1, -1: -8, 1: 8, 2: -1}
SECOND = {-2: -1, -1: 16, 0: -30, 1: 16, 2: -1}
SIXTH = {-3: 1, -2: -6, -1: 15, 0: -20, 1: 15, 2: -6, 3: 1}
BLOCKS = [(None, 0)] + [(a, o) for a in range(2) for o in (-2, -1, 1, 2)]
ALONG = [(2, "first"), (2, "second")]
SIDES = [(a, sign) for a in range(2) for sign in (-1, 1)]
f32, bf16 = jnp.float32, jnp.bfloat16


def up_to(n, m):
    return -(-n // m) * m


def block_columns(block, fields):
    cols = np.zeros((16, 2 * fields), np.float32)
    for c in range(fields // ROWS):
        for h in range(2):
            for r in range(ROWS):
                n = (c * 2 + h) * ROWS + r
                cols[7, n] = c * ROWS + r
                cols[8, n] = 1 - h
    if block is None:
        return cols
    axis, o = block
    if o in ("first", "second"):
        cols[axis + (3 if o == "second" else 0)] = 1
        return cols
    for a in range(3):
        if axis is None or a == axis:
            cols[a] = FIRST.get(o, 0)
            cols[3 + a] = SECOND.get(o, 0)
            cols[6] += SIXTH[o]
    return cols


def coefficients(fields):
    groups = [BLOCKS, ALONG]
    for a, sign in SIDES:
        groups += [[(a, sign), (a, 2 * sign)], [(a, 2 * sign), None]]
    out = []
    for g in groups:
        cols = np.concatenate([block_columns(b, fields) for b in g], axis=1)
        out.append(np.pad(cols, ((0, 0), (0, up_to(cols.shape[1], 256) - cols.shape[1]))))
    return np.concatenate(out, axis=1)


def band(length):
    out = np.zeros((2, length, 3, length), np.float32)
    for n, terms in enumerate((FIRST, SECOND, SIXTH)):
        for o, factor in terms.items():
            for lane in range(length):
                if o and 0 <= lane + o < length:
                    out[0, lane + o, n, lane] = factor
                at = (lane + SLOT // 2) % SLOT - SLOT // 2
                if (0 <= at + o < H and at < 0) or (-H <= at + o < 0 <= at):
                    out[1, (lane + o) % length, n, lane] = factor
    return out.reshape(2 * length, 3 * length)


def scratch(dims):
    F, NX, NY, NZ = dims
    chunks = F // ROWS
    groups = NX * NY * SLOT // NZ
    tile = (ROWS, NZ)
    out = dict(
        shift=pltpu.SMEM((3,), jnp.int32),
        own=pltpu.VMEM((NX, NY, F, NZ), f32),
        par=pltpu.VMEM((NX, NY, F, NZ), f32),
        advect=pltpu.VMEM((3, F, F), f32),
        diffuse=pltpu.VMEM((3, F, F), f32),
        coef=pltpu.VMEM(coefficients(F).shape, f32),
        band=pltpu.VMEM((2 * NZ, 3 * NZ), bf16),
        w_early=pltpu.VMEM((3 * F, len(BLOCKS) * 2 * F), bf16),
        w_along=pltpu.VMEM((2 * F, len(ALONG) * 2 * F), bf16),
        ub=pltpu.VMEM((NX + 2 * H, NY + 2 * H, chunks, 2 * ROWS, NZ), bf16),
        rim=pltpu.VMEM((chunks, groups) + tile, f32),
        rim_up=pltpu.VMEM((chunks, groups) + tile, f32),
        rim_low=pltpu.VMEM((chunks, groups) + tile, f32),
        epk=pltpu.VMEM((chunks, 3) + tile, f32),
        ein=pltpu.VMEM((chunks, 4) + tile, f32),
    )
    for c in range(chunks):
        kind = KINDS[c % 3]
        if kind != "y":
            out[f"rawx{c}"] = pltpu.VMEM((W, NY) + tile, f32)
        if kind != "x":
            out[f"rawy{c}"] = pltpu.VMEM((NX, W) + tile, f32)
        ext = (W if kind != "y" else 0, W if kind != "x" else 0)
        out[f"zs{c}"] = pltpu.VMEM((NX + ext[0], NY + ext[1]) + tile, f32)
        for way, size in (("x", (NX, W)), ("y", (W, NY))):
            if kind in (way, "split"):
                out[f"fw{way}{c}"] = pltpu.VMEM(size + tile, f32)
                out[f"te{way}{c}"] = pltpu.VMEM(size + tile, f32)
    out["count"] = pltpu.VMEM((chunks * 8 * NX * NY,) + tile, f32)
    n = sum(ARRIVALS[KINDS[c % 3]] for c in range(chunks)) + len(SIDES) + 2
    out["send_sem"] = pltpu.SemaphoreType.DMA((ROUTES,))
    out["recv_sem"] = pltpu.SemaphoreType.DMA((n,))
    out["load_sem"] = pltpu.SemaphoreType.DMA((7,))
    return out


def split16(u):
    low = u - u.astype(bf16).astype(f32)
    return jnp.concatenate([u, low], axis=0).astype(bf16)


def add_side(box, acc, out_acc, w_late, n, again=None):
    a, sign = SIDES[n]
    NX, NY, F, NZ = acc.shape[0], acc.shape[1], acc.shape[2] // 2, acc.shape[3]
    length, across = ((NX, NY), (NY, NX))[a]
    linear_rows, smooth_rows = pl.ds(0, F), pl.ds(F, F)

    def spot(depth, i):
        at = length - 1 - depth if sign > 0 else depth
        return (at, i) if a == 0 else (i, at)

    for i0 in range(0, across, 2):
        columns, smooth = [], []
        for i in (i0, i0 + 1):
            near = []
            for h in range(1, H + 1):
                x, y = spot(-h, i)
                near.append(box[x + H, y + H])
            smooth.append((15.0 * near[0] - 6.0 * near[1] + near[2], near[1] - 6.0 * near[0], near[0]))
            parts = [split16(u[c:c + ROWS]) for u in near[:2] for c in range(0, F, ROWS)]
            columns.append(jnp.concatenate(parts, axis=0))
        out = jnp.dot(w_late[n], jnp.concatenate(columns, axis=1), preferred_element_type=f32)
        for q in range(2):
            part = out[:, q * NZ:(q + 1) * NZ]
            for d in range(H):
                x, y = spot(d, i0 + q)
                source = out_acc if again is not None and again(x, y) else acc
                linear = source[x, y, linear_rows]
                if d < 2:
                    mine = part[2 * F * d:2 * F * (d + 1)]
                    linear = linear + (mine[:F] + mine[F:])
                out_acc[x, y, linear_rows] = linear
                out_acc[x, y, smooth_rows] = source[x, y, smooth_rows] + smooth[q][d]


def finished(box, acc, x, y):
    u = box[x + H, y + H]
    F = u.shape[0]
    lapse = (1.0 + 0.25 * jnp.tanh(u[0:1])) * (1.0 / 12.0)
    slope = lapse * acc[x, y, pl.ds(0, F)] + acc[x, y, pl.ds(F, F)] * (1.0 / 64.0)
    return slope, u + 0.125 * slope


def kernel(
    dims, shift_hbm, now_hbm, parent_hbm, advect_hbm, diffuse_hbm, coef_hbm, band_hbm,
    slope_ref, value_ref, acc, box, w_late, *refs
):
    F, NX, NY, NZ = dims
    chunks = F // ROWS
    cells = NX * NY
    s = dict(zip(scratch(dims), refs))
    own, par, ub = s["own"], s["par"], s["ub"]
    epk, ein, rim, rim_up, rim_low = s["epk"], s["ein"], s["rim"], s["rim_up"], s["rim_low"]
    slots = NZ // SLOT
    groups = cells // slots
    me = {a: lax.axis_index(a) for a in AXES}
    size = {a: lax.axis_size(a) for a in AXES}
    below = {a: me[a] > 0 for a in AXES}
    above = {a: me[a] < size[a] - 1 for a in AXES}
    sems = iter(range(1000))
    kinds = [KINDS[c % 3] for c in range(chunks)]
    rows = [pl.ds(c * ROWS, ROWS) for c in range(chunks)]

    def load_cells(src, dst, n):
        def step(x, _):
            for y in range(NY):
                pltpu.make_async_copy(src.at[:, x * NY + y], dst.at[x, y], s["load_sem"].at[n]).start()
            return 0

        lax.fori_loop(0, NX, step, 0)

    singles = [
        pltpu.make_async_copy(src, dst, s["load_sem"].at[2 + n])
        for n, (src, dst) in enumerate((
            (shift_hbm, s["shift"]), (advect_hbm, s["advect"]),
            (diffuse_hbm, s["diffuse"]), (coef_hbm, s["coef"]), (band_hbm, s["band"]),
        ))
    ]
    DX, DY, DZ = {"gx": -1}, {"gy": -1}, {"gz": -1}
    UX, UY, UZ = {"gx": 1}, {"gy": 1}, {"gz": 1}
    barrier = pltpu.get_barrier_semaphore()
    count = 0
    for to in (DX, UX, DY, UY, DZ, UZ, UX | UZ, UY | UZ):
        cond = back = None
        for a, by in to.items():
            one, two = (below[a], above[a]) if by < 0 else (above[a], below[a])
            cond = one if cond is None else cond & one
            back = two if back is None else back & two

        @pl.when(cond)
        def _(to=to):
            pl.semaphore_signal(
                barrier, inc=1, device_id={a: me[a] + by for a, by in to.items()}, device_id_type=MESH
            )
        count = count + jnp.where(back, 1, 0)

    singles[0].start()
    load_cells(now_hbm, own, 0)
    pl.semaphore_wait(barrier, count)

    routes = {}

    class Route:
        def __init__(self, to):
            self.to = to
            self.send_sem = s["send_sem"].at[len(routes)]
            self.tiles = 0
            self.sends = self.gets = None
            for a, by in to.items():
                sends = below[a] if by < 0 else above[a]
                gets = above[a] if by < 0 else below[a]
                self.sends = sends if self.sends is None else self.sends & sends
                self.gets = gets if self.gets is None else self.gets & gets

        def copy(self, src, dst, recv_sem):
            return pltpu.make_async_remote_copy(
                src_ref=src, dst_ref=dst, send_sem=self.send_sem, recv_sem=recv_sem,
                device_id={a: me[a] + by for a, by in self.to.items()}, device_id_type=MESH,
            )

        def all_sent(self):
            done = s["count"].at[pl.ds(0, self.tiles // 2)]
            pl.when(self.sends)(self.copy(done, done, s["recv_sem"].at[0]).wait_send)

    def route(to):
        key = tuple(sorted(to.items()))
        if key not in routes:
            routes[key] = Route(to)
        return routes[key]

    class Arrival:
        def __init__(self, to):
            self.route = route(to)
            self.recv_sem = s["recv_sem"].at[next(sems)]
            self.tiles = 0

        def arrived(self):
            done = s["count"].at[pl.ds(0, self.tiles // 2)]
            pl.when(self.route.gets)(self.route.copy(done, done, self.recv_sem).wait_recv)

    def size_of(ref):
        return int(np.prod(ref.shape)) // (HALF * NZ)

    class Message:
        def __init__(self, src, dst, to, arrival=None):
            self.arrival = arrival or Arrival(to)
            self.route = route(to)
            tiles = size_of(dst)
            self.arrival.tiles += tiles
            self.route.tiles += tiles
            self.src, self.dst = src, dst

        def start(self):
            pl.when(self.route.sends)(self.route.copy(self.src, self.dst, self.arrival.recv_sem).start)

        def arrived(self):
            self.arrival.arrived()

    message = Message

    lowx, lowy = pl.ds(0, W), pl.ds(0, W)
    raw, edge, diag, forward = {}, {}, {}, {}
    whole = pl.ds(0, ROWS)

    def halves_of(src, dst, way, fields, to):
        arrival = Arrival(to)
        out = []
        for h in range(2):
            n = (NX if way == "x" else NY) // 2
            span = pl.ds(h * n, n)
            at = (span, slice(None), fields) if way == "x" else (slice(None), span, fields)
            out.append([message(src.at[at], dst.at[at], to, arrival)])
        return out

    for c, kind in enumerate(kinds):
        if kind == "x":
            spans = [pl.ds(h * (NY // 2), NY // 2) for h in range(2)]
            raw[c] = [message(own.at[lowx, n, rows[c]], s[f"rawx{c}"].at[:, n], DX) for n in spans]
            diag[c] = [message(epk.at[c, 0], ein.at[c, 2], DX | DZ)]
            forward[c] = halves_of(s[f"fwx{c}"], s[f"tex{c}"], "x", whole, DY)
        elif kind == "y":
            spans = [pl.ds(h * (NX // 2), NX // 2) for h in range(2)]
            raw[c] = [message(own.at[n, lowy, rows[c]], s[f"rawy{c}"].at[n], DY) for n in spans]
            diag[c] = [message(epk.at[c, 0], ein.at[c, 2], DY | DZ)]
            forward[c] = halves_of(s[f"fwy{c}"], s[f"tey{c}"], "y", whole, DX)
        else:
            a_rows, b_rows = pl.ds(0, HALF), pl.ds(HALF, HALF)
            raw[c] = [
                message(own.at[lowx, :, pl.ds(c * ROWS, HALF)], s[f"rawx{c}"].at[:, :, a_rows], DX),
                message(own.at[:, lowy, pl.ds(c * ROWS + HALF, HALF)], s[f"rawy{c}"].at[:, :, b_rows], DY),
            ]
            diag[c] = [
                message(epk.at[c, 0], ein.at[c, 2], DX | DZ), message(epk.at[c, 2], ein.at[c, 3], DY | DZ),
            ]
            along_x = halves_of(s[f"fwx{c}"], s[f"tex{c}"], "x", a_rows, DY)
            along_y = halves_of(s[f"fwy{c}"], s[f"tey{c}"], "y", b_rows, DX)
            forward[c] = [x + y for x, y in zip(along_x, along_y)]
        edge[c] = message(epk.at[c, pl.ds(0, 2)], ein.at[c, pl.ds(0, 2)], DZ)

    inside = {(a, sign): Arrival({AXES[a]: -sign}) for a, sign in SIDES}
    rims_in = [Arrival(DZ), Arrival(UZ)]

    def halo(c, a, by, lo, hi, part=None):
        fields = rows[c] if part is None else pl.ds(c * ROWS + part * HALF, HALF)
        n = (NX, NY)[a]
        src = pl.ds(H, H) if by < 0 else pl.ds(n, H)
        dst = pl.ds(n + H, H) if by < 0 else pl.ds(0, H)
        span = pl.ds(H + lo, hi - lo)
        to = {AXES[a]: by}
        if a == 0:
            return message(box.at[src, span, fields], box.at[dst, span, fields], to, inside[(a, -by)])
        return message(box.at[span, src, fields], box.at[span, dst, fields], to, inside[(a, -by)])

    early_halo, late_halo, rims = {}, {}, {}
    hx, hy = NX // 2, NY // 2
    for c, kind in enumerate(kinds):
        if kind == "x":
            early_halo[c] = [halo(c, 1, -1, 0, NX), halo(c, 0, 1, 0, hy)]
            late_halo[c] = [halo(c, 0, -1, 0, NY), halo(c, 0, 1, hy, NY), halo(c, 1, 1, 0, NX)]
        elif kind == "y":
            early_halo[c] = [halo(c, 0, -1, 0, NY), halo(c, 1, 1, 0, hx)]
            late_halo[c] = [halo(c, 1, -1, 0, NX), halo(c, 1, 1, hx, NX), halo(c, 0, 1, 0, NY)]
        else:
            early_halo[c] = [
                halo(c, 1, -1, 0, NX, 0), halo(c, 0, -1, 0, NY, 1), halo(c, 0, 1, 0, hy, 0), halo(c, 1, 1, 0, hx, 1),
            ]
            late_halo[c] = [
                halo(c, 0, -1, 0, NY, 0), halo(c, 1, -1, 0, NX, 1), halo(c, 0, 1, hy, NY, 0),
                halo(c, 1, 1, hx, NX, 1), halo(c, 0, 1, 0, NY, 1), halo(c, 1, 1, 0, NX, 0),
            ]
        rims[c] = [
            message(rim.at[c], rim_up.at[c], DZ, rims_in[0]), message(rim.at[c], rim_low.at[c], UZ, rims_in[1]),
        ]

    lane = lax.broadcasted_iota(jnp.int32, (ROWS, NZ), 1)
    thin = lane // W
    wide = ((lane + SLOT // 2) % NZ) // SLOT
    blank = jnp.zeros((ROWS, NZ), f32)

    def pack(c, n, along, q):
        packed = blank
        across = NY if along == "x" else NX
        for slot in range(W * across):
            i, j = q * W + slot // across, slot % across
            x, y = (i, j) if along == "x" else (j, i)
            packed = jnp.where(thin == slot, pltpu.roll(own[x, y, rows[c]], W * slot, 1), packed)
        epk[c, n] = packed

    pltpu.make_async_copy(par, own, s["load_sem"].at[0]).wait()
    one_way = [c for c in range(chunks) if kinds[c] != "split"]
    both = [c for c in range(chunks) if kinds[c] == "split"]
    for c in one_way:
        raw[c][0].start()
    for c in one_way:
        pack(c, 0, kinds[c], 0)
        diag[c][0].start()
        raw[c][1].start()
    for c in one_way:
        pack(c, 1, kinds[c], 1)
        edge[c].start()
    for c in both:
        pack(c, 0, "x", 0)
        pack(c, 2, "y", 0)
        for d in diag[c]:
            d.start()
        for r in raw[c]:
            r.start()
        pack(c, 1, "x", 1)
        edge[c].start()

    for load in singles[1:]:
        load.start()
    load_cells(parent_hbm, par, 1)
    zero16 = jnp.zeros((2 * ROWS, NZ), bf16)

    def clear(i, _):
        for c in range(chunks):
            for o in range(H):
                ub[o, i + H, c] = zero16
                ub[NX + H + o, i + H, c] = zero16
                ub[i + H, o, c] = zero16
                ub[i + H, NY + H + o, c] = zero16
        return 0

    lax.fori_loop(0, NX, clear, 0)

    singles[0].wait()
    move = [s["shift"][d] for d in range(3)]
    sz = move[2]

    def weights():
        for load in singles[1:]:
            load.wait()
        mats = []
        for m in (s["advect"], s["diffuse"]):
            for a in range(3):
                one = m[a]
                high = one.astype(bf16).astype(f32)
                mid = (one - high).astype(bf16).astype(f32)
                mats.append(jnp.concatenate([high, mid, one - high - mid], axis=0).astype(bf16))

        def columns(at, width, ks):
            table = s["coef"][:, at:at + width]
            hit = lax.broadcasted_iota(jnp.int32, (F, width), 0).astype(f32) == table[7:8]
            smooth = jnp.where(hit, table[6:7], 0.0)
            total = None
            for k in ks:
                spread = jnp.where(hit, table[k:k + 1], 0.0).astype(bf16)
                part = jnp.dot(mats[k], spread, preferred_element_type=f32)
                total = part if total is None else total + part
            w = total[:F] + total[F:2 * F] + total[2 * F:]
            high = w.astype(bf16).astype(f32)
            return jnp.concatenate([high, (w - high) * table[8:9], smooth], axis=0)

        k_early = len(BLOCKS) * 2 * F
        for at in range(0, up_to(k_early, 256), 256):
            n = min(256, k_early - at)
            s["w_early"][:, at:at + n] = columns(at, 256, range(6))[:, :n].astype(bf16)
        at = up_to(k_early, 256)
        k_along = len(ALONG) * 2 * F
        s["w_along"][...] = columns(at, up_to(k_along, 256), (2, 5))[:2 * F, :k_along].astype(bf16)
        at += up_to(k_along, 256)
        k_late = 2 * 2 * F
        step = up_to(k_late, 256)
        for n, (a, sign) in enumerate(SIDES):
            parts = [columns(at + d * step, step, (a, 3 + a))[:2 * F] for d in range(2)]
            w_late[n] = jnp.concatenate(parts, axis=0)[:, :k_late].astype(bf16)
            at += 2 * step

    def z_row(row, packed, slot):
        tail = pltpu.roll(packed, NZ - W * slot - sz, 1)
        return jnp.where(lane >= NZ - sz, tail, pltpu.roll(row, NZ - sz, 1))

    def z_own(c, xs, ys):
        kind = kinds[c]
        for x in range(*xs):
            for y in range(*ys):
                q, slot = (x // W, x % W * NY + y) if kind != "y" else (y // W, y % W * NX + x)
                s[f"zs{c}"][x, y] = z_row(own[x, y, rows[c]], ein[c, q], slot)

    def z_ext_x(c, lo, hi):
        for x in range(W):
            for y in range(lo, hi):
                s[f"zs{c}"][NX + x, y] = z_row(s[f"rawx{c}"][x, y], ein[c, 2], x * NY + y)

    def z_ext_y(c, lo, hi):
        n = 3 if kinds[c] == "split" else 2
        for x in range(lo, hi):
            for y in range(W):
                s[f"zs{c}"][x, NY + y] = z_row(s[f"rawy{c}"][x, y], ein[c, n], y * NX + x)

    def make_forward(c, half):
        zs = s[f"zs{c}"]

        def step(i, _):
            for j in range(W):
                if kinds[c] != "y":
                    s[f"fwx{c}"][i, j] = zs[i + move[0], j]
                if kinds[c] != "x":
                    s[f"fwy{c}"][j, i] = zs[j, i + move[1]]
            return 0

        lax.fori_loop(half * hx, (half + 1) * hx, step, 0)
        for f in forward[c][half]:
            f.start()

    in_z = me["gz"] * NZ + lane + sz < size["gz"] * NZ

    upper = lax.broadcasted_iota(jnp.int32, (ROWS, NZ), 0) < HALF

    def renew(c, xs, ys, late, part=None, whole=True):
        kind, zs = kinds[c], s[f"zs{c}"]

        def step(x, _):
            in_x = me["gx"] * NX + x + move[0] < size["gx"] * NX
            for y in range(*ys):
                in_y = me["gy"] * NY + y + move[1] < size["gy"] * NY
                X, Y = x + move[0], y + move[1]
                if late:
                    if kind != "y":
                        x_first = jnp.where(
                            Y < NY, zs[X, jnp.minimum(Y, NY - 1)], s[f"tex{c}"][x, jnp.maximum(Y - NY, 0)]
                        )
                    if kind != "x":
                        y_first = jnp.where(
                            X < NX, zs[jnp.minimum(X, NX - 1), Y], s[f"tey{c}"][jnp.maximum(X - NX, 0), y]
                        )
                    row = x_first if kind == "x" else y_first
                    if kind == "split":
                        row = jnp.where(upper, x_first, y_first)
                else:
                    row = zs[X, Y]
                row = jnp.where(in_z & (in_x & in_y), row, par[x, y, rows[c]])
                if part is None:
                    box[x + H, y + H, rows[c]] = row
                else:
                    kept = slice(part * HALF, (part + 1) * HALF)
                    box[x + H, y + H, pl.ds(c * ROWS + part * HALF, HALF)] = row[kept]
                if whole:
                    ub[x + H, y + H, c] = split16(row)
            return 0

        lax.fori_loop(*xs, step, 0)

    def renew_early(c):
        if kinds[c] == "x":
            renew(c, (0, NX), (0, hy), False)
        elif kinds[c] == "y":
            renew(c, (0, hx), (0, NY), False)
        else:
            renew(c, (0, hx), (0, hy), False)
            renew(c, (hx, NX), (0, hy), False, 0, False)
            renew(c, (0, hx), (hy, NY), False, 1, False)
        for h in early_halo[c]:
            h.start()

    def renew_late(c):
        for f in forward[c][0]:
            f.arrived()
        if kinds[c] == "x":
            renew(c, (0, NX), (hy, NY), True)
        elif kinds[c] == "y":
            renew(c, (hx, NX), (0, NY), True)
        else:
            renew(c, (hx, NX), (0, hy), True, 1)
            renew(c, (0, hx), (hy, NY), True, 0)
            renew(c, (hx, NX), (hy, NY), True)
        for h in late_halo[c]:
            h.start()

        for g in range(groups):
            packed = blank
            for j in range(slots):
                x, y = g * (slots // NY) + j // NY, j % NY
                packed = jnp.where(wide == j, pltpu.roll(box[x + H, y + H, rows[c]], SLOT * j, 1), packed)
            rim[c, g] = packed
        for r in rims[c]:
            r.start()

    for c in one_way:
        edge[c].arrived()
        z_own(c, (0, NX if kinds[c] == "x" else hx), (0, NY if kinds[c] == "y" else hy))
        make_forward(c, 0)
    for c in both:
        edge[c].arrived()
        z_own(c, (0, NX), (0, NY))
        make_forward(c, 0)
    for c in one_way:
        z_own(c, (0 if kinds[c] == "x" else hx, NX), (0 if kinds[c] == "y" else hy, NY))
    for c in one_way:
        diag[c][0].arrived()
        raw[c][0].arrived()
        if kinds[c] == "x":
            z_ext_x(c, 0, hy)
        else:
            z_ext_y(c, 0, hx)
        make_forward(c, 1)
    for c in one_way:
        raw[c][1].arrived()
        if kinds[c] == "x":
            z_ext_x(c, hy, NY)
        else:
            z_ext_y(c, hx, NX)
    for c in both:
        for d in diag[c]:
            d.arrived()
        raw[c][0].arrived()
        z_ext_x(c, 0, NY)
        raw[c][1].arrived()
        z_ext_y(c, 0, NX)
        make_forward(c, 1)
    pltpu.make_async_copy(own, par, s["load_sem"].at[1]).wait()
    for c in (*one_way, *both):
        renew_early(c)
    weights()
    for c in (*one_way, *both):
        renew_late(c)

    def early(x):
        for y0 in range(0, NY, 2):
            sides = []
            for y in (y0, y0 + 1):
                parts = []
                for a, o in BLOCKS:
                    dx, dy = (0, o) if a == 1 else (o, 0)
                    parts += [ub[x + H + dx, y + H + dy, c] for c in range(chunks)]
                sides.append(jnp.concatenate(parts, axis=0))
            out = jnp.dot(s["w_early"][...], jnp.concatenate(sides, axis=1), preferred_element_type=f32)
            for q in range(2):
                part = out[:, q * NZ:(q + 1) * NZ]
                smooth = part[2 * F:]
                for o in (-H, H):
                    for u, v in ((x + o, y0 + q), (x, y0 + q + o)):
                        if 0 <= u < NX and 0 <= v < NY:
                            smooth = smooth + box[u + H, v + H]
                acc[x, y0 + q, pl.ds(0, F)] = part[:F] + part[F:2 * F]
                acc[x, y0 + q, pl.ds(F, F)] = smooth

    for x in range(NX):
        early(x)

    def summed(spread, n):
        at = n * 2 * ROWS
        return spread[at:at + ROWS] + spread[at + ROWS:at + 2 * ROWS]

    def mixed_along(columns):
        sides = [
            jnp.concatenate([split16(t[:, n * NZ:(n + 1) * NZ]) for n in range(2) for t in terms], axis=0)
            for terms in columns
        ]
        out = jnp.dot(s["w_along"][...], jnp.concatenate(sides, axis=1), preferred_element_type=f32)
        out = out[:F] + out[F:]
        return [out[:, q * NZ:(q + 1) * NZ] for q in range(2)]

    def along(x):
        lines = [ub[x + H, y + H, c] for y in range(NY) for c in range(chunks)]
        spread = jnp.dot(jnp.concatenate(lines, axis=0), s["band"][:NZ], preferred_element_type=f32)
        terms = [[summed(spread, y * chunks + c) for c in range(chunks)] for y in range(NY)]
        for y0 in range(0, NY, 2):
            linear = mixed_along(terms[y0:y0 + 2])
            for q in range(2):
                acc[x, y0 + q, pl.ds(0, F)] += linear[q]
                for c in range(chunks):
                    acc[x, y0 + q, pl.ds(F + c * ROWS, ROWS)] += terms[y0 + q][c][:, 2 * NZ:]

    for x in range(NX):
        along(x)

    for r in rims_in:
        r.arrived()

    lines = []
    for g in range(groups):
        for c in range(chunks):
            lines.append(split16(jnp.where(
                lane % SLOT < SLOT // 2,
                jnp.where(above["gz"], rim_up[c, g], 0.0), jnp.where(below["gz"], rim_low[c, g], 0.0),
            )))
    spread = jnp.dot(jnp.concatenate(lines, axis=0), s["band"][NZ:], preferred_element_type=f32)
    terms = [[summed(spread, g * chunks + c) for c in range(chunks)] for g in range(groups)]
    at_ends = (lane < SLOT // 2) | (lane >= NZ - SLOT // 2)
    for g0 in range(0, groups, 2):
        linear = mixed_along(terms[g0:g0 + 2])
        for q in range(2):
            g = g0 + q
            lapse = (1.0 + 0.25 * jnp.tanh(rim[0, g, 0:1, :])) * (64.0 / 12.0)
            for c in range(chunks):
                extra = lapse * linear[q][c * ROWS:(c + 1) * ROWS] + terms[g][c][:, 2 * NZ:]
                for j in range(slots):
                    x, y = g * (slots // NY) + j // NY, j % NY
                    placed = jnp.where(at_ends, pltpu.roll(extra, (NZ - SLOT * j) % NZ, 1), 0.0)
                    acc[x, y, pl.ds(F + c * ROWS, ROWS)] += placed

    for a in range(2):
        n = SIDES.index((a, -1))
        inside[(a, -1)].arrived()
        pl.when(below[AXES[a]])(functools.partial(add_side, box, acc, acc, w_late, n))

    def finish(x, _):
        for y in range(NY - H):
            slope_ref[x * NY + y], value_ref[x * NY + y] = finished(box, acc, x, y)
        return 0

    lax.fori_loop(0, NX - H, finish, 0)

    for a in range(2):
        inside[(a, 1)].arrived()

        @pl.when(jnp.logical_not(above[AXES[a]]))
        def _(a=a):
            def step(i, _):
                for h in range(H):
                    at = (NX, NY)[a] + H + h
                    where = (at, i + H) if a == 0 else (i + H, at)
                    box[where] = jnp.zeros((F, NZ), f32)
                return 0

            lax.fori_loop(0, (NY, NX)[a], step, 0)

    for r in routes.values():
        r.all_sent()


def put_out(slope_in, value_in, acc_in, box, w_late, slope_hbm, value_hbm, slope_rest, value_rest, acc, sem):
    NX, NY = acc_in.shape[:2]
    sources = ((slope_in, slope_rest, slope_hbm), (value_in, value_rest, value_hbm))

    def send(x, y, rest):
        k = x * NY + y
        for n, source in enumerate(sources):
            pltpu.make_async_copy(source[rest].at[k], source[2].at[:, k], sem.at[n]).start()

    for x in range(NX - H):
        for y in range(NY - H):
            send(x, y, 0)
    add_side(box, acc_in, acc, w_late, SIDES.index((0, 1)))
    add_side(box, acc_in, acc, w_late, SIDES.index((1, 1)), lambda x, y: x >= NX - H)

    def finish(x, y):
        k = x * NY + y
        slope_rest[k], value_rest[k] = finished(box, acc, x, y)

    for x in range(NX):
        for y in range(NY - H if x < NX - H else 0, NY):
            finish(x, y)
            send(x, y, 1)
    for n in range(2):
        pltpu.make_async_copy(slope_rest, value_rest, sem.at[n]).wait()


def local(fields_now, parent, advect, diffuse, box_shift):
    dims = fields_now.shape
    F, NX, NY, NZ = dims
    flat = (F, NX * NY, NZ)
    by_cell = (NX * NY, F, NZ)
    vmem = pl.BlockSpec(memory_space=pltpu.VMEM)
    hbm = pl.BlockSpec(memory_space=pltpu.HBM)
    operands = [
        pltpu.with_memory_space_constraint(x, pltpu.HBM)
        for x in (
            box_shift, fields_now.reshape(flat), parent.reshape(flat), advect, diffuse,
            jnp.asarray(coefficients(F)), jnp.asarray(band(NZ), bf16),
        )
    ]
    held = [
        pltpu.VMEM((NX, NY, 2 * F, NZ), f32),
        pltpu.VMEM((NX + 2 * H, NY + 2 * H, F, NZ), f32),
        pltpu.VMEM((len(SIDES), 4 * F, 4 * F), bf16),
    ]
    results = pl.pallas_call(
        functools.partial(kernel, dims),
        out_shape=[pltpu.VMEM(by_cell, f32)] * 2 + held,
        in_specs=[hbm] * len(operands),
        out_specs=[vmem] * 5,
        scratch_shapes=list(scratch(dims).values()),
        compiler_params=pltpu.CompilerParams(
            collective_id=0, has_side_effects=True, vmem_limit_bytes=VMEM_BYTES
        ),
    )(*operands)
    slope, value = pl.pallas_call(
        put_out,
        out_shape=[jax.ShapeDtypeStruct(flat, f32)] * 2,
        in_specs=[vmem] * 5,
        out_specs=[hbm] * 2,
        scratch_shapes=[pltpu.VMEM(by_cell, f32)] * 2 + [held[0], pltpu.SemaphoreType.DMA((2,))],
        compiler_params=pltpu.CompilerParams(vmem_limit_bytes=VMEM_BYTES),
    )(*results)
    return slope.reshape(dims), value.reshape(dims)


VMEM_BYTES = 40 * 2**20


def solution(mesh):
    return jax.shard_map(
        local,
        mesh=mesh,
        in_specs=(P(None, "gx", "gy", "gz"), P(None, "gx", "gy", "gz"), P(), P(), P()),
        out_specs=(P(None, "gx", "gy", "gz"), P(None, "gx", "gy", "gz")),
        check_vma=False,
    )
```

```python
import functools

import jax
import jax.numpy as jnp
import numpy as np
from jax import lax
from jax.experimental import pallas as pl
from jax.experimental.pallas import tpu as pltpu
from jax.sharding import PartitionSpec as P

MESH = pl.DeviceIdType.MESH
W = 4
H = 3
SLOT = 8
ROWS = 8
AXES = ("gx", "gy", "gz")
KINDS = ("x", "y", "split")
HALF = ROWS // 2
ARRIVALS = {"x": 5, "y": 5, "split": 7}
ROUTES = 8
FIRST = {-2: 1, -1: -8, 1: 8, 2: -1}
SECOND = {-2: -1, -1: 16, 0: -30, 1: 16, 2: -1}
SIXTH = {-3: 1, -2: -6, -1: 15, 0: -20, 1: 15, 2: -6, 3: 1}
BLOCKS = [(None, 0)] + [(a, o) for a in range(2) for o in (-2, -1, 1, 2)]
ALONG = [(2, "first"), (2, "second")]
SIDES = [(a, sign) for a in range(2) for sign in (-1, 1)]
f32, bf16 = jnp.float32, jnp.bfloat16


def up_to(n, m):
    return -(-n // m) * m


def block_columns(block, fields):
    cols = np.zeros((16, 2 * fields), np.float32)
    for c in range(fields // ROWS):
        for h in range(2):
            for r in range(ROWS):
                n = (c * 2 + h) * ROWS + r
                cols[7, n] = c * ROWS + r
                cols[8, n] = 1 - h
    if block is None:
        return cols
    axis, o = block
    if o in ("first", "second"):
        cols[axis + (3 if o == "second" else 0)] = 1
        return cols
    for a in range(3):
        if axis is None or a == axis:
            cols[a] = FIRST.get(o, 0)
            cols[3 + a] = SECOND.get(o, 0)
            cols[6] += SIXTH[o]
    return cols


def coefficients(fields):
    groups = [BLOCKS, ALONG]
    for a, sign in SIDES:
        groups += [[(a, sign), (a, 2 * sign)], [(a, 2 * sign), None]]
    out = []
    for g in groups:
        cols = np.concatenate([block_columns(b, fields) for b in g], axis=1)
        out.append(np.pad(cols, ((0, 0), (0, up_to(cols.shape[1], 256) - cols.shape[1]))))
    return np.concatenate(out, axis=1)


def band(length):
    out = np.zeros((2, length, 3, length), np.float32)
    for n, terms in enumerate((FIRST, SECOND, SIXTH)):
        for o, factor in terms.items():
            for lane in range(length):
                if o and 0 <= lane + o < length:
                    out[0, lane + o, n, lane] = factor
                at = (lane + SLOT // 2) % SLOT - SLOT // 2
                if (0 <= at + o < H and at < 0) or (-H <= at + o < 0 <= at):
                    out[1, (lane + o) % length, n, lane] = factor
    return out.reshape(2 * length, 3 * length)


def scratch(dims):
    F, NX, NY, NZ = dims
    chunks = F // ROWS
    groups = NX * NY * SLOT // NZ
    tile = (ROWS, NZ)
    out = dict(
        shift=pltpu.SMEM((3,), jnp.int32),
        own=pltpu.VMEM((NX, NY, F, NZ), f32),
        par=pltpu.VMEM((NX, NY, F, NZ), f32),
        advect=pltpu.VMEM((3, F, F), f32),
        diffuse=pltpu.VMEM((3, F, F), f32),
        coef=pltpu.VMEM(coefficients(F).shape, f32),
        band=pltpu.VMEM((2 * NZ, 3 * NZ), bf16),
        w_early=pltpu.VMEM((3 * F, len(BLOCKS) * 2 * F), bf16),
        w_along=pltpu.VMEM((2 * F, len(ALONG) * 2 * F), bf16),
        ub=pltpu.VMEM((NX + 2 * H, NY + 2 * H, chunks, 2 * ROWS, NZ), bf16),
        rim=pltpu.VMEM((chunks, groups) + tile, f32),
        rim_up=pltpu.VMEM((chunks, groups) + tile, f32),
        rim_low=pltpu.VMEM((chunks, groups) + tile, f32),
        epk=pltpu.VMEM((chunks, 3) + tile, f32),
        ein=pltpu.VMEM((chunks, 4) + tile, f32),
    )
    for c in range(chunks):
        kind = KINDS[c % 3]
        if kind != "y":
            out[f"rawx{c}"] = pltpu.VMEM((W, NY) + tile, f32)
        if kind != "x":
            out[f"rawy{c}"] = pltpu.VMEM((NX, W) + tile, f32)
        ext = (W if kind != "y" else 0, W if kind != "x" else 0)
        out[f"zs{c}"] = pltpu.VMEM((NX + ext[0], NY + ext[1]) + tile, f32)
        for way, size in (("x", (NX, W)), ("y", (W, NY))):
            if kind in (way, "split"):
                out[f"fw{way}{c}"] = pltpu.VMEM(size + tile, f32)
                out[f"te{way}{c}"] = pltpu.VMEM(size + tile, f32)
    out["count"] = pltpu.VMEM((chunks * 8 * NX * NY,) + tile, f32)
    n = sum(ARRIVALS[KINDS[c % 3]] for c in range(chunks)) + len(SIDES) + 2
    out["send_sem"] = pltpu.SemaphoreType.DMA((ROUTES,))
    out["recv_sem"] = pltpu.SemaphoreType.DMA((n,))
    out["load_sem"] = pltpu.SemaphoreType.DMA((7,))
    return out


def split16(u):
    low = u - u.astype(bf16).astype(f32)
    return jnp.concatenate([u, low], axis=0).astype(bf16)


def add_side(box, acc, out_acc, w_late, n, again=None):
    a, sign = SIDES[n]
    NX, NY, F, NZ = acc.shape[0], acc.shape[1], acc.shape[2] // 2, acc.shape[3]
    length, across = ((NX, NY), (NY, NX))[a]
    linear_rows, smooth_rows = pl.ds(0, F), pl.ds(F, F)

    def spot(depth, i):
        at = length - 1 - depth if sign > 0 else depth
        return (at, i) if a == 0 else (i, at)

    for i0 in range(0, across, 2):
        columns, smooth = [], []
        for i in (i0, i0 + 1):
            near = []
            for h in range(1, H + 1):
                x, y = spot(-h, i)
                near.append(box[x + H, y + H])
            smooth.append((15.0 * near[0] - 6.0 * near[1] + near[2], near[1] - 6.0 * near[0], near[0]))
            parts = [split16(u[c:c + ROWS]) for u in near[:2] for c in range(0, F, ROWS)]
            columns.append(jnp.concatenate(parts, axis=0))
        out = jnp.dot(w_late[n], jnp.concatenate(columns, axis=1), preferred_element_type=f32)
        for q in range(2):
            part = out[:, q * NZ:(q + 1) * NZ]
            for d in range(H):
                x, y = spot(d, i0 + q)
                source = out_acc if again is not None and again(x, y) else acc
                linear = source[x, y, linear_rows]
                if d < 2:
                    mine = part[2 * F * d:2 * F * (d + 1)]
                    linear = linear + (mine[:F] + mine[F:])
                out_acc[x, y, linear_rows] = linear
                out_acc[x, y, smooth_rows] = source[x, y, smooth_rows] + smooth[q][d]


def finished(box, acc, x, y):
    u = box[x + H, y + H]
    F = u.shape[0]
    lapse = (1.0 + 0.25 * jnp.tanh(u[0:1])) * (1.0 / 12.0)
    slope = lapse * acc[x, y, pl.ds(0, F)] + acc[x, y, pl.ds(F, F)] * (1.0 / 64.0)
    return slope, u + 0.125 * slope


def kernel(
    dims, shift_hbm, now_hbm, parent_hbm, advect_hbm, diffuse_hbm, coef_hbm, band_hbm,
    slope_ref, value_ref, acc, box, w_late, *refs
):
    F, NX, NY, NZ = dims
    chunks = F // ROWS
    cells = NX * NY
    s = dict(zip(scratch(dims), refs))
    own, par, ub = s["own"], s["par"], s["ub"]
    epk, ein, rim, rim_up, rim_low = s["epk"], s["ein"], s["rim"], s["rim_up"], s["rim_low"]
    slots = NZ // SLOT
    groups = cells // slots
    me = {a: lax.axis_index(a) for a in AXES}
    size = {a: lax.axis_size(a) for a in AXES}
    below = {a: me[a] > 0 for a in AXES}
    above = {a: me[a] < size[a] - 1 for a in AXES}
    sems = iter(range(1000))
    kinds = [KINDS[c % 3] for c in range(chunks)]
    rows = [pl.ds(c * ROWS, ROWS) for c in range(chunks)]

    def load_cells(src, dst, n):
        def step(x, _):
            for y in range(NY):
                pltpu.make_async_copy(src.at[:, x * NY + y], dst.at[x, y], s["load_sem"].at[n]).start()
            return 0

        lax.fori_loop(0, NX, step, 0)

    singles = [
        pltpu.make_async_copy(src, dst, s["load_sem"].at[2 + n])
        for n, (src, dst) in enumerate((
            (shift_hbm, s["shift"]), (advect_hbm, s["advect"]),
            (diffuse_hbm, s["diffuse"]), (coef_hbm, s["coef"]), (band_hbm, s["band"]),
        ))
    ]
    DX, DY, DZ = {"gx": -1}, {"gy": -1}, {"gz": -1}
    UX, UY, UZ = {"gx": 1}, {"gy": 1}, {"gz": 1}
    barrier = pltpu.get_barrier_semaphore()
    count = 0
    for to in (UX, UY, UZ, UX | UZ, UY | UZ):
        cond = back = None
        for a, by in to.items():
            one, two = (below[a], above[a]) if by < 0 else (above[a], below[a])
            cond = one if cond is None else cond & one
            back = two if back is None else back & two

        @pl.when(cond)
        def _(to=to):
            pl.semaphore_signal(
                barrier, inc=1, device_id={a: me[a] + by for a, by in to.items()}, device_id_type=MESH
            )
        count = count + jnp.where(back, 1, 0)

    singles[0].start()
    load_cells(now_hbm, own, 0)
    @pl.when(count > 0)
    def _():
        pl.semaphore_wait(barrier, count)


    routes = {}

    class Route:
        def __init__(self, to):
            self.to = to
            self.send_sem = s["send_sem"].at[len(routes)]
            self.tiles = 0
            self.sends = self.gets = None
            for a, by in to.items():
                sends = below[a] if by < 0 else above[a]
                gets = above[a] if by < 0 else below[a]
                self.sends = sends if self.sends is None else self.sends & sends
                self.gets = gets if self.gets is None else self.gets & gets

        def copy(self, src, dst, recv_sem):
            return pltpu.make_async_remote_copy(
                src_ref=src, dst_ref=dst, send_sem=self.send_sem, recv_sem=recv_sem,
                device_id={a: me[a] + by for a, by in self.to.items()}, device_id_type=MESH,
            )

        def all_sent(self):
            done = s["count"].at[pl.ds(0, self.tiles // 2)]
            pl.when(self.sends)(self.copy(done, done, s["recv_sem"].at[0]).wait_send)

    def route(to):
        key = tuple(sorted(to.items()))
        if key not in routes:
            routes[key] = Route(to)
        return routes[key]

    class Arrival:
        def __init__(self, to):
            self.route = route(to)
            self.recv_sem = s["recv_sem"].at[next(sems)]
            self.tiles = 0

        def arrived(self):
            done = s["count"].at[pl.ds(0, self.tiles // 2)]
            pl.when(self.route.gets)(self.route.copy(done, done, self.recv_sem).wait_recv)

    def size_of(ref):
        return int(np.prod(ref.shape)) // (HALF * NZ)

    class Message:
        def __init__(self, src, dst, to, arrival=None, parts=None):
            self.arrival = arrival or Arrival(to)
            self.route = route(to)
            tiles = size_of(dst)
            self.arrival.tiles += tiles
            self.route.tiles += tiles
            self.src, self.dst, self.parts = src, dst, parts

        def start(self):
            pl.when(self.route.sends)(self.route.copy(self.src, self.dst, self.arrival.recv_sem).start)

        def start_parts(self, i):
            @pl.when(self.route.sends)
            def _():
                for j in range(W):
                    self.route.copy(*self.parts(i, j), self.arrival.recv_sem).start()

        def arrived(self):
            self.arrival.arrived()

    message = Message

    lowx, lowy = pl.ds(0, W), pl.ds(0, W)
    raw, edge, diag, forward = {}, {}, {}, {}
    whole = pl.ds(0, ROWS)

    def halves_of(src, dst, way, fields, to):
        arrival = Arrival(to)
        out = []
        for h in range(2):
            n = (NX if way == "x" else NY) // 2
            span = pl.ds(h * n, n)
            at = (span, slice(None), fields) if way == "x" else (slice(None), span, fields)
            out.append([message(src.at[at], dst.at[at], to, arrival)])
        return out

    for c, kind in enumerate(kinds):
        if kind == "x":
            def cell(i, j, half, c=c):
                x, y = i, j + half * (NY // 2)
                return now_hbm.at[rows[c], x * NY + y], s[f"rawx{c}"].at[x, y]

            halves = [s[f"rawx{c}"].at[:, pl.ds(h * (NY // 2), NY // 2)] for h in range(2)]
            raw[c] = [message(r, r, DX, parts=functools.partial(cell, half=h)) for h, r in enumerate(halves)]
            diag[c] = [message(epk.at[c, 0], ein.at[c, 2], DX | DZ)]
            forward[c] = halves_of(s[f"fwx{c}"], s[f"tex{c}"], "x", whole, DY)
        elif kind == "y":
            def cell(i, j, half, c=c):
                x, y = i + half * (NX // 2), j
                return now_hbm.at[rows[c], x * NY + y], s[f"rawy{c}"].at[x, y]

            halves = [s[f"rawy{c}"].at[pl.ds(h * (NX // 2), NX // 2)] for h in range(2)]
            raw[c] = [message(r, r, DY, parts=functools.partial(cell, half=h)) for h, r in enumerate(halves)]
            diag[c] = [message(epk.at[c, 0], ein.at[c, 2], DY | DZ)]
            forward[c] = halves_of(s[f"fwy{c}"], s[f"tey{c}"], "y", whole, DX)
        else:
            a_rows, b_rows = pl.ds(0, HALF), pl.ds(HALF, HALF)
            raw[c] = [
                message(own.at[lowx, :, pl.ds(c * ROWS, HALF)], s[f"rawx{c}"].at[:, :, a_rows], DX),
                message(own.at[:, lowy, pl.ds(c * ROWS + HALF, HALF)], s[f"rawy{c}"].at[:, :, b_rows], DY),
            ]
            diag[c] = [
                message(epk.at[c, 0], ein.at[c, 2], DX | DZ), message(epk.at[c, 2], ein.at[c, 3], DY | DZ),
            ]
            along_x = halves_of(s[f"fwx{c}"], s[f"tex{c}"], "x", a_rows, DY)
            along_y = halves_of(s[f"fwy{c}"], s[f"tey{c}"], "y", b_rows, DX)
            forward[c] = [x + y for x, y in zip(along_x, along_y)]
        edge[c] = message(epk.at[c, pl.ds(0, 2)], ein.at[c, pl.ds(0, 2)], DZ)

    inside = {(a, sign): Arrival({AXES[a]: -sign}) for a, sign in SIDES}
    rims_in = [Arrival(DZ), Arrival(UZ)]

    def halo(c, a, by, lo, hi, part=None):
        fields = rows[c] if part is None else pl.ds(c * ROWS + part * HALF, HALF)
        n = (NX, NY)[a]
        src = pl.ds(H, H) if by < 0 else pl.ds(n, H)
        dst = pl.ds(n + H, H) if by < 0 else pl.ds(0, H)
        span = pl.ds(H + lo, hi - lo)
        to = {AXES[a]: by}
        if a == 0:
            return message(box.at[src, span, fields], box.at[dst, span, fields], to, inside[(a, -by)])
        return message(box.at[span, src, fields], box.at[span, dst, fields], to, inside[(a, -by)])

    early_halo, late_halo, rims = {}, {}, {}
    hx, hy = NX // 2, NY // 2
    for c, kind in enumerate(kinds):
        if kind == "x":
            early_halo[c] = [halo(c, 1, -1, 0, NX), halo(c, 0, 1, 0, hy)]
            late_halo[c] = [halo(c, 0, -1, 0, NY), halo(c, 0, 1, hy, NY), halo(c, 1, 1, 0, NX)]
        elif kind == "y":
            early_halo[c] = [halo(c, 0, -1, 0, NY), halo(c, 1, 1, 0, hx)]
            late_halo[c] = [halo(c, 1, -1, 0, NX), halo(c, 1, 1, hx, NX), halo(c, 0, 1, 0, NY)]
        else:
            early_halo[c] = [
                halo(c, 1, -1, 0, NX, 0), halo(c, 0, -1, 0, NY, 1), halo(c, 0, 1, 0, hy, 0), halo(c, 1, 1, 0, hx, 1),
            ]
            late_halo[c] = [
                halo(c, 0, -1, 0, NY, 0), halo(c, 1, -1, 0, NX, 1), halo(c, 0, 1, hy, NY, 0),
                halo(c, 1, 1, hx, NX, 1), halo(c, 0, 1, 0, NY, 1), halo(c, 1, 1, 0, NX, 0),
            ]
        rims[c] = [
            message(rim.at[c], rim_up.at[c], DZ, rims_in[0]), message(rim.at[c], rim_low.at[c], UZ, rims_in[1]),
        ]

    def send_raw(i, _, half):
        for c, kind in enumerate(kinds):
            if kind != "split":
                raw[c][half].start_parts(i)
        return 0

    def send_raws(half, lo, hi):
        lax.fori_loop(lo, hi, functools.partial(send_raw, half=half), 0)

    send_raws(0, 0, W)
    send_raws(1, 0, W // 2)

    lane = lax.broadcasted_iota(jnp.int32, (ROWS, NZ), 1)
    thin = lane // W
    wide = ((lane + SLOT // 2) % NZ) // SLOT
    blank = jnp.zeros((ROWS, NZ), f32)

    def pack(c, n, along, q):
        packed = blank
        across = NY if along == "x" else NX
        for slot in range(W * across):
            i, j = q * W + slot // across, slot % across
            x, y = (i, j) if along == "x" else (j, i)
            packed = jnp.where(thin == slot, pltpu.roll(own[x, y, rows[c]], W * slot, 1), packed)
        epk[c, n] = packed

    pltpu.make_async_copy(par, own, s["load_sem"].at[0]).wait()
    one_way = [c for c in range(chunks) if kinds[c] != "split"]
    both = [c for c in range(chunks) if kinds[c] == "split"]
    for c in one_way:
        pack(c, 0, kinds[c], 0)
        diag[c][0].start()
    send_raws(1, W // 2, W)
    for c in one_way:
        pack(c, 1, kinds[c], 1)
        edge[c].start()
    for c in both:
        pack(c, 0, "x", 0)
        pack(c, 2, "y", 0)
        for d in diag[c]:
            d.start()
        for r in raw[c]:
            r.start()
        pack(c, 1, "x", 1)
        edge[c].start()

    for load in singles[1:]:
        load.start()
    load_cells(parent_hbm, par, 1)
    zero16 = jnp.zeros((2 * ROWS, NZ), bf16)

    def clear(i, _):
        for c in range(chunks):
            for o in range(H):
                ub[o, i + H, c] = zero16
                ub[NX + H + o, i + H, c] = zero16
                ub[i + H, o, c] = zero16
                ub[i + H, NY + H + o, c] = zero16
        return 0

    lax.fori_loop(0, NX, clear, 0)

    singles[0].wait()
    move = [s["shift"][d] for d in range(3)]
    sz = move[2]

    def weights():
        for load in singles[1:]:
            load.wait()
        mats = []
        for m in (s["advect"], s["diffuse"]):
            for a in range(3):
                one = m[a]
                high = one.astype(bf16).astype(f32)
                mid = (one - high).astype(bf16).astype(f32)
                mats.append(jnp.concatenate([high, mid, one - high - mid], axis=0).astype(bf16))

        def columns(at, width, ks):
            table = s["coef"][:, at:at + width]
            hit = lax.broadcasted_iota(jnp.int32, (F, width), 0).astype(f32) == table[7:8]
            smooth = jnp.where(hit, table[6:7], 0.0)
            total = None
            for k in ks:
                spread = jnp.where(hit, table[k:k + 1], 0.0).astype(bf16)
                part = jnp.dot(mats[k], spread, preferred_element_type=f32)
                total = part if total is None else total + part
            w = total[:F] + total[F:2 * F] + total[2 * F:]
            high = w.astype(bf16).astype(f32)
            return jnp.concatenate([high, (w - high) * table[8:9], smooth], axis=0)

        k_early = len(BLOCKS) * 2 * F
        for at in range(0, up_to(k_early, 256), 256):
            n = min(256, k_early - at)
            s["w_early"][:, at:at + n] = columns(at, 256, range(6))[:, :n].astype(bf16)
        at = up_to(k_early, 256)
        k_along = len(ALONG) * 2 * F
        s["w_along"][...] = columns(at, up_to(k_along, 256), (2, 5))[:2 * F, :k_along].astype(bf16)
        at += up_to(k_along, 256)
        k_late = 2 * 2 * F
        step = up_to(k_late, 256)
        for n, (a, sign) in enumerate(SIDES):
            parts = [columns(at + d * step, step, (a, 3 + a))[:2 * F] for d in range(2)]
            w_late[n] = jnp.concatenate(parts, axis=0)[:, :k_late].astype(bf16)
            at += 2 * step

    def z_row(row, packed, slot):
        tail = pltpu.roll(packed, NZ - W * slot - sz, 1)
        return jnp.where(lane >= NZ - sz, tail, pltpu.roll(row, NZ - sz, 1))

    def z_own(c, xs, ys):
        kind = kinds[c]
        for x in range(*xs):
            for y in range(*ys):
                q, slot = (x // W, x % W * NY + y) if kind != "y" else (y // W, y % W * NX + x)
                s[f"zs{c}"][x, y] = z_row(own[x, y, rows[c]], ein[c, q], slot)

    def z_ext_x(c, lo, hi):
        for x in range(W):
            for y in range(lo, hi):
                s[f"zs{c}"][NX + x, y] = z_row(s[f"rawx{c}"][x, y], ein[c, 2], x * NY + y)

    def z_ext_y(c, lo, hi):
        n = 3 if kinds[c] == "split" else 2
        for x in range(lo, hi):
            for y in range(W):
                s[f"zs{c}"][x, NY + y] = z_row(s[f"rawy{c}"][x, y], ein[c, n], y * NX + x)

    def make_forward(c, half):
        zs = s[f"zs{c}"]

        def step(i, _):
            for j in range(W):
                if kinds[c] != "y":
                    s[f"fwx{c}"][i, j] = zs[i + move[0], j]
                if kinds[c] != "x":
                    s[f"fwy{c}"][j, i] = zs[j, i + move[1]]
            return 0

        lax.fori_loop(half * hx, (half + 1) * hx, step, 0)
        for f in forward[c][half]:
            f.start()

    in_z = me["gz"] * NZ + lane + sz < size["gz"] * NZ

    upper = lax.broadcasted_iota(jnp.int32, (ROWS, NZ), 0) < HALF

    def renew(c, xs, ys, late, part=None, whole=True):
        kind, zs = kinds[c], s[f"zs{c}"]

        def step(x, _):
            in_x = me["gx"] * NX + x + move[0] < size["gx"] * NX
            for y in range(*ys):
                in_y = me["gy"] * NY + y + move[1] < size["gy"] * NY
                X, Y = x + move[0], y + move[1]
                if late:
                    if kind != "y":
                        x_first = jnp.where(
                            Y < NY, zs[X, jnp.minimum(Y, NY - 1)], s[f"tex{c}"][x, jnp.maximum(Y - NY, 0)]
                        )
                    if kind != "x":
                        y_first = jnp.where(
                            X < NX, zs[jnp.minimum(X, NX - 1), Y], s[f"tey{c}"][jnp.maximum(X - NX, 0), y]
                        )
                    row = x_first if kind == "x" else y_first
                    if kind == "split":
                        row = jnp.where(upper, x_first, y_first)
                else:
                    row = zs[X, Y]
                row = jnp.where(in_z & (in_x & in_y), row, par[x, y, rows[c]])
                if part is None:
                    box[x + H, y + H, rows[c]] = row
                else:
                    kept = slice(part * HALF, (part + 1) * HALF)
                    box[x + H, y + H, pl.ds(c * ROWS + part * HALF, HALF)] = row[kept]
                if whole:
                    ub[x + H, y + H, c] = split16(row)
            return 0

        lax.fori_loop(*xs, step, 0)

    def renew_early(c):
        if kinds[c] == "x":
            renew(c, (0, NX), (0, hy), False)
        elif kinds[c] == "y":
            renew(c, (0, hx), (0, NY), False)
        else:
            renew(c, (0, hx), (0, hy), False)
            renew(c, (hx, NX), (0, hy), False, 0, False)
            renew(c, (0, hx), (hy, NY), False, 1, False)
        for h in early_halo[c]:
            h.start()

    def renew_late(c):
        for f in forward[c][0]:
            f.arrived()
        if kinds[c] == "x":
            renew(c, (0, NX), (hy, NY), True)
        elif kinds[c] == "y":
            renew(c, (hx, NX), (0, NY), True)
        else:
            renew(c, (hx, NX), (0, hy), True, 1)
            renew(c, (0, hx), (hy, NY), True, 0)
            renew(c, (hx, NX), (hy, NY), True)
        for h in late_halo[c]:
            h.start()

        for g in range(groups):
            packed = blank
            for j in range(slots):
                x, y = g * (slots // NY) + j // NY, j % NY
                packed = jnp.where(wide == j, pltpu.roll(box[x + H, y + H, rows[c]], SLOT * j, 1), packed)
            rim[c, g] = packed
        for r in rims[c]:
            r.start()

    for c in one_way:
        edge[c].arrived()
        z_own(c, (0, NX if kinds[c] == "x" else hx), (0, NY if kinds[c] == "y" else hy))
        make_forward(c, 0)
    for c in both:
        edge[c].arrived()
        z_own(c, (0, NX), (0, NY))
        make_forward(c, 0)
    for c in one_way:
        z_own(c, (0 if kinds[c] == "x" else hx, NX), (0 if kinds[c] == "y" else hy, NY))
    for c in one_way:
        diag[c][0].arrived()
        raw[c][0].arrived()
        if kinds[c] == "x":
            z_ext_x(c, 0, hy)
        else:
            z_ext_y(c, 0, hx)
        make_forward(c, 1)
    for c in one_way:
        raw[c][1].arrived()
        if kinds[c] == "x":
            z_ext_x(c, hy, NY)
        else:
            z_ext_y(c, hx, NX)
    for c in both:
        for d in diag[c]:
            d.arrived()
        raw[c][0].arrived()
        z_ext_x(c, 0, NY)
        raw[c][1].arrived()
        z_ext_y(c, 0, NX)
        make_forward(c, 1)
    pltpu.make_async_copy(own, par, s["load_sem"].at[1]).wait()
    for c in (*one_way, *both):
        renew_early(c)
    weights()
    for c in (*one_way, *both):
        renew_late(c)

    def early(x):
        for y0 in range(0, NY, 2):
            sides = []
            for y in (y0, y0 + 1):
                parts = []
                for a, o in BLOCKS:
                    dx, dy = (0, o) if a == 1 else (o, 0)
                    parts += [ub[x + H + dx, y + H + dy, c] for c in range(chunks)]
                sides.append(jnp.concatenate(parts, axis=0))
            out = jnp.dot(s["w_early"][...], jnp.concatenate(sides, axis=1), preferred_element_type=f32)
            for q in range(2):
                part = out[:, q * NZ:(q + 1) * NZ]
                smooth = part[2 * F:]
                for o in (-H, H):
                    for u, v in ((x + o, y0 + q), (x, y0 + q + o)):
                        if 0 <= u < NX and 0 <= v < NY:
                            smooth = smooth + box[u + H, v + H]
                acc[x, y0 + q, pl.ds(0, F)] = part[:F] + part[F:2 * F]
                acc[x, y0 + q, pl.ds(F, F)] = smooth

    for x in range(NX):
        early(x)

    def summed(spread, n):
        at = n * 2 * ROWS
        return spread[at:at + ROWS] + spread[at + ROWS:at + 2 * ROWS]

    def mixed_along(columns):
        sides = [
            jnp.concatenate([split16(t[:, n * NZ:(n + 1) * NZ]) for n in range(2) for t in terms], axis=0)
            for terms in columns
        ]
        out = jnp.dot(s["w_along"][...], jnp.concatenate(sides, axis=1), preferred_element_type=f32)
        out = out[:F] + out[F:]
        return [out[:, q * NZ:(q + 1) * NZ] for q in range(2)]

    def along(x):
        lines = [ub[x + H, y + H, c] for y in range(NY) for c in range(chunks)]
        spread = jnp.dot(jnp.concatenate(lines, axis=0), s["band"][:NZ], preferred_element_type=f32)
        terms = [[summed(spread, y * chunks + c) for c in range(chunks)] for y in range(NY)]
        for y0 in range(0, NY, 2):
            linear = mixed_along(terms[y0:y0 + 2])
            for q in range(2):
                acc[x, y0 + q, pl.ds(0, F)] += linear[q]
                for c in range(chunks):
                    acc[x, y0 + q, pl.ds(F + c * ROWS, ROWS)] += terms[y0 + q][c][:, 2 * NZ:]

    for x in range(NX):
        along(x)

    for r in rims_in:
        r.arrived()

    lines = []
    for g in range(groups):
        for c in range(chunks):
            lines.append(split16(jnp.where(
                lane % SLOT < SLOT // 2,
                jnp.where(above["gz"], rim_up[c, g], 0.0), jnp.where(below["gz"], rim_low[c, g], 0.0),
            )))
    spread = jnp.dot(jnp.concatenate(lines, axis=0), s["band"][NZ:], preferred_element_type=f32)
    terms = [[summed(spread, g * chunks + c) for c in range(chunks)] for g in range(groups)]
    at_ends = (lane < SLOT // 2) | (lane >= NZ - SLOT // 2)
    for g0 in range(0, groups, 2):
        linear = mixed_along(terms[g0:g0 + 2])
        for q in range(2):
            g = g0 + q
            lapse = (1.0 + 0.25 * jnp.tanh(rim[0, g, 0:1, :])) * (64.0 / 12.0)
            for c in range(chunks):
                extra = lapse * linear[q][c * ROWS:(c + 1) * ROWS] + terms[g][c][:, 2 * NZ:]
                for j in range(slots):
                    x, y = g * (slots // NY) + j // NY, j % NY
                    placed = jnp.where(at_ends, pltpu.roll(extra, (NZ - SLOT * j) % NZ, 1), 0.0)
                    acc[x, y, pl.ds(F + c * ROWS, ROWS)] += placed

    for a in range(2):
        n = SIDES.index((a, -1))
        inside[(a, -1)].arrived()
        pl.when(below[AXES[a]])(functools.partial(add_side, box, acc, acc, w_late, n))

    def finish(x, _):
        for y in range(NY - H):
            slope_ref[x * NY + y], value_ref[x * NY + y] = finished(box, acc, x, y)
        return 0

    lax.fori_loop(0, NX - H, finish, 0)

    for a in range(2):
        inside[(a, 1)].arrived()

        @pl.when(jnp.logical_not(above[AXES[a]]))
        def _(a=a):
            def step(i, _):
                for h in range(H):
                    at = (NX, NY)[a] + H + h
                    where = (at, i + H) if a == 0 else (i + H, at)
                    box[where] = jnp.zeros((F, NZ), f32)
                return 0

            lax.fori_loop(0, (NY, NX)[a], step, 0)

    for r in routes.values():
        r.all_sent()


def put_out(slope_in, value_in, acc_in, box, w_late, slope_hbm, value_hbm, slope_rest, value_rest, acc, sem):
    NX, NY = acc_in.shape[:2]
    sources = ((slope_in, slope_rest, slope_hbm), (value_in, value_rest, value_hbm))

    def send(x, y, rest):
        k = x * NY + y
        for n, source in enumerate(sources):
            pltpu.make_async_copy(source[rest].at[k], source[2].at[:, k], sem.at[n]).start()

    for x in range(NX - H):
        for y in range(NY - H):
            send(x, y, 0)
    add_side(box, acc_in, acc, w_late, SIDES.index((0, 1)))
    add_side(box, acc_in, acc, w_late, SIDES.index((1, 1)), lambda x, y: x >= NX - H)

    def finish(x, y):
        k = x * NY + y
        slope_rest[k], value_rest[k] = finished(box, acc, x, y)

    for x in range(NX):
        for y in range(NY - H if x < NX - H else 0, NY):
            finish(x, y)
            send(x, y, 1)
    for n in range(2):
        pltpu.make_async_copy(slope_rest, value_rest, sem.at[n]).wait()


def local(fields_now, parent, advect, diffuse, box_shift):
    dims = fields_now.shape
    F, NX, NY, NZ = dims
    flat = (F, NX * NY, NZ)
    by_cell = (NX * NY, F, NZ)
    vmem = pl.BlockSpec(memory_space=pltpu.VMEM)
    hbm = pl.BlockSpec(memory_space=pltpu.HBM)
    operands = [
        pltpu.with_memory_space_constraint(x, pltpu.HBM)
        for x in (
            box_shift, fields_now.reshape(flat), parent.reshape(flat), advect, diffuse,
            jnp.asarray(coefficients(F)), jnp.asarray(band(NZ), bf16),
        )
    ]
    held = [
        pltpu.VMEM((NX, NY, 2 * F, NZ), f32),
        pltpu.VMEM((NX + 2 * H, NY + 2 * H, F, NZ), f32),
        pltpu.VMEM((len(SIDES), 4 * F, 4 * F), bf16),
    ]
    results = pl.pallas_call(
        functools.partial(kernel, dims),
        out_shape=[pltpu.VMEM(by_cell, f32)] * 2 + held,
        in_specs=[hbm] * len(operands),
        out_specs=[vmem] * 5,
        scratch_shapes=list(scratch(dims).values()),
        compiler_params=pltpu.CompilerParams(
            collective_id=0, has_side_effects=True, vmem_limit_bytes=VMEM_BYTES
        ),
    )(*operands)
    slope, value = pl.pallas_call(
        put_out,
        out_shape=[jax.ShapeDtypeStruct(flat, f32)] * 2,
        in_specs=[vmem] * 5,
        out_specs=[hbm] * 2,
        scratch_shapes=[pltpu.VMEM(by_cell, f32)] * 2 + [held[0], pltpu.SemaphoreType.DMA((2,))],
        compiler_params=pltpu.CompilerParams(vmem_limit_bytes=VMEM_BYTES),
    )(*results)
    return slope.reshape(dims), value.reshape(dims)


VMEM_BYTES = 40 * 2**20


def solution(mesh):
    return jax.shard_map(
        local,
        mesh=mesh,
        in_specs=(P(None, "gx", "gy", "gz"), P(None, "gx", "gy", "gz"), P(), P(), P()),
        out_specs=(P(None, "gx", "gy", "gz"), P(None, "gx", "gy", "gz")),
        check_vma=False,
    )
```

```python
import functools

import jax
import jax.numpy as jnp
import numpy as np
from jax import lax
from jax.experimental import pallas as pl
from jax.experimental.pallas import tpu as pltpu
from jax.sharding import PartitionSpec as P

MESH = pl.DeviceIdType.MESH
W = 4
H = 3
SLOT = 8
ROWS = 8
AXES = ("gx", "gy", "gz")
KINDS = ("x", "y", "split")
HALF = ROWS // 2
ARRIVALS = {"x": 5, "y": 5, "split": 7}
ROUTES = 8
FIRST = {-2: 1, -1: -8, 1: 8, 2: -1}
SECOND = {-2: -1, -1: 16, 0: -30, 1: 16, 2: -1}
SIXTH = {-3: 1, -2: -6, -1: 15, 0: -20, 1: 15, 2: -6, 3: 1}
BLOCKS = [(None, 0)] + [(a, o) for a in range(2) for o in (-2, -1, 1, 2)]
ALONG = [(2, "first"), (2, "second")]
SIDES = [(a, sign) for a in range(2) for sign in (-1, 1)]
f32, bf16 = jnp.float32, jnp.bfloat16


def up_to(n, m):
    return -(-n // m) * m


def block_columns(block, fields):
    cols = np.zeros((16, 2 * fields), np.float32)
    for c in range(fields // ROWS):
        for h in range(2):
            for r in range(ROWS):
                n = (c * 2 + h) * ROWS + r
                cols[7, n] = c * ROWS + r
                cols[8, n] = 1 - h
    if block is None:
        return cols
    axis, o = block
    if o in ("first", "second"):
        cols[axis + (3 if o == "second" else 0)] = 1
        return cols
    for a in range(3):
        if axis is None or a == axis:
            cols[a] = FIRST.get(o, 0)
            cols[3 + a] = SECOND.get(o, 0)
            cols[6] += SIXTH[o]
    return cols


def coefficients(fields):
    groups = [BLOCKS, ALONG]
    for a, sign in SIDES:
        groups += [[(a, sign), (a, 2 * sign)], [(a, 2 * sign), None]]
    out = []
    for g in groups:
        cols = np.concatenate([block_columns(b, fields) for b in g], axis=1)
        out.append(np.pad(cols, ((0, 0), (0, up_to(cols.shape[1], 256) - cols.shape[1]))))
    return np.concatenate(out, axis=1)


def band(length):
    out = np.zeros((2, length, 3, length), np.float32)
    for n, terms in enumerate((FIRST, SECOND, SIXTH)):
        for o, factor in terms.items():
            for lane in range(length):
                if o and 0 <= lane + o < length:
                    out[0, lane + o, n, lane] = factor
                at = (lane + SLOT // 2) % SLOT - SLOT // 2
                if (0 <= at + o < H and at < 0) or (-H <= at + o < 0 <= at):
                    out[1, (lane + o) % length, n, lane] = factor
    return out.reshape(2 * length, 3 * length)


def scratch(dims):
    F, NX, NY, NZ = dims
    chunks = F // ROWS
    groups = NX * NY * SLOT // NZ
    tile = (ROWS, NZ)
    out = dict(
        shift=pltpu.SMEM((3,), jnp.int32),
        own=pltpu.VMEM((NX, NY, F, NZ), f32),
        par=pltpu.VMEM((NX, NY, F, NZ), f32),
        advect=pltpu.VMEM((3, F, F), f32),
        diffuse=pltpu.VMEM((3, F, F), f32),
        coef=pltpu.VMEM(coefficients(F).shape, f32),
        band=pltpu.VMEM((2 * NZ, 3 * NZ), bf16),
        w_early=pltpu.VMEM((3 * F, len(BLOCKS) * 2 * F), bf16),
        w_along=pltpu.VMEM((2 * F, len(ALONG) * 2 * F), bf16),
        ub=pltpu.VMEM((NX + 2 * H, NY + 2 * H, chunks, 2 * ROWS, NZ), bf16),
        rim=pltpu.VMEM((chunks, groups) + tile, f32),
        rim_up=pltpu.VMEM((chunks, groups) + tile, f32),
        rim_low=pltpu.VMEM((chunks, groups) + tile, f32),
        epk=pltpu.VMEM((chunks, 3) + tile, f32),
        ein=pltpu.VMEM((chunks, 4) + tile, f32),
    )
    for c in range(chunks):
        kind = KINDS[c % 3]
        if kind != "y":
            out[f"rawx{c}"] = pltpu.VMEM((W, NY) + tile, f32)
        if kind != "x":
            out[f"rawy{c}"] = pltpu.VMEM((NX, W) + tile, f32)
        ext = (W if kind != "y" else 0, W if kind != "x" else 0)
        out[f"zs{c}"] = pltpu.VMEM((NX + ext[0], NY + ext[1]) + tile, f32)
        for way, size in (("x", (NX, W)), ("y", (W, NY))):
            if kind in (way, "split"):
                out[f"fw{way}{c}"] = pltpu.VMEM(size + tile, f32)
                out[f"te{way}{c}"] = pltpu.VMEM(size + tile, f32)
    out["count"] = pltpu.VMEM((chunks * 8 * NX * NY,) + tile, f32)
    n = sum(ARRIVALS[KINDS[c % 3]] for c in range(chunks)) + len(SIDES) + 2
    out["send_sem"] = pltpu.SemaphoreType.DMA((ROUTES,))
    out["recv_sem"] = pltpu.SemaphoreType.DMA((n,))
    out["load_sem"] = pltpu.SemaphoreType.DMA((7,))
    return out


def split16(u):
    low = u - u.astype(bf16).astype(f32)
    return jnp.concatenate([u, low], axis=0).astype(bf16)


def add_side(box, acc, out_acc, w_late, n, again=None):
    a, sign = SIDES[n]
    NX, NY, F, NZ = acc.shape[0], acc.shape[1], acc.shape[2] // 2, acc.shape[3]
    length, across = ((NX, NY), (NY, NX))[a]
    linear_rows, smooth_rows = pl.ds(0, F), pl.ds(F, F)

    def spot(depth, i):
        at = length - 1 - depth if sign > 0 else depth
        return (at, i) if a == 0 else (i, at)

    for i0 in range(0, across, 2):
        columns, smooth = [], []
        for i in (i0, i0 + 1):
            near = []
            for h in range(1, H + 1):
                x, y = spot(-h, i)
                near.append(box[x + H, y + H])
            smooth.append((15.0 * near[0] - 6.0 * near[1] + near[2], near[1] - 6.0 * near[0], near[0]))
            parts = [split16(u[c:c + ROWS]) for u in near[:2] for c in range(0, F, ROWS)]
            columns.append(jnp.concatenate(parts, axis=0))
        out = jnp.dot(w_late[n], jnp.concatenate(columns, axis=1), preferred_element_type=f32)
        for q in range(2):
            part = out[:, q * NZ:(q + 1) * NZ]
            for d in range(H):
                x, y = spot(d, i0 + q)
                source = out_acc if again is not None and again(x, y) else acc
                linear = source[x, y, linear_rows]
                if d < 2:
                    mine = part[2 * F * d:2 * F * (d + 1)]
                    linear = linear + (mine[:F] + mine[F:])
                out_acc[x, y, linear_rows] = linear
                out_acc[x, y, smooth_rows] = source[x, y, smooth_rows] + smooth[q][d]


def finished(box, acc, x, y):
    u = box[x + H, y + H]
    F = u.shape[0]
    lapse = (1.0 + 0.25 * jnp.tanh(u[0:1])) * (1.0 / 12.0)
    slope = lapse * acc[x, y, pl.ds(0, F)] + acc[x, y, pl.ds(F, F)] * (1.0 / 64.0)
    return slope, u + 0.125 * slope


def kernel(
    dims, shift_hbm, now_hbm, parent_hbm, advect_hbm, diffuse_hbm, coef_hbm, band_hbm,
    slope_ref, value_ref, acc, box, w_late, *refs
):
    F, NX, NY, NZ = dims
    chunks = F // ROWS
    cells = NX * NY
    s = dict(zip(scratch(dims), refs))
    own, par, ub = s["own"], s["par"], s["ub"]
    epk, ein, rim, rim_up, rim_low = s["epk"], s["ein"], s["rim"], s["rim_up"], s["rim_low"]
    slots = NZ // SLOT
    groups = cells // slots
    me = {a: lax.axis_index(a) for a in AXES}
    size = {a: lax.axis_size(a) for a in AXES}
    below = {a: me[a] > 0 for a in AXES}
    above = {a: me[a] < size[a] - 1 for a in AXES}
    sems = iter(range(1000))
    kinds = [KINDS[c % 3] for c in range(chunks)]
    rows = [pl.ds(c * ROWS, ROWS) for c in range(chunks)]

    def load_cells(src, dst, n):
        def step(x, _):
            for y in range(NY):
                pltpu.make_async_copy(src.at[:, x * NY + y], dst.at[x, y], s["load_sem"].at[n]).start()
            return 0

        lax.fori_loop(0, NX, step, 0)

    singles = [
        pltpu.make_async_copy(src, dst, s["load_sem"].at[2 + n])
        for n, (src, dst) in enumerate((
            (shift_hbm, s["shift"]), (advect_hbm, s["advect"]),
            (diffuse_hbm, s["diffuse"]), (coef_hbm, s["coef"]), (band_hbm, s["band"]),
        ))
    ]
    DX, DY, DZ = {"gx": -1}, {"gy": -1}, {"gz": -1}
    UX, UY, UZ = {"gx": 1}, {"gy": 1}, {"gz": 1}
    barrier = pltpu.get_barrier_semaphore()
    count = 0
    for to in (UX, UY, UZ, UX | UZ, UY | UZ):
        cond = back = None
        for a, by in to.items():
            one, two = (below[a], above[a]) if by < 0 else (above[a], below[a])
            cond = one if cond is None else cond & one
            back = two if back is None else back & two

        @pl.when(cond)
        def _(to=to):
            pl.semaphore_signal(
                barrier, inc=1, device_id={a: me[a] + by for a, by in to.items()}, device_id_type=MESH
            )
        count = count + jnp.where(back, 1, 0)

    singles[0].start()
    load_cells(now_hbm, own, 0)
    @pl.when(count > 0)
    def _():
        pl.semaphore_wait(barrier, count)


    routes = {}

    class Route:
        def __init__(self, to):
            self.to = to
            self.send_sem = s["send_sem"].at[len(routes)]
            self.tiles = 0
            self.sends = self.gets = None
            for a, by in to.items():
                sends = below[a] if by < 0 else above[a]
                gets = above[a] if by < 0 else below[a]
                self.sends = sends if self.sends is None else self.sends & sends
                self.gets = gets if self.gets is None else self.gets & gets

        def copy(self, src, dst, recv_sem):
            return pltpu.make_async_remote_copy(
                src_ref=src, dst_ref=dst, send_sem=self.send_sem, recv_sem=recv_sem,
                device_id={a: me[a] + by for a, by in self.to.items()}, device_id_type=MESH,
            )

        def all_sent(self):
            done = s["count"].at[pl.ds(0, self.tiles // 2)]
            pl.when(self.sends)(self.copy(done, done, s["recv_sem"].at[0]).wait_send)

    def route(to):
        key = tuple(sorted(to.items()))
        if key not in routes:
            routes[key] = Route(to)
        return routes[key]

    class Arrival:
        def __init__(self, to):
            self.route = route(to)
            self.recv_sem = s["recv_sem"].at[next(sems)]
            self.tiles = 0

        def arrived(self):
            done = s["count"].at[pl.ds(0, self.tiles // 2)]
            pl.when(self.route.gets)(self.route.copy(done, done, self.recv_sem).wait_recv)

    def size_of(ref):
        return int(np.prod(ref.shape)) // (HALF * NZ)

    class Message:
        def __init__(self, src, dst, to, arrival=None, parts=None):
            self.arrival = arrival or Arrival(to)
            self.route = route(to)
            tiles = size_of(dst)
            self.arrival.tiles += tiles
            self.route.tiles += tiles
            self.src, self.dst, self.parts = src, dst, parts

        def start(self):
            pl.when(self.route.sends)(self.route.copy(self.src, self.dst, self.arrival.recv_sem).start)

        def start_parts(self, i):
            @pl.when(self.route.sends)
            def _():
                for j in range(W):
                    self.route.copy(*self.parts(i, j), self.arrival.recv_sem).start()

        def arrived(self):
            self.arrival.arrived()

    message = Message

    lowx, lowy = pl.ds(0, W), pl.ds(0, W)
    raw, edge, diag, forward = {}, {}, {}, {}
    whole = pl.ds(0, ROWS)

    def halves_of(src, dst, way, fields, to):
        arrival = Arrival(to)
        out = []
        for h in range(2):
            n = (NX if way == "x" else NY) // 2
            span = pl.ds(h * n, n)
            at = (span, slice(None), fields) if way == "x" else (slice(None), span, fields)
            out.append([message(src.at[at], dst.at[at], to, arrival)])
        return out

    for c, kind in enumerate(kinds):
        if kind == "x":
            def cell(i, j, half, c=c):
                x, y = i, j + half * (NY // 2)
                return now_hbm.at[rows[c], x * NY + y], s[f"rawx{c}"].at[x, y]

            halves = [s[f"rawx{c}"].at[:, pl.ds(h * (NY // 2), NY // 2)] for h in range(2)]
            raw[c] = [
                message(halves[0], halves[0], DX, parts=functools.partial(cell, half=0)),
                message(own.at[lowx, pl.ds(NY // 2, NY // 2), rows[c]], halves[1], DX),
            ]
            diag[c] = [message(epk.at[c, 0], ein.at[c, 2], DX | DZ)]
            forward[c] = halves_of(s[f"fwx{c}"], s[f"tex{c}"], "x", whole, DY)
        elif kind == "y":
            def cell(i, j, half, c=c):
                x, y = i + half * (NX // 2), j
                return now_hbm.at[rows[c], x * NY + y], s[f"rawy{c}"].at[x, y]

            halves = [s[f"rawy{c}"].at[pl.ds(h * (NX // 2), NX // 2)] for h in range(2)]
            raw[c] = [
                message(halves[0], halves[0], DY, parts=functools.partial(cell, half=0)),
                message(own.at[pl.ds(NX // 2, NX // 2), lowy, rows[c]], halves[1], DY),
            ]
            diag[c] = [message(epk.at[c, 0], ein.at[c, 2], DY | DZ)]
            forward[c] = halves_of(s[f"fwy{c}"], s[f"tey{c}"], "y", whole, DX)
        else:
            a_rows, b_rows = pl.ds(0, HALF), pl.ds(HALF, HALF)
            raw[c] = [
                message(own.at[lowx, :, pl.ds(c * ROWS, HALF)], s[f"rawx{c}"].at[:, :, a_rows], DX),
                message(own.at[:, lowy, pl.ds(c * ROWS + HALF, HALF)], s[f"rawy{c}"].at[:, :, b_rows], DY),
            ]
            diag[c] = [
                message(epk.at[c, 0], ein.at[c, 2], DX | DZ), message(epk.at[c, 2], ein.at[c, 3], DY | DZ),
            ]
            along_x = halves_of(s[f"fwx{c}"], s[f"tex{c}"], "x", a_rows, DY)
            along_y = halves_of(s[f"fwy{c}"], s[f"tey{c}"], "y", b_rows, DX)
            forward[c] = [x + y for x, y in zip(along_x, along_y)]
        edge[c] = message(epk.at[c, pl.ds(0, 2)], ein.at[c, pl.ds(0, 2)], DZ)

    inside = {(a, sign): Arrival({AXES[a]: -sign}) for a, sign in SIDES}
    rims_in = [Arrival(DZ), Arrival(UZ)]

    def halo(c, a, by, lo, hi, part=None):
        fields = rows[c] if part is None else pl.ds(c * ROWS + part * HALF, HALF)
        n = (NX, NY)[a]
        src = pl.ds(H, H) if by < 0 else pl.ds(n, H)
        dst = pl.ds(n + H, H) if by < 0 else pl.ds(0, H)
        span = pl.ds(H + lo, hi - lo)
        to = {AXES[a]: by}
        if a == 0:
            return message(box.at[src, span, fields], box.at[dst, span, fields], to, inside[(a, -by)])
        return message(box.at[span, src, fields], box.at[span, dst, fields], to, inside[(a, -by)])

    early_halo, late_halo, rims = {}, {}, {}
    hx, hy = NX // 2, NY // 2
    for c, kind in enumerate(kinds):
        if kind == "x":
            early_halo[c] = [halo(c, 1, -1, 0, NX), halo(c, 0, 1, 0, hy)]
            late_halo[c] = [halo(c, 0, -1, 0, NY), halo(c, 0, 1, hy, NY), halo(c, 1, 1, 0, NX)]
        elif kind == "y":
            early_halo[c] = [halo(c, 0, -1, 0, NY), halo(c, 1, 1, 0, hx)]
            late_halo[c] = [halo(c, 1, -1, 0, NX), halo(c, 1, 1, hx, NX), halo(c, 0, 1, 0, NY)]
        else:
            early_halo[c] = [
                halo(c, 1, -1, 0, NX, 0), halo(c, 0, -1, 0, NY, 1), halo(c, 0, 1, 0, hy, 0), halo(c, 1, 1, 0, hx, 1),
            ]
            late_halo[c] = [
                halo(c, 0, -1, 0, NY, 0), halo(c, 1, -1, 0, NX, 1), halo(c, 0, 1, hy, NY, 0),
                halo(c, 1, 1, hx, NX, 1), halo(c, 0, 1, 0, NY, 1), halo(c, 1, 1, 0, NX, 0),
            ]
        rims[c] = [
            message(rim.at[c], rim_up.at[c], DZ, rims_in[0]), message(rim.at[c], rim_low.at[c], UZ, rims_in[1]),
        ]

    def send_raw(i, _, half):
        for c, kind in enumerate(kinds):
            if kind != "split":
                raw[c][half].start_parts(i)
        return 0

    def send_raws(half, lo, hi):
        lax.fori_loop(lo, hi, functools.partial(send_raw, half=half), 0)

    send_raws(0, 0, W)

    lane = lax.broadcasted_iota(jnp.int32, (ROWS, NZ), 1)
    thin = lane // W
    wide = ((lane + SLOT // 2) % NZ) // SLOT
    blank = jnp.zeros((ROWS, NZ), f32)

    def pack(c, n, along, q):
        packed = blank
        across = NY if along == "x" else NX
        for slot in range(W * across):
            i, j = q * W + slot // across, slot % across
            x, y = (i, j) if along == "x" else (j, i)
            packed = jnp.where(thin == slot, pltpu.roll(own[x, y, rows[c]], W * slot, 1), packed)
        epk[c, n] = packed

    pltpu.make_async_copy(par, own, s["load_sem"].at[0]).wait()
    one_way = [c for c in range(chunks) if kinds[c] != "split"]
    both = [c for c in range(chunks) if kinds[c] == "split"]
    for c in one_way:
        pack(c, 0, kinds[c], 0)
        diag[c][0].start()
        raw[c][1].start()
    for c in one_way:
        pack(c, 1, kinds[c], 1)
        edge[c].start()
    for c in both:
        pack(c, 0, "x", 0)
        pack(c, 2, "y", 0)
        for d in diag[c]:
            d.start()
        for r in raw[c]:
            r.start()
        pack(c, 1, "x", 1)
        edge[c].start()

    for load in singles[1:]:
        load.start()
    load_cells(parent_hbm, par, 1)
    zero16 = jnp.zeros((2 * ROWS, NZ), bf16)

    def clear(i, _):
        for c in range(chunks):
            for o in range(H):
                ub[o, i + H, c] = zero16
                ub[NX + H + o, i + H, c] = zero16
                ub[i + H, o, c] = zero16
                ub[i + H, NY + H + o, c] = zero16
        return 0

    lax.fori_loop(0, NX, clear, 0)

    singles[0].wait()
    move = [s["shift"][d] for d in range(3)]
    sz = move[2]

    def weights():
        for load in singles[1:]:
            load.wait()
        mats = []
        for m in (s["advect"], s["diffuse"]):
            for a in range(3):
                one = m[a]
                high = one.astype(bf16).astype(f32)
                mid = (one - high).astype(bf16).astype(f32)
                mats.append(jnp.concatenate([high, mid, one - high - mid], axis=0).astype(bf16))

        def columns(at, width, ks):
            table = s["coef"][:, at:at + width]
            hit = lax.broadcasted_iota(jnp.int32, (F, width), 0).astype(f32) == table[7:8]
            smooth = jnp.where(hit, table[6:7], 0.0)
            total = None
            for k in ks:
                spread = jnp.where(hit, table[k:k + 1], 0.0).astype(bf16)
                part = jnp.dot(mats[k], spread, preferred_element_type=f32)
                total = part if total is None else total + part
            w = total[:F] + total[F:2 * F] + total[2 * F:]
            high = w.astype(bf16).astype(f32)
            return jnp.concatenate([high, (w - high) * table[8:9], smooth], axis=0)

        k_early = len(BLOCKS) * 2 * F
        for at in range(0, up_to(k_early, 256), 256):
            n = min(256, k_early - at)
            s["w_early"][:, at:at + n] = columns(at, 256, range(6))[:, :n].astype(bf16)
        at = up_to(k_early, 256)
        k_along = len(ALONG) * 2 * F
        s["w_along"][...] = columns(at, up_to(k_along, 256), (2, 5))[:2 * F, :k_along].astype(bf16)
        at += up_to(k_along, 256)
        k_late = 2 * 2 * F
        step = up_to(k_late, 256)
        for n, (a, sign) in enumerate(SIDES):
            parts = [columns(at + d * step, step, (a, 3 + a))[:2 * F] for d in range(2)]
            w_late[n] = jnp.concatenate(parts, axis=0)[:, :k_late].astype(bf16)
            at += 2 * step

    def z_row(row, packed, slot):
        tail = pltpu.roll(packed, NZ - W * slot - sz, 1)
        return jnp.where(lane >= NZ - sz, tail, pltpu.roll(row, NZ - sz, 1))

    def z_own(c, xs, ys):
        kind = kinds[c]
        for x in range(*xs):
            for y in range(*ys):
                q, slot = (x // W, x % W * NY + y) if kind != "y" else (y // W, y % W * NX + x)
                s[f"zs{c}"][x, y] = z_row(own[x, y, rows[c]], ein[c, q], slot)

    def z_ext_x(c, lo, hi):
        for x in range(W):
            for y in range(lo, hi):
                s[f"zs{c}"][NX + x, y] = z_row(s[f"rawx{c}"][x, y], ein[c, 2], x * NY + y)

    def z_ext_y(c, lo, hi):
        n = 3 if kinds[c] == "split" else 2
        for x in range(lo, hi):
            for y in range(W):
                s[f"zs{c}"][x, NY + y] = z_row(s[f"rawy{c}"][x, y], ein[c, n], y * NX + x)

    def make_forward(c, half):
        zs = s[f"zs{c}"]

        def step(i, _):
            for j in range(W):
                if kinds[c] != "y":
                    s[f"fwx{c}"][i, j] = zs[i + move[0], j]
                if kinds[c] != "x":
                    s[f"fwy{c}"][j, i] = zs[j, i + move[1]]
            return 0

        lax.fori_loop(half * hx, (half + 1) * hx, step, 0)
        for f in forward[c][half]:
            f.start()

    in_z = me["gz"] * NZ + lane + sz < size["gz"] * NZ

    upper = lax.broadcasted_iota(jnp.int32, (ROWS, NZ), 0) < HALF

    def renew(c, xs, ys, late, part=None, whole=True):
        kind, zs = kinds[c], s[f"zs{c}"]

        def step(x, _):
            in_x = me["gx"] * NX + x + move[0] < size["gx"] * NX
            for y in range(*ys):
                in_y = me["gy"] * NY + y + move[1] < size["gy"] * NY
                X, Y = x + move[0], y + move[1]
                if late:
                    if kind != "y":
                        x_first = jnp.where(
                            Y < NY, zs[X, jnp.minimum(Y, NY - 1)], s[f"tex{c}"][x, jnp.maximum(Y - NY, 0)]
                        )
                    if kind != "x":
                        y_first = jnp.where(
                            X < NX, zs[jnp.minimum(X, NX - 1), Y], s[f"tey{c}"][jnp.maximum(X - NX, 0), y]
                        )
                    row = x_first if kind == "x" else y_first
                    if kind == "split":
                        row = jnp.where(upper, x_first, y_first)
                else:
                    row = zs[X, Y]
                row = jnp.where(in_z & (in_x & in_y), row, par[x, y, rows[c]])
                if part is None:
                    box[x + H, y + H, rows[c]] = row
                else:
                    kept = slice(part * HALF, (part + 1) * HALF)
                    box[x + H, y + H, pl.ds(c * ROWS + part * HALF, HALF)] = row[kept]
                if whole:
                    ub[x + H, y + H, c] = split16(row)
            return 0

        lax.fori_loop(*xs, step, 0)

    def renew_early(c):
        if kinds[c] == "x":
            renew(c, (0, NX), (0, hy), False)
        elif kinds[c] == "y":
            renew(c, (0, hx), (0, NY), False)
        else:
            renew(c, (0, hx), (0, hy), False)
            renew(c, (hx, NX), (0, hy), False, 0, False)
            renew(c, (0, hx), (hy, NY), False, 1, False)
        for h in early_halo[c]:
            h.start()

    def renew_late(c):
        for f in forward[c][0]:
            f.arrived()
        if kinds[c] == "x":
            renew(c, (0, NX), (hy, NY), True)
        elif kinds[c] == "y":
            renew(c, (hx, NX), (0, NY), True)
        else:
            renew(c, (hx, NX), (0, hy), True, 1)
            renew(c, (0, hx), (hy, NY), True, 0)
            renew(c, (hx, NX), (hy, NY), True)
        for h in late_halo[c]:
            h.start()

        for g in range(groups):
            packed = blank
            for j in range(slots):
                x, y = g * (slots // NY) + j // NY, j % NY
                packed = jnp.where(wide == j, pltpu.roll(box[x + H, y + H, rows[c]], SLOT * j, 1), packed)
            rim[c, g] = packed
        for r in rims[c]:
            r.start()

    for c in one_way:
        edge[c].arrived()
        z_own(c, (0, NX if kinds[c] == "x" else hx), (0, NY if kinds[c] == "y" else hy))
        make_forward(c, 0)
    for c in both:
        edge[c].arrived()
        z_own(c, (0, NX), (0, NY))
        make_forward(c, 0)
    for c in one_way:
        z_own(c, (0 if kinds[c] == "x" else hx, NX), (0 if kinds[c] == "y" else hy, NY))
    for c in one_way:
        diag[c][0].arrived()
        raw[c][0].arrived()
        if kinds[c] == "x":
            z_ext_x(c, 0, hy)
        else:
            z_ext_y(c, 0, hx)
        make_forward(c, 1)
    for c in one_way:
        raw[c][1].arrived()
        if kinds[c] == "x":
            z_ext_x(c, hy, NY)
        else:
            z_ext_y(c, hx, NX)
    for c in both:
        for d in diag[c]:
            d.arrived()
        raw[c][0].arrived()
        z_ext_x(c, 0, NY)
        raw[c][1].arrived()
        z_ext_y(c, 0, NX)
        make_forward(c, 1)
    pltpu.make_async_copy(own, par, s["load_sem"].at[1]).wait()
    for c in (*one_way, *both):
        renew_early(c)
    weights()
    for c in (*one_way, *both):
        renew_late(c)

    def early(x):
        for y0 in range(0, NY, 2):
            sides = []
            for y in (y0, y0 + 1):
                parts = []
                for a, o in BLOCKS:
                    dx, dy = (0, o) if a == 1 else (o, 0)
                    parts += [ub[x + H + dx, y + H + dy, c] for c in range(chunks)]
                sides.append(jnp.concatenate(parts, axis=0))
            out = jnp.dot(s["w_early"][...], jnp.concatenate(sides, axis=1), preferred_element_type=f32)
            for q in range(2):
                part = out[:, q * NZ:(q + 1) * NZ]
                smooth = part[2 * F:]
                for o in (-H, H):
                    for u, v in ((x + o, y0 + q), (x, y0 + q + o)):
                        if 0 <= u < NX and 0 <= v < NY:
                            smooth = smooth + box[u + H, v + H]
                acc[x, y0 + q, pl.ds(0, F)] = part[:F] + part[F:2 * F]
                acc[x, y0 + q, pl.ds(F, F)] = smooth

    for x in range(NX):
        early(x)

    def summed(spread, n):
        at = n * 2 * ROWS
        return spread[at:at + ROWS] + spread[at + ROWS:at + 2 * ROWS]

    def mixed_along(columns):
        sides = [
            jnp.concatenate([split16(t[:, n * NZ:(n + 1) * NZ]) for n in range(2) for t in terms], axis=0)
            for terms in columns
        ]
        out = jnp.dot(s["w_along"][...], jnp.concatenate(sides, axis=1), preferred_element_type=f32)
        out = out[:F] + out[F:]
        return [out[:, q * NZ:(q + 1) * NZ] for q in range(2)]

    def along(x):
        lines = [ub[x + H, y + H, c] for y in range(NY) for c in range(chunks)]
        spread = jnp.dot(jnp.concatenate(lines, axis=0), s["band"][:NZ], preferred_element_type=f32)
        terms = [[summed(spread, y * chunks + c) for c in range(chunks)] for y in range(NY)]
        for y0 in range(0, NY, 2):
            linear = mixed_along(terms[y0:y0 + 2])
            for q in range(2):
                acc[x, y0 + q, pl.ds(0, F)] += linear[q]
                for c in range(chunks):
                    acc[x, y0 + q, pl.ds(F + c * ROWS, ROWS)] += terms[y0 + q][c][:, 2 * NZ:]

    for x in range(NX):
        along(x)

    for r in rims_in:
        r.arrived()

    lines = []
    for g in range(groups):
        for c in range(chunks):
            lines.append(split16(jnp.where(
                lane % SLOT < SLOT // 2,
                jnp.where(above["gz"], rim_up[c, g], 0.0), jnp.where(below["gz"], rim_low[c, g], 0.0),
            )))
    spread = jnp.dot(jnp.concatenate(lines, axis=0), s["band"][NZ:], preferred_element_type=f32)
    terms = [[summed(spread, g * chunks + c) for c in range(chunks)] for g in range(groups)]
    at_ends = (lane < SLOT // 2) | (lane >= NZ - SLOT // 2)
    for g0 in range(0, groups, 2):
        linear = mixed_along(terms[g0:g0 + 2])
        for q in range(2):
            g = g0 + q
            lapse = (1.0 + 0.25 * jnp.tanh(rim[0, g, 0:1, :])) * (64.0 / 12.0)
            for c in range(chunks):
                extra = lapse * linear[q][c * ROWS:(c + 1) * ROWS] + terms[g][c][:, 2 * NZ:]
                for j in range(slots):
                    x, y = g * (slots // NY) + j // NY, j % NY
                    placed = jnp.where(at_ends, pltpu.roll(extra, (NZ - SLOT * j) % NZ, 1), 0.0)
                    acc[x, y, pl.ds(F + c * ROWS, ROWS)] += placed

    for a in range(2):
        n = SIDES.index((a, -1))
        inside[(a, -1)].arrived()
        pl.when(below[AXES[a]])(functools.partial(add_side, box, acc, acc, w_late, n))

    def finish(x, _):
        for y in range(NY - H):
            slope_ref[x * NY + y], value_ref[x * NY + y] = finished(box, acc, x, y)
        return 0

    lax.fori_loop(0, NX - H, finish, 0)

    for a in range(2):
        inside[(a, 1)].arrived()

        @pl.when(jnp.logical_not(above[AXES[a]]))
        def _(a=a):
            def step(i, _):
                for h in range(H):
                    at = (NX, NY)[a] + H + h
                    where = (at, i + H) if a == 0 else (i + H, at)
                    box[where] = jnp.zeros((F, NZ), f32)
                return 0

            lax.fori_loop(0, (NY, NX)[a], step, 0)

    for r in routes.values():
        r.all_sent()


def put_out(slope_in, value_in, acc_in, box, w_late, slope_hbm, value_hbm, slope_rest, value_rest, acc, sem):
    NX, NY = acc_in.shape[:2]
    sources = ((slope_in, slope_rest, slope_hbm), (value_in, value_rest, value_hbm))

    def send(x, y, rest):
        k = x * NY + y
        for n, source in enumerate(sources):
            pltpu.make_async_copy(source[rest].at[k], source[2].at[:, k], sem.at[n]).start()

    for x in range(NX - H):
        for y in range(NY - H):
            send(x, y, 0)
    add_side(box, acc_in, acc, w_late, SIDES.index((0, 1)))
    add_side(box, acc_in, acc, w_late, SIDES.index((1, 1)), lambda x, y: x >= NX - H)

    def finish(x, y):
        k = x * NY + y
        slope_rest[k], value_rest[k] = finished(box, acc, x, y)

    for x in range(NX):
        for y in range(NY - H if x < NX - H else 0, NY):
            finish(x, y)
            send(x, y, 1)
    for n in range(2):
        pltpu.make_async_copy(slope_rest, value_rest, sem.at[n]).wait()


def local(fields_now, parent, advect, diffuse, box_shift):
    dims = fields_now.shape
    F, NX, NY, NZ = dims
    flat = (F, NX * NY, NZ)
    by_cell = (NX * NY, F, NZ)
    vmem = pl.BlockSpec(memory_space=pltpu.VMEM)
    hbm = pl.BlockSpec(memory_space=pltpu.HBM)
    operands = [
        pltpu.with_memory_space_constraint(x, pltpu.HBM)
        for x in (
            box_shift, fields_now.reshape(flat), parent.reshape(flat), advect, diffuse,
            jnp.asarray(coefficients(F)), jnp.asarray(band(NZ), bf16),
        )
    ]
    held = [
        pltpu.VMEM((NX, NY, 2 * F, NZ), f32),
        pltpu.VMEM((NX + 2 * H, NY + 2 * H, F, NZ), f32),
        pltpu.VMEM((len(SIDES), 4 * F, 4 * F), bf16),
    ]
    results = pl.pallas_call(
        functools.partial(kernel, dims),
        out_shape=[pltpu.VMEM(by_cell, f32)] * 2 + held,
        in_specs=[hbm] * len(operands),
        out_specs=[vmem] * 5,
        scratch_shapes=list(scratch(dims).values()),
        compiler_params=pltpu.CompilerParams(
            collective_id=0, has_side_effects=True, vmem_limit_bytes=VMEM_BYTES
        ),
    )(*operands)
    slope, value = pl.pallas_call(
        put_out,
        out_shape=[jax.ShapeDtypeStruct(flat, f32)] * 2,
        in_specs=[vmem] * 5,
        out_specs=[hbm] * 2,
        scratch_shapes=[pltpu.VMEM(by_cell, f32)] * 2 + [held[0], pltpu.SemaphoreType.DMA((2,))],
        compiler_params=pltpu.CompilerParams(vmem_limit_bytes=VMEM_BYTES),
    )(*results)
    return slope.reshape(dims), value.reshape(dims)


VMEM_BYTES = 40 * 2**20


def solution(mesh):
    return jax.shard_map(
        local,
        mesh=mesh,
        in_specs=(P(None, "gx", "gy", "gz"), P(None, "gx", "gy", "gz"), P(), P(), P()),
        out_specs=(P(None, "gx", "gy", "gz"), P(None, "gx", "gy", "gz")),
        check_vma=False,
    )
```
